32 devices in a mesh: dp: 32 (over z, y, x, core).
Axes of the slice: x: 2, y: 2, z: 4, core: 2. Of those that a mesh axis runs over, the one named last changes fastest.
Arguments:
- tokens: bfloat16 [8192, 1024], P('dp'), may hold values from -6 to 6
- cotangent: bfloat16 [8192, 1024], P('dp'), may hold values from -6 to 6
- destination: int32 [8192], replicated, may hold values from 0 to 8191, as said below
- lengths: int32 [32, 4], P('dp'), may hold values from 1 to 192, 256 in all within a row
- norm_gains: bfloat16 [2, 2, 1024], P(None, None, 'dp'), may hold values from 0.5 to 1.5
- in_proj: bfloat16 [2, 1024, 3352], P(None, 'dp'), may hold values from -0.1875 to 0.1875
- conv_weight: bfloat16 [2, 4, 1792], P(None, None, 'dp'), may hold values from -3 to 3
- ssm_gain: bfloat16 [2, 1536], P(None, 'dp'), may hold values from 0.5 to 1.5
- mixer_out: bfloat16 [2, 1536, 1024], P(None, 'dp'), may hold values from -0.15625 to 0.15625
- qkv_proj: bfloat16 [2, 1024, 768], P(None, 'dp'), may hold values from -0.1875 to 0.1875
- attn_out: bfloat16 [2, 512, 1024], P(None, 'dp'), may hold values from -1 to 1
- gate_up: bfloat16 [2, 1024, 4096], P(None, 'dp'), may hold values from -0.1875 to 0.1875
- down_proj: bfloat16 [2, 2048, 1024], P(None, 'dp'), may hold values from -0.125 to 0.125
- a_log: float32 [2, 24], replicated, may hold values from 0 to 2.5
- d_skip: float32 [2, 24], replicated, may hold values from 0.5 to 1.5
- dt_bias: float32 [2, 24], replicated, may hold values from -6 to -2
Outputs:
- out_tokens: bfloat16 [8192, 1024], P('dp')
- in_grad: float32 [8192, 1024], P('dp')
- grad_norm_gains: float32 [2, 2, 1024], P(None, None, 'dp')
- grad_in_proj: float32 [2, 1024, 3352], P(None, 'dp')
- grad_conv_weight: float32 [2, 4, 1792], P(None, None, 'dp')
- grad_ssm_gain: float32 [2, 1536], P(None, 'dp')
- grad_mixer_out: float32 [2, 1536, 1024], P(None, 'dp')
- grad_qkv_proj: float32 [2, 1024, 768], P(None, 'dp')
- grad_attn_out: float32 [2, 512, 1024], P(None, 'dp')
- grad_gate_up: float32 [2, 1024, 4096], P(None, 'dp')
- grad_down_proj: float32 [2, 2048, 1024], P(None, 'dp')
- grad_a_log: float32 [2, 24], replicated
- grad_d_skip: float32 [2, 24], replicated
- grad_dt_bias: float32 [2, 24], replicated
The draws below stay inside these ranges and needn't reach their ends.
Inputs may be any that keep to these rules, and one draw needn't show every extreme that they name: `destination`: A permutation of the dealt rows; the 256 rows that arrive on each device are dealt in equal numbers to every device. Each device's 4 lengths add up to 256, and the longest of them is exactly 192.
All inputs are finite; a program needn't handle non-finite values.
Results may differ from the reference program's by a relative error of at most 0.023.
Values may be sent and summed in bfloat16 or wider, within the bound.
A program may use at most 320 MiB of HBM per device.

```python
import math
import jax
import jax.numpy as jnp
import numpy as np
from jax import lax

D = 1024
FF = 2048
HEADS = 24
HDIM = 64
STATE = 128
CONV = 4
QH = 8
KVH = 2
HD = 64
LAYERS = 2
SCAN_BLOCK = 128
DOCS = 4
TOK_DEV = 256
SEQ_MAX = 192
TOKENS = 8192
INNER = 1536
CONVCH = 1792
INPROJ = 3352
QKV = 768
N_DP = 32


def draw_destination(key, part):
    devices = TOKENS // TOK_DEV
    share = TOK_DEV // devices
    keys = jax.random.split(jax.random.fold_in(key, 11), 2 * devices)
    ranking = jax.vmap(lambda item: jax.random.permutation(item, TOK_DEV))(keys[:devices]).astype(jnp.int32)
    seating = jax.vmap(lambda item: jax.random.permutation(item, TOK_DEV))(keys[devices:]).astype(jnp.int32)
    target = ranking // share
    within = ranking % share
    source = jnp.arange(devices, dtype=jnp.int32)[:, None]
    placed = seating[target, source * share + within]
    return (target * TOK_DEV + placed).reshape(-1)


def level_of(own_key, dims, shards, smallest, high):
    def one(dim, blocks):
        heights = jax.random.uniform(jax.random.fold_in(jax.random.fold_in(own_key, 6), dim), (blocks,), jnp.float32, smallest / len(shards), high / len(shards))
        return jnp.repeat(jnp.exp(heights), dims[dim] // blocks).reshape((-1,) + (1,) * (len(dims) - dim - 1))

    level = one(*shards[0])
    for cut in shards[1:]:
        level = level * one(*cut)
    return level


def profile(amount, total, limit, slope):
    portions = [(1 << 20) // math.isqrt(grade ** slope) + 1 for grade in range(2, amount + 1)]
    rest, holding = total - limit - (amount - 1), [1] * (amount - 1)
    while rest > 0:
        candidates = [i for i in range(amount - 1) if holding[i] < limit]
        whole, budget = sum([portions[i] for i in candidates]), rest
        for i in candidates:
            more = min(limit - holding[i], max(1, budget * portions[i] // whole), rest)
            holding[i] = holding[i] + more
            rest = rest - more
    return np.array([limit] + holding)


def uneven_parts(stream_key, count, total, limit, lean):
    if count == 2:
        one = jax.random.randint(stream_key, (), max(1, total - limit), min(limit, total - 1) + 1)
        return jnp.stack([one, total - one])
    sizes = jnp.asarray(profile(count, total, limit, lean), jnp.int32)
    pairs = (count - 1) // 2
    source_of, receiver = sizes[1:1 + 2 * pairs:2], sizes[2:2 + 2 * pairs:2]
    room = jnp.minimum(source_of - 1, limit - receiver)
    moved = jax.random.randint(jax.random.fold_in(stream_key, 1), (pairs,), 0, 1 << 20) % (room + 1)
    sizes = sizes.at[1:1 + 2 * pairs:2].set(source_of - moved).at[2:2 + 2 * pairs:2].set(receiver + moved)
    return sizes[jax.random.permutation(jax.random.fold_in(stream_key, 2), count)]


def noise(stream_key, extent, width, bound, shards=(), kind=jnp.bfloat16):
    values = jax.random.normal(stream_key, extent, jnp.float32) * width
    if len(shards) > 0:
        values = level_of(stream_key, extent, shards, -0.22, 0.18) * values
    return jnp.clip(values, min=-bound, max=bound).astype(kind)


def setup_inputs(seed: int = 0) -> dict:
    arg_keys = jax.random.split(jax.random.key(seed), 17)
    return {
        "tokens": noise(arg_keys[0], (TOKENS, D), 1.0, 6.0, ((0, 32),)),
        "cotangent": noise(arg_keys[1], (TOKENS, D), 1.0, 6.0, ((0, 32),)),
        "destination": draw_destination(jax.random.fold_in(arg_keys[16], 71), 0),
        "lengths": jax.vmap(lambda own: uneven_parts(own, DOCS, TOK_DEV, SEQ_MAX, 2))(jax.random.split(arg_keys[3], N_DP)).reshape((N_DP, DOCS)).astype(jnp.int32),
        "norm_gains": jnp.clip(1.0 + 0.1 * jax.random.normal(arg_keys[4], (LAYERS, 2, D), jnp.float32), 0.5, 1.5).astype(jnp.bfloat16),
        "in_proj": noise(arg_keys[5], (LAYERS, D, INPROJ), D ** -0.5, 0.1875, ((1, 32),)),
        "conv_weight": noise(arg_keys[6], (LAYERS, CONV, CONVCH), CONV ** -0.5, 3.0, ((2, 32),)),
        "ssm_gain": jnp.clip(1.0 + 0.1 * jax.random.normal(arg_keys[7], (LAYERS, INNER), jnp.float32), 0.5, 1.5).astype(jnp.bfloat16),
        "mixer_out": noise(arg_keys[8], (LAYERS, INNER, D), INNER ** -0.5, 0.15625, ((1, 32),)),
        "qkv_proj": noise(arg_keys[9], (LAYERS, D, QKV), D ** -0.5, 0.1875, ((1, 32),)),
        "attn_out": noise(arg_keys[10], (LAYERS, QH * HD, D), (QH * HD // 16) ** -0.5, 1.0, ((1, 32),)),
        "gate_up": noise(arg_keys[11], (LAYERS, D, 2 * FF), D ** -0.5, 0.1875, ((1, 32),)),
        "down_proj": noise(arg_keys[12], (LAYERS, FF, D), FF ** -0.5, 0.125, ((1, 32),)),
        "a_log": jnp.clip(jax.random.uniform(arg_keys[13], (LAYERS, HEADS), jnp.float32, 0.0, 2.5), 0.0, 2.5),
        "d_skip": jnp.clip(jax.random.uniform(arg_keys[14], (LAYERS, HEADS), jnp.float32, 0.5, 1.5), 0.5, 1.5),
        "dt_bias": jnp.clip(jax.random.uniform(arg_keys[15], (LAYERS, HEADS), jnp.float32, -6.0, -2.0), -6.0, -2.0),
    }


@jax.custom_vjp
def low(v):
    return lax.optimization_barrier(v.astype(jnp.bfloat16)).astype(jnp.float32)

@jax.custom_vjp
def low_back(v):
    return v

def low_keep(v):
    return (low(v), None)

def low_pass(kept, grad):
    return (grad,)

def back_keep(v):
    return (v, None)

def back_low(kept, grad):
    return (low(grad),)
low.defvjp(low_keep, low_pass)
low_back.defvjp(back_keep, back_low)
EPSILON = 1e-05
ROPE_BASE = 100000000000.0
SCORE_SCALE = 0.125
HIGHEST = lax.Precision.HIGHEST

def project(left, right, precise):
    return jnp.dot(left, right, preferred_element_type=jnp.float32, precision=precise)

def rms_norm(values, gain):
    return values * lax.rsqrt(lax.optimization_barrier(jnp.mean(values * values, axis=-1, keepdims=True)) + EPSILON) * gain

def doc_layout(doc_lengths, rows_count):
    rows_index = jnp.arange(rows_count, dtype=jnp.int32)
    doc_lengths = doc_lengths.astype(jnp.int32)
    doc_ends = jnp.cumsum(doc_lengths, dtype=jnp.int32).astype(jnp.int32)
    segment = lax.optimization_barrier(jnp.sum((rows_index[:, None] >= doc_ends[None, :]).astype(jnp.int32), axis=1, dtype=jnp.int32)).astype(jnp.int32)
    doc_starts = (doc_ends - doc_lengths).astype(jnp.int32)
    member = (segment[:, None] == jnp.arange(doc_lengths.shape[0], dtype=jnp.int32)[None, :]).astype(jnp.int32)
    position = (rows_index - lax.optimization_barrier(jnp.sum(member * doc_starts[None, :], axis=1, dtype=jnp.int32))).astype(jnp.int32)
    return (segment, position)

def causal_conv(channels, kernel, position):
    taps = kernel.shape[0]
    summed = channels * kernel[taps - 1]
    for offset in range(1, taps):
        shifted = jnp.pad(channels, ((offset, 0), (0, 0)))[:channels.shape[0]]
        valid = (position >= offset).astype(channels.dtype)
        summed = summed + shifted * kernel[taps - 1 - offset] * valid[:, None]
    return summed

def rotate(values, position):
    half_dim = values.shape[-1] // 2
    inverse = ROPE_BASE ** (-(jnp.arange(half_dim, dtype=jnp.float32) * 2.0 / values.shape[-1]))
    angles = position.astype(jnp.float32)[:, None] * inverse[None, :]
    target = (values.shape[0],) + (1,) * (values.ndim - 2) + (half_dim,)
    cosine = jnp.cos(angles).reshape(target)
    sine = jnp.sin(angles).reshape(target)
    front = values[..., :half_dim]
    rear = values[..., half_dim:]
    return jnp.concatenate([front * cosine - rear * sine, rear * cosine + front * sine], axis=-1)

def block_step(carry, inputs):
    state, last_segment = carry
    x_part, b_part, c_part, dt_part, decay_log, seg_part = inputs
    cumul = jnp.cumsum(decay_log, axis=0)
    block_len = seg_part.shape[0]
    rows_index = jnp.arange(block_len, dtype=jnp.int32)
    inside = (seg_part[:, None] == seg_part[None, :]) & (rows_index[:, None] >= rows_index[None, :])
    gaps = cumul[:, None, :] - cumul[None, :, :]
    decay = jnp.exp(jnp.minimum(gaps, 0.0)) * inside[:, :, None].astype(cumul.dtype)
    affinity = project(c_part, b_part.T, HIGHEST)
    scaled = x_part * dt_part[:, :, None]
    within = jnp.einsum('ijh,jhp->ihp', decay * affinity[:, :, None], scaled, precision=HIGHEST)
    enters = (seg_part == last_segment).astype(cumul.dtype)
    from_state = jnp.einsum('in,hpn->ihp', c_part, state, precision=HIGHEST)
    carried = from_state * (jnp.exp(cumul) * enters[:, None])[:, :, None]
    final_segment = seg_part[block_len - 1].astype(jnp.int32)
    same_final = (seg_part == final_segment).astype(cumul.dtype)
    toward = jnp.exp(cumul[block_len - 1][None, :] - cumul) * same_final[:, None]
    fresh = jnp.einsum('jh,jhp,jn->hpn', toward, scaled, b_part, precision=HIGHEST)
    retain = jnp.exp(cumul[block_len - 1]) * (final_segment == last_segment).astype(cumul.dtype)
    new_state = state * retain[:, None, None] + fresh
    return ((new_state, final_segment), within + carried)

def state_space(x_heads, b_all, c_all, dt_all, rates, segment):
    rows_count = x_heads.shape[0]
    blocks = rows_count // SCAN_BLOCK

    def split_rows(values):
        return values.reshape((blocks, SCAN_BLOCK) + values.shape[1:])
    start = (jnp.zeros((HEADS, HDIM, STATE), jnp.float32), jnp.array(-1, dtype=jnp.int32))
    decay_log = dt_all * rates[None, :]
    inputs = (split_rows(x_heads), split_rows(b_all), split_rows(c_all), split_rows(dt_all), split_rows(decay_log), split_rows(segment.astype(jnp.int32)))
    _, outputs = lax.scan(jax.checkpoint(block_step), start, inputs)
    return outputs.reshape(rows_count, HEADS, HDIM)

def attention(normed, w_qkv, w_attn, segment, position, precise):
    rows_count = normed.shape[0]
    packed = low_back(project(normed, w_qkv, precise))
    queries = packed[:, :QH * HD].reshape(rows_count, KVH, QH // KVH, HD)
    key_heads = packed[:, QH * HD:(QH + KVH) * HD].reshape(rows_count, KVH, HD)
    value_heads = low(packed[:, (QH + KVH) * HD:].reshape(rows_count, KVH, HD))
    queries = low(rotate(queries, position))
    key_heads = low(rotate(key_heads, position))
    raw_scores = jnp.einsum('skgd,tkd->kgst', queries, key_heads, precision=precise)
    scores = low_back(raw_scores) * SCORE_SCALE
    rows_index = jnp.arange(rows_count, dtype=jnp.int32)
    allowed = (segment[:, None] == segment[None, :]) & (rows_index[:, None] >= rows_index[None, :])
    scores = jnp.where(allowed[None, None, :, :], scores, -1e+30)
    largest = lax.optimization_barrier(jnp.max(scores, axis=-1, keepdims=True))
    expo = jnp.exp(scores - largest)
    probs = low(expo / lax.optimization_barrier(jnp.sum(expo, axis=-1, keepdims=True)))
    context = jnp.einsum('kgst,tkd->skgd', probs, value_heads, precision=precise)
    context = low(low_back(context.reshape(rows_count, QH * HD)))
    return low_back(project(context, w_attn, precise))

def hybrid_layer(hidden, segment, position, weights, head_params, precise):
    gains, w_in, kernel, gain_inner, w_mix, w_qkv, w_attn, w_gate_up, w_down = weights
    log_rates, skip_coef, step_bias = head_params
    rows_count = hidden.shape[0]
    normed = low(rms_norm(hidden, gains[0]))
    inner = low_back(project(normed, w_in, precise))
    gate_z = inner[:, :INNER]
    conv_in = inner[:, INNER:INNER + CONVCH]
    step_raw = inner[:, INNER + CONVCH:]
    conv_out = jax.nn.silu(causal_conv(conv_in, kernel, position))
    x_heads = conv_out[:, :INNER].reshape(rows_count, HEADS, HDIM)
    b_all = conv_out[:, INNER:INNER + STATE]
    c_all = conv_out[:, INNER + STATE:]
    dt_all = jax.nn.softplus(step_raw + step_bias[None, :])
    rates = -jnp.exp(log_rates)
    scanned = state_space(x_heads, b_all, c_all, dt_all, rates, segment) + skip_coef[None, :, None] * x_heads
    gated = scanned.reshape(rows_count, INNER) * jax.nn.silu(gate_z)
    mixed = low(rms_norm(gated, gain_inner))
    mamba_branch = low_back(project(mixed, w_mix, precise))
    attn_branch = attention(normed, w_qkv, w_attn, segment, position, precise)
    middle = hidden + mamba_branch + attn_branch
    normed_two = low(rms_norm(middle, gains[1]))
    gate_values = low_back(project(normed_two, w_gate_up, precise))
    activated = low(jax.nn.silu(gate_values[:, :FF]) * gate_values[:, FF:])
    return middle + low_back(project(activated, w_down, precise))

def reference(tokens, cotangent, destination, lengths, norm_gains, in_proj, conv_weight, ssm_gain, mixer_out, qkv_proj, attn_out, gate_up, down_proj, a_log, d_skip, dt_bias):
    start_rows = jnp.zeros((TOKENS, D), jnp.float32).at[destination].set(tokens.astype(jnp.float32))
    start_cot = jnp.zeros((TOKENS, D), jnp.float32).at[destination].set(cotangent.astype(jnp.float32))
    segments, positions = jax.vmap(lambda row: doc_layout(row, TOK_DEV))(lengths)
    weights = tuple((item.astype(jnp.float32) for item in (norm_gains, in_proj, conv_weight, ssm_gain, mixer_out, qkv_proj, attn_out, gate_up, down_proj)))
    heads = tuple((item.astype(jnp.float32) for item in (a_log, d_skip, dt_bias)))

    def forward(rows, weight_set, head_set):

        def slab(carry, inputs):
            hidden, segment, position = inputs
            for layer_idx in range(LAYERS):
                layer_weights = tuple((item[layer_idx] for item in weight_set))
                layer_heads = tuple((item[layer_idx] for item in head_set))
                hidden = hybrid_layer(hidden, segment, position, layer_weights, layer_heads, HIGHEST)
            return (carry, hidden)
        _, result = lax.scan(jax.checkpoint(slab), None, (rows.reshape(N_DP, TOK_DEV, D), segments, positions))
        return result
    result, puller = jax.vjp(forward, start_rows, weights, heads)
    grad_rows, grad_weights, grad_heads = puller(start_cot.reshape(N_DP, TOK_DEV, D))
    out_tokens = result.reshape(TOKENS, D)[destination].astype(jnp.bfloat16)
    in_grad = grad_rows.reshape(TOKENS, D)[destination]
    return (out_tokens, in_grad, grad_weights[0], grad_weights[1], grad_weights[2], grad_weights[3], grad_weights[4], grad_weights[5], grad_weights[6], grad_weights[7], grad_weights[8], grad_heads[0], grad_heads[1], grad_heads[2])
```

```python
import jax
import jax.numpy as jnp
from jax import lax
from jax.sharding import PartitionSpec as P

FF = 2048
HEADS = 24
HDIM = 64
STATE = 128
QH = 8
KVH = 2
HD = 64
LAYERS = 2
SCAN_BLOCK = 128
INNER = 1536
CONVCH = 1792


EPSILON = 1e-05
ROPE_BASE = 100000000000.0
SCORE_SCALE = 0.125
HIGHEST = lax.Precision.HIGHEST
PLAIN = lax.Precision.DEFAULT


def lower_value(v):
    return lax.optimization_barrier(v.astype(jnp.bfloat16)).astype(jnp.float32)


def passing_value(v):
    return v


def rounder_keep(v):
    return (lower_value(v), None)


def rounder_pass(kept, grad):
    return (grad,)


def plain_keep(v):
    return (v, None)


def plain_lower(kept, grad):
    return (lower_value(grad),)


def make_rounders():
    value_round = jax.custom_vjp(lower_value)
    value_round.defvjp(rounder_keep, rounder_pass)
    grad_round = jax.custom_vjp(passing_value)
    grad_round.defvjp(plain_keep, plain_lower)
    return (value_round, grad_round)


def project(left, right, precise):
    return jnp.dot(left, right, preferred_element_type=jnp.float32, precision=precise)


def rms_norm(values, gain):
    return values * lax.rsqrt(jnp.mean(values * values, axis=-1, keepdims=True) + EPSILON) * gain


def doc_layout(doc_lengths, rows_count):
    rows_index = jnp.arange(rows_count, dtype=jnp.int32)
    doc_ends = jnp.cumsum(doc_lengths, dtype=jnp.int32)
    segment = jnp.sum(
        (rows_index[:, None] >= doc_ends[None, :]).astype(jnp.int32), axis=1, dtype=jnp.int32
    )
    doc_starts = doc_ends - doc_lengths
    member = (
        segment[:, None] == jnp.arange(doc_lengths.shape[0], dtype=jnp.int32)[None, :]
    ).astype(jnp.int32)
    position = rows_index - jnp.sum(member * doc_starts[None, :], axis=1, dtype=jnp.int32)
    return (segment, position)


def causal_conv(channels, kernel, position):
    taps = kernel.shape[0]
    summed = channels * kernel[taps - 1]
    for offset in range(1, taps):
        shifted = jnp.pad(channels, ((offset, 0), (0, 0)))[: channels.shape[0]]
        valid = (position >= offset).astype(channels.dtype)
        summed = summed + shifted * kernel[taps - 1 - offset] * valid[:, None]
    return summed


def rotate(values, position):
    half_dim = values.shape[-1] // 2
    inverse = ROPE_BASE ** (-(jnp.arange(half_dim, dtype=jnp.float32) * 2.0 / values.shape[-1]))
    angles = position.astype(jnp.float32)[:, None] * inverse[None, :]
    target = (values.shape[0],) + (1,) * (values.ndim - 2) + (half_dim,)
    cosine = jnp.cos(angles).reshape(target)
    sine = jnp.sin(angles).reshape(target)
    front = values[..., :half_dim]
    rear = values[..., half_dim:]
    return jnp.concatenate([front * cosine - rear * sine, rear * cosine + front * sine], axis=-1)


def state_space(x_heads, b_all, c_all, dt_all, rates, segment):
    rows_count = x_heads.shape[0]
    rows_index = jnp.arange(rows_count, dtype=jnp.int32)
    inside = (segment[:, None] == segment[None, :]) & (rows_index[:, None] >= rows_index[None, :])
    mask = inside.astype(jnp.float32)
    cumul = project(mask, dt_all * rates[None, :], HIGHEST).T
    gaps = cumul[:, :, None] - cumul[:, None, :]
    decay = jnp.exp(jnp.where(inside[None], jnp.minimum(gaps, 0.0), -1e30))
    affinity = project(c_all, b_all.T, HIGHEST)
    scaled = x_heads * dt_all[:, :, None]
    return jnp.einsum("hij,jhp->ihp", decay * affinity[None], scaled, precision=HIGHEST)


def attention(normed, w_qkv, w_attn, segment, position, precise, rounders):
    value_round, grad_round = rounders
    rows_count = normed.shape[0]
    packed = grad_round(project(normed, w_qkv, precise))
    queries = packed[:, : QH * HD].reshape(rows_count, KVH, QH // KVH, HD)
    key_heads = packed[:, QH * HD : (QH + KVH) * HD].reshape(rows_count, KVH, HD)
    value_heads = value_round(packed[:, (QH + KVH) * HD :].reshape(rows_count, KVH, HD))
    queries = value_round(rotate(queries, position))
    key_heads = value_round(rotate(key_heads, position))
    raw_scores = jnp.einsum("skgd,tkd->kgst", queries, key_heads, precision=precise)
    scores = grad_round(raw_scores) * SCORE_SCALE
    rows_index = jnp.arange(rows_count, dtype=jnp.int32)
    allowed = (segment[:, None] == segment[None, :]) & (rows_index[:, None] >= rows_index[None, :])
    scores = jnp.where(allowed[None, None, :, :], scores, -1e30)
    largest = jnp.max(scores, axis=-1, keepdims=True)
    expo = jnp.exp(scores - largest)
    probs = value_round(expo / jnp.sum(expo, axis=-1, keepdims=True))
    context = jnp.einsum("kgst,tkd->skgd", probs, value_heads, precision=precise)
    context = value_round(grad_round(context.reshape(rows_count, QH * HD)))
    return grad_round(project(context, w_attn, precise))


def hybrid_layer(hidden, segment, position, weights, head_params, precise, rounders):
    value_round, grad_round = rounders
    gains, w_in, kernel, gain_inner, w_mix, w_qkv, w_attn, w_gate_up, w_down = weights
    log_rates, skip_coef, step_bias = head_params
    rows_count = hidden.shape[0]
    normed = value_round(rms_norm(hidden, gains[0]))
    inner = grad_round(project(normed, w_in, precise))
    gate_z = inner[:, :INNER]
    conv_in = inner[:, INNER : INNER + CONVCH]
    step_raw = inner[:, INNER + CONVCH :]
    conv_out = jax.nn.silu(causal_conv(conv_in, kernel, position))
    x_heads = conv_out[:, :INNER].reshape(rows_count, HEADS, HDIM)
    b_all = conv_out[:, INNER : INNER + STATE]
    c_all = conv_out[:, INNER + STATE :]
    dt_all = jax.nn.softplus(step_raw + step_bias[None, :])
    rates = -jnp.exp(log_rates)
    scanned = (
        state_space(x_heads, b_all, c_all, dt_all, rates, segment)
        + skip_coef[None, :, None] * x_heads
    )
    gated = scanned.reshape(rows_count, INNER) * jax.nn.silu(gate_z)
    mixed = value_round(rms_norm(gated, gain_inner))
    mamba_branch = grad_round(project(mixed, w_mix, precise))
    attn_branch = attention(normed, w_qkv, w_attn, segment, position, precise, rounders)
    middle = hidden + mamba_branch + attn_branch
    normed_two = value_round(rms_norm(middle, gains[1]))
    gate_values = grad_round(project(normed_two, w_gate_up, precise))
    activated = value_round(jax.nn.silu(gate_values[:, :FF]) * gate_values[:, FF:])
    return middle + grad_round(project(activated, w_down, precise))


def shards(
    tokens,
    cotangent,
    destination,
    lengths,
    norm_gains,
    in_proj,
    conv_weight,
    ssm_gain,
    mixer_out,
    qkv_proj,
    attn_out,
    gate_up,
    down_proj,
    a_log,
    d_skip,
    dt_bias,
):
    rounders = make_rounders()
    devices = lax.axis_size("dp")
    myself = lax.axis_index("dp")
    rows_here = tokens.shape[0]
    share = rows_here // devices
    model_width = tokens.shape[1]
    slabs = destination.reshape(devices, rows_here)
    local_rows = jnp.arange(rows_here, dtype=jnp.int32)
    own_slab = lax.dynamic_slice_in_dim(slabs, myself, 1, 0)[0]
    order = jnp.argsort(own_slab // rows_here * rows_here + local_rows)
    outgoing_rows = tokens[order].reshape(devices, share, model_width)
    outgoing_cot = cotangent[order].reshape(devices, share, model_width)
    arrived = (
        lax.all_to_all(outgoing_rows, "dp", split_axis=0, concat_axis=0, tiled=True),
        lax.all_to_all(outgoing_cot, "dp", split_axis=0, concat_axis=0, tiled=True),
    )
    ranking = jnp.where(
        slabs // rows_here == myself, local_rows[None, :], rows_here + local_rows[None, :]
    )
    chosen = jnp.argsort(ranking, axis=1)[:, :share]
    places = (jnp.take_along_axis(slabs, chosen, axis=1) % rows_here).reshape(-1)
    hidden = (
        jnp.zeros((rows_here, model_width), jnp.float32)
        .at[places]
        .set(arrived[0].reshape(-1, model_width).astype(jnp.float32))
    )
    upstream = (
        jnp.zeros((rows_here, model_width), jnp.float32)
        .at[places]
        .set(arrived[1].reshape(-1, model_width).astype(jnp.float32))
    )
    segment, position = doc_layout(lengths[0], rows_here)

    def gather_layer(layer_idx):
        pieces = (
            lax.all_gather(norm_gains[layer_idx], "dp", axis=1, tiled=True),
            lax.all_gather(in_proj[layer_idx], "dp", axis=0, tiled=True),
            lax.all_gather(conv_weight[layer_idx], "dp", axis=1, tiled=True),
            lax.all_gather(ssm_gain[layer_idx], "dp", axis=0, tiled=True),
            lax.all_gather(mixer_out[layer_idx], "dp", axis=0, tiled=True),
            lax.all_gather(qkv_proj[layer_idx], "dp", axis=0, tiled=True),
            lax.all_gather(attn_out[layer_idx], "dp", axis=0, tiled=True),
            lax.all_gather(gate_up[layer_idx], "dp", axis=0, tiled=True),
            lax.all_gather(down_proj[layer_idx], "dp", axis=0, tiled=True),
        )
        return tuple((piece.astype(jnp.float32) for piece in pieces))

    def heads_of(layer_idx):
        return (a_log[layer_idx], d_skip[layer_idx], dt_bias[layer_idx])

    def layer_step(layer_input, weights, head_params):
        return hybrid_layer(layer_input, segment, position, weights, head_params, PLAIN, rounders)

    inputs_kept = []
    for layer_idx in range(LAYERS):
        weights = gather_layer(layer_idx)
        hidden, puller = jax.vjp(layer_step, hidden, weights, heads_of(layer_idx))
        inputs_kept.append(puller)
    leaving = hidden.astype(jnp.bfloat16)[places].reshape(devices, share, model_width)
    returned = lax.all_to_all(leaving, "dp", split_axis=0, concat_axis=0, tiled=True)
    out_tokens = (
        jnp.zeros((rows_here, model_width), jnp.bfloat16)
        .at[order]
        .set(returned.reshape(-1, model_width))
    )
    flowing = upstream
    owned_parts = [None] * LAYERS
    head_parts = [None] * LAYERS
    for layer_idx in reversed(range(LAYERS)):
        flowing, weight_terms, head_terms = inputs_kept[layer_idx](flowing)
        weight_terms = tuple(
            term.astype(jnp.bfloat16) if place > 3 or place == 1 else term
            for place, term in enumerate(weight_terms)
        )
        owned_parts[layer_idx] = (
            lax.psum_scatter(weight_terms[0], "dp", scatter_dimension=1, tiled=True),
            lax.psum_scatter(weight_terms[1], "dp", scatter_dimension=0, tiled=True),
            lax.psum_scatter(weight_terms[2], "dp", scatter_dimension=1, tiled=True),
            lax.psum_scatter(weight_terms[3], "dp", scatter_dimension=0, tiled=True),
            lax.psum_scatter(weight_terms[4], "dp", scatter_dimension=0, tiled=True),
            lax.psum_scatter(weight_terms[5], "dp", scatter_dimension=0, tiled=True),
            lax.psum_scatter(weight_terms[6], "dp", scatter_dimension=0, tiled=True),
            lax.psum_scatter(weight_terms[7], "dp", scatter_dimension=0, tiled=True),
            lax.psum_scatter(weight_terms[8], "dp", scatter_dimension=0, tiled=True),
        )
        head_parts[layer_idx] = head_terms
    stacked = tuple(
        (
            jnp.stack([owned_parts[layer_idx][member] for layer_idx in range(LAYERS)]).astype(jnp.float32)
            for member in range(9)
        )
    )
    head_local = tuple(
        (
            jnp.stack([head_parts[layer_idx][member] for layer_idx in range(LAYERS)])
            for member in range(3)
        )
    )
    head_total = lax.psum((head_local[0], head_local[1], head_local[2]), "dp")
    sending_back = flowing[places].reshape(devices, share, model_width)
    grads_home = lax.all_to_all(
        sending_back.astype(jnp.bfloat16), "dp", split_axis=0, concat_axis=0, tiled=True
    ).astype(sending_back.dtype)
    in_grad = (
        jnp.zeros((rows_here, model_width), jnp.float32)
        .at[order]
        .set(grads_home.reshape(-1, model_width))
    )
    return (
        out_tokens,
        in_grad,
        stacked[0],
        stacked[1],
        stacked[2],
        stacked[3],
        stacked[4],
        stacked[5],
        stacked[6],
        stacked[7],
        stacked[8],
        head_total[0],
        head_total[1],
        head_total[2],
    )


def solution(mesh):
    placed = (
        P("dp", None),
        P("dp", None),
        P(),
        P("dp", None),
        P(None, None, "dp"),
        P(None, "dp", None),
        P(None, None, "dp"),
        P(None, "dp"),
        P(None, "dp", None),
        P(None, "dp", None),
        P(None, "dp", None),
        P(None, "dp", None),
        P(None, "dp", None),
        P(),
        P(),
        P(),
    )
    return jax.shard_map(
        shards,
        mesh=mesh,
        in_specs=placed,
        out_specs=(
            P("dp", None),
            P("dp", None),
            P(None, None, "dp"),
            P(None, "dp", None),
            P(None, None, "dp"),
            P(None, "dp"),
            P(None, "dp", None),
            P(None, "dp", None),
            P(None, "dp", None),
            P(None, "dp", None),
            P(None, "dp", None),
            P(),
            P(),
            P(),
        ),
        check_vma=False,
    )
```

```python
import functools

import jax
import jax.numpy as jnp
from jax import lax
from jax.experimental import pallas as pl
from jax.experimental.pallas import tpu as pltpu
from jax.sharding import PartitionSpec as P

FF = 2048
HEADS = 24
HDIM = 64
STATE = 128
QH = 8
KVH = 2
HD = 64
LAYERS = 2
INNER = 1536
CONVCH = 1792
TAPS = 4
EPSILON = 1e-05
ROPE_BASE = 100000000000.0
SCORE_SCALE = 0.125
HIGHEST = lax.Precision.HIGHEST
F32 = jnp.float32
BF16 = jnp.bfloat16
MESH = pl.DeviceIdType.MESH

AG_CHUNKS = [(1, 3, (4, 3, 1, 2)), (0, 2, (1, 4, 3, 2)), (0, 3, (4, 3, 2, 1)), (0, 5, (2, 4, 3, 1)), (0, 0, (4, 3, 2, 1)), (1, 2, (1, 4, 3, 2)), (1, 1, (4, 3, 1, 2)), (1, 5, (4, 3, 1, 2)), (0, 4, (2, 1, 4, 3)), (1, 4, (4, 3, 1, 2)), (0, 1, (2, 1, 4, 3)), (1, 0, (4, 3, 2, 1))]
AG_EVENTS = [(1, 0), (0, 0), (5, 0), (2, 0), (3, 0), (8, 0), (10, 0), (4, 0), (6, 0), (7, 0), (8, 1), (0, 1), (10, 1), (2, 1), (0, 2), (9, 0), (2, 2), (0, 3), (2, 3), (11, 0), (4, 1), (1, 1), (6, 1), (5, 1), (7, 1), (6, 2), (3, 1), (4, 2), (7, 2), (6, 3), (9, 1), (7, 3), (11, 1), (4, 3), (8, 2), (1, 2), (5, 2), (10, 2), (3, 2), (11, 2), (9, 2), (1, 3), (5, 3), (3, 3), (8, 3), (10, 3), (9, 3), (11, 3)]
RS_CHUNKS = [(0, 0, 1792, (1, 2, 3, 4)), (1, 0, 512, (2, 3, 4, 1)), (2, 384, 768, (2, 3, 4, 1)), (0, 1792, 3352, (3, 4, 1, 2)), (4, 2048, 4096, (1, 2, 3, 4)), (5, 0, 512, (1, 2, 3, 4)), (5, 512, 1024, (1, 2, 3, 4)), (4, 0, 2048, (2, 3, 4, 1)), (3, 512, 1024, (3, 4, 1, 2)), (1, 512, 1024, (1, 2, 3, 4)), (2, 0, 384, (2, 1, 3, 4)), (3, 0, 512, (1, 2, 3, 4))]
RS_EVENTS = [(0, -1), (1, -1), (2, -1), (3, -1), (4, -1), (5, -1), (6, -1), (7, -1), (8, -1), (9, -1), (10, -1), (11, -1), (1, 0), (2, 0), (0, 0), (3, 0), (8, 0), (1, 1), (2, 1), (7, 0), (10, 0), (3, 1), (4, 0), (8, 1), (1, 2), (2, 2), (0, 1), (5, 0), (7, 1), (0, 2), (4, 1), (6, 0), (5, 1), (7, 2), (4, 2), (0, 3), (9, 0), (6, 1), (5, 2), (11, 0), (10, 1), (9, 1), (4, 3), (6, 2), (11, 1), (3, 2), (8, 2), (10, 2), (5, 3), (1, 3), (2, 3), (9, 2), (6, 3), (3, 3), (10, 3), (11, 2), (7, 3), (8, 3), (9, 3), (11, 3)]

SMALL_ROWS = 16


def dot(left, right):
    return jnp.dot(left, right, preferred_element_type=F32)


def dot_rt(left, right):
    return lax.dot_general(left, right, (((1,), (1,)), ((), ())), preferred_element_type=F32)


def flip(me, bit):
    step = 1 << bit
    return me + step * (1 - 2 * ((me // step) % 2))


def place(bits, free, mine, flipped=()):
    return tuple(
        slice(None) if b in free else 1 - mine[b] if b in flipped else mine[b]
        for b in reversed(range(bits))
    )


def greet(me, bits):
    barrier = pltpu.get_barrier_semaphore()
    for b in range(bits):
        pl.semaphore_signal(barrier, inc=1, device_id=(flip(me, b),), device_id_type=MESH)
    pl.semaphore_wait(barrier, bits)


def remote(me, src, dst, send, recv, bit):
    return pltpu.make_async_remote_copy(
        src_ref=src,
        dst_ref=dst,
        send_sem=send,
        recv_sem=recv,
        device_id=(flip(me, bit),),
        device_id_type=MESH,
    )


def gather_kernel(devices, chunks, events, layers, arrays, *refs):
    bits = devices.bit_length() - 1
    ins = refs[:arrays]
    outs = refs[arrays : arrays + layers * arrays]
    send_sem, recv_sem, csend_sem, crecv_sem, own_sem = refs[arrays + layers * arrays :]
    me = lax.axis_index("dp")
    mine = [(me // (1 << b)) % 2 for b in range(bits)]
    greet(me, bits)
    own, sends, cores, pending = [], [], [], {}
    for c, (l, a, order) in enumerate(chunks):
        here = outs[l * arrays + a].at[place(bits, (), mine)]
        src = ins[a].at[l]
        copy = remote(me, src, here, send_sem.at[c, 0], recv_sem.at[c, 0], order[0])
        copy.start()
        pending[c] = copy
        sends.append(copy)
        local = pltpu.make_async_copy(src, here, own_sem.at[c])
        local.start()
        own.append(local)
    for c, (l, a, order) in enumerate(chunks):
        here = outs[l * arrays + a].at[place(bits, (), mine)]
        copy = remote(me, ins[a].at[l], here, csend_sem.at[c, 0], crecv_sem.at[c, 0], 0)
        copy.start()
        sends.append(copy)
        cores.append(copy)
    for local in own:
        local.wait()
    for c, s in events:
        l, a, order = chunks[c]
        full = outs[l * arrays + a]
        pending[c].wait_recv()
        if s + 1 < bits - 1:
            view = full.at[place(bits, order[: s + 1], mine)]
            copy = remote(
                me, view, view, send_sem.at[c, s + 1], recv_sem.at[c, s + 1], order[s + 1]
            )
            copy.start()
            pending[c] = copy
            sends.append(copy)
        new = full.at[place(bits, order[:s], mine, (order[s],))]
        copy = remote(me, new, new, csend_sem.at[c, s + 1], crecv_sem.at[c, s + 1], 0)
        copy.start()
        sends.append(copy)
        cores.append(copy)
    for copy in sends:
        copy.wait_send()
    for copy in cores:
        copy.wait_recv()


def gather_all(shards, devices):
    bits = devices.bit_length() - 1
    layers = shards[0].shape[0]
    chunks = list(AG_CHUNKS)
    events = list(AG_EVENTS)
    extra = len(shards) - 1
    for layer in range(layers):
        c = len(chunks)
        chunks.append((layer, extra, (4, 3, 2, 1)))
        for s in range(bits - 1):
            events.insert(3 + layer + 6 * s, (c, s))
    n = len(chunks)
    outs = [
        jax.ShapeDtypeStruct((2,) * bits + s.shape[1:], s.dtype)
        for _ in range(layers)
        for s in shards
    ]
    res = pl.pallas_call(
        functools.partial(gather_kernel, devices, chunks, events, layers, len(shards)),
        out_shape=outs,
        in_specs=[pl.BlockSpec(memory_space=pltpu.VMEM)] * len(shards),
        out_specs=[pl.BlockSpec(memory_space=pl.ANY)] * len(outs),
        scratch_shapes=[pltpu.SemaphoreType.DMA((n, bits - 1))] * 2
        + [pltpu.SemaphoreType.DMA((n, bits))] * 2
        + [pltpu.SemaphoreType.DMA((n,))],
        compiler_params=pltpu.CompilerParams(collective_id=0, has_side_effects=True),
        name="gather_all",
    )(*shards)
    full = [r.reshape((devices * r.shape[-2], r.shape[-1])) for r in res]
    return [full[l * len(shards) : (l + 1) * len(shards)] for l in range(layers)]


PAIRS = ((0, 0), (1, 2), (0, 1), (2, 2), (3, 3), (4, 4))


def scatter_kernel(devices, arrs, nx, ny, *refs):
    bits = devices.bit_length() - 1
    chunks, events = RS_CHUNKS, RS_EVENTS
    half = devices // 2
    na, nc = len(arrs), len(chunks)
    groups, at = [], 0
    for size in (nx, ny, 1, na, 1, nx, ny, nc, nc * (bits - 1), bits - 1, bits):
        groups.append(refs[at : at + size])
        at += size
    xs, ys, small, outs, small_out, xr, yr, sums, parts, small_mid, small_got = groups
    small, small_out = small[0], small_out[0]
    xs_s, xs_r, ys_s, ys_r, st_s, st_r, sm_s, sm_r = refs[at:]
    me = lax.axis_index("dp")
    mine = [(me // (1 << b)) % 2 for b in range(bits)]
    greet(me, bits)
    core = mine[0]
    swaps_x, swaps_y, got_x, got_y = {}, {}, set(), set()
    for a, _, _, _ in chunks:
        xi, yi = PAIRS[a]
        if xi not in swaps_x:
            swaps_x[xi] = remote(
                me, xs[xi].at[:, 1 - core], xr[xi], xs_s.at[xi], xs_r.at[xi], 0
            )
            swaps_x[xi].start()
        if yi not in swaps_y:
            swaps_y[yi] = remote(me, ys[yi], yr[yi], ys_s.at[yi], ys_r.at[yi], 0)
            swaps_y[yi].start()
    sends, pending = [], {}

    def small_send(s):
        src = small if s == 0 else small_mid[s - 1]
        copy = remote(me, src, small_got[s], sm_s.at[s], sm_r.at[s], s)
        copy.start()
        pending["small"] = copy
        sends.append(copy)

    def small_receive(s):
        src = small if s == 0 else small_mid[s - 1]
        pending["small"].wait_recv()
        total = src[...] + small_got[s][...]
        if s + 1 < bits:
            small_mid[s][...] = total
            small_send(s + 1)
        else:
            small_out[...] = total

    def send(c, s):
        order = chunks[c][3]
        index = tuple(
            1 - mine[q] if q == order[s] else mine[q] if q in order[:s] else slice(None)
            for q in reversed(range(1, bits))
        )
        copy = remote(
            me,
            sums[c].at[index],
            parts[c * (bits - 1) + s],
            st_s.at[c, s],
            st_r.at[c, s],
            order[s],
        )
        copy.start()
        pending[c] = copy
        sends.append(copy)

    def compute(c):
        a, first, end, _ = chunks[c]
        xi, yi = PAIRS[a]
        rows = arrs[a][0]
        if xi not in got_x:
            swaps_x[xi].wait_recv()
            got_x.add(xi)
        if yi not in got_y:
            swaps_y[yi].wait_recv()
            got_y.add(yi)

        def tile(start, width, offset):
            left = xs[xi][:, core].reshape(half * rows, -1)
            other = xr[xi][...].reshape(half * rows, -1)
            value = dot(left, ys[yi][:, pl.ds(start, width)])
            value = value + dot(other, yr[yi][:, pl.ds(start, width)])
            sums[c][..., pl.ds(offset, width)] = value.astype(BF16).reshape(
                (2,) * (bits - 1) + (rows, width)
            )

        width, step = end - first, 256
        whole = width // step

        @pl.loop(0, whole)
        def _(i):
            tile(
                pl.multiple_of(first + i * step, 128), step, pl.multiple_of(i * step, 128)
            )

        if width % step:
            tile(first + whole * step, width % step, whole * step)
        send(c, 0)

    def receive(c, s):
        a, first, end, order = chunks[c]
        pending[c].wait_recv()
        fixed = order[: s + 1]
        free = [q for q in reversed(range(1, bits)) if q not in fixed]

        def add(j, last):
            here, there, pos = [], [], len(free)
            for q in reversed(range(1, bits)):
                if q in fixed:
                    here.append(mine[q])
                else:
                    pos -= 1
                    value = (j // (1 << pos)) % 2
                    here.append(value)
                    there.append(value)
            part = parts[c * (bits - 1) + s]
            total = part[tuple(there)].astype(F32) + sums[c][tuple(here)].astype(F32)
            if last:
                outs[a][:, first:end] = total
            else:
                sums[c][tuple(here)] = total.astype(BF16)

        if not free:
            add(0, True)
        else:

            @pl.loop(0, 1 << len(free))
            def _(j):
                add(j, False)

            send(c, s + 1)

    small_send(0)
    taken = 0
    for at, (c, s) in enumerate(events):
        if s < 0:
            compute(c)
        else:
            receive(c, s)
            if taken < bits and at % 4 == 0:
                small_receive(taken)
                taken += 1
    for copy in list(swaps_x.values()) + list(swaps_y.values()) + sends:
        copy.wait_send()


def scatter_layer(turned, grads, small, devices, layer):
    bits = devices.bit_length() - 1
    nx, ny = len(turned), len(grads)
    half = devices // 2
    split = [x.reshape(half, 2, x.shape[0] // devices, x.shape[1]) for x in turned]
    arrs = [(turned[xi].shape[0] // devices, grads[yi].shape[1]) for xi, yi in PAIRS]
    scratch = [pltpu.VMEM((half, x.shape[0] // devices, x.shape[1]), BF16) for x in turned]
    scratch += [pltpu.VMEM(y.shape, BF16) for y in grads]
    for a, first, end, _ in RS_CHUNKS:
        scratch.append(pltpu.VMEM((2,) * (bits - 1) + (arrs[a][0], end - first), BF16))
    for a, first, end, _ in RS_CHUNKS:
        for s in range(bits - 1):
            scratch.append(pltpu.VMEM((2,) * (bits - 2 - s) + (arrs[a][0], end - first), BF16))
    scratch += [pltpu.VMEM(small.shape, F32)] * (2 * bits - 1)
    dma = pltpu.SemaphoreType.DMA
    scratch += [dma((nx,))] * 2 + [dma((ny,))] * 2 + [dma((len(RS_CHUNKS), bits - 1))] * 2
    scratch += [dma((bits,))] * 2
    vmem = pl.BlockSpec(memory_space=pltpu.VMEM)
    outs = [jax.ShapeDtypeStruct(shape, F32) for shape in arrs]
    outs.append(jax.ShapeDtypeStruct(small.shape, F32))
    return pl.pallas_call(
        functools.partial(scatter_kernel, devices, arrs, nx, ny),
        out_shape=outs,
        in_specs=[vmem] * (nx + ny + 1),
        out_specs=[vmem] * len(outs),
        scratch_shapes=scratch,
        compiler_params=pltpu.CompilerParams(
            collective_id=1, has_side_effects=True, vmem_limit_bytes=60 * 1024 * 1024
        ),
        name="scatter_layer",
    )(*split, *grads, small)


def scatter_plain(turned, grads, small):
    owned = [
        lax.psum_scatter(
            dot(turned[xi], grads[yi]).astype(BF16), "dp", scatter_dimension=0, tiled=True
        ).astype(F32)
        for xi, yi in PAIRS
    ]
    return owned + [lax.psum(small, "dp")]


def doc_layout(doc_lengths, rows_count):
    rows_index = jnp.arange(rows_count, dtype=jnp.int32)
    doc_ends = jnp.cumsum(doc_lengths, dtype=jnp.int32)
    later = (rows_index[:, None] >= doc_ends[None, :]).astype(jnp.int32)
    segment = jnp.sum(later, axis=1, dtype=jnp.int32)
    position = rows_index - jnp.sum(later * doc_lengths[None, :], axis=1, dtype=jnp.int32)
    return (segment, position)


def causal_conv(channels, kernel, position):
    summed = channels * kernel[TAPS - 1]
    for offset in range(1, TAPS):
        shifted = jnp.pad(channels, ((offset, 0), (0, 0)))[: channels.shape[0]]
        valid = (position >= offset).astype(channels.dtype)
        summed = summed + shifted * kernel[TAPS - 1 - offset] * valid[:, None]
    return summed


def mixer_core(inner, kernel, head_params, position, inside):
    log_rates, skip_coef, step_bias = head_params
    rows_count = inner.shape[0]
    gate_z = inner[:, :INNER]
    conv_in = inner[:, INNER : INNER + CONVCH]
    step_raw = inner[:, INNER + CONVCH :]
    conv_out = jax.nn.silu(causal_conv(conv_in, kernel, position))
    x_heads = conv_out[:, :INNER].reshape(rows_count, HEADS, HDIM)
    b_all = conv_out[:, INNER : INNER + STATE]
    c_all = conv_out[:, INNER + STATE :]
    dt_all = jax.nn.softplus(step_raw + step_bias[None, :])
    rates = -jnp.exp(log_rates)
    cumul = jnp.dot(inside.astype(F32), dt_all * rates[None, :], precision=HIGHEST).T
    gaps = cumul[:, :, None] - cumul[:, None, :]
    decay = jnp.exp(jnp.where(inside[None], jnp.minimum(gaps, 0.0), -1e30))
    affinity = jnp.dot(c_all, b_all.T, precision=HIGHEST)
    scaled = x_heads * dt_all[:, :, None]
    scanned = jnp.einsum("hij,jhp->ihp", decay * affinity[None], scaled, precision=HIGHEST)
    scanned = scanned + skip_coef[None, :, None] * x_heads
    return scanned.reshape(rows_count, INNER) * jax.nn.silu(gate_z)


def rotate(values, cosine, sine):
    front, rear = values[..., : HD // 2], values[..., HD // 2 :]
    return jnp.concatenate([front * cosine - rear * sine, rear * cosine + front * sine], axis=-1)


def attention_forward(packed, tables, inside):
    rows = packed.shape[0]
    cosine, sine = tables
    heads = packed[:, : (QH + KVH) * HD].reshape(rows, QH + KVH, HD)
    turned = rotate(heads, cosine[:, None], sine[:, None]).astype(BF16)
    query = turned[:, :QH].reshape(rows, KVH, QH // KVH, HD)
    key = turned[:, QH:]
    value = packed[:, (QH + KVH) * HD :].astype(BF16).reshape(rows, KVH, HD)
    scores = jnp.einsum("skgd,tkd->kgst", query, key, preferred_element_type=F32) * SCORE_SCALE
    scores = jnp.where(inside[None, None], scores, -1e30)
    expo = jnp.exp(scores - jnp.max(scores, axis=-1, keepdims=True))
    probs = expo / jnp.sum(expo, axis=-1, keepdims=True)
    low = probs.astype(BF16)
    context = jnp.einsum("kgst,tkd->skgd", low, value, preferred_element_type=F32)
    return context.reshape(rows, QH * HD).astype(BF16), (query, key, value, probs, low)


def attention_backward(dcontext, kept, tables):
    query, key, value, probs, low = kept
    rows = dcontext.shape[0]
    cosine, sine = tables
    grad = dcontext.reshape(rows, KVH, QH // KVH, HD)
    dvalue = jnp.einsum("kgst,skgd->tkd", low, grad, preferred_element_type=F32)
    dprobs = jnp.einsum("skgd,tkd->kgst", grad, value, preferred_element_type=F32)
    dscores = probs * (dprobs - jnp.sum(probs * dprobs, axis=-1, keepdims=True))
    dscores = (dscores * SCORE_SCALE).astype(BF16)
    dquery = jnp.einsum("kgst,tkd->skgd", dscores, key, preferred_element_type=F32)
    dkey = jnp.einsum("kgst,skgd->tkd", dscores, query, preferred_element_type=F32)
    both = jnp.concatenate([dquery.reshape(rows, QH, HD), dkey], axis=1)
    both = rotate(both, cosine[:, None], -sine[:, None]).reshape(rows, (QH + KVH) * HD)
    return jnp.concatenate([both, dvalue.reshape(rows, KVH * HD)], axis=1).astype(BF16)


def inverse_rms(values):
    return lax.rsqrt(jnp.mean(values * values, axis=-1, keepdims=True) + EPSILON)


def norm_backward(grad, values, scale, gain):
    normed = values * scale
    grad_gain = jnp.sum(grad * normed, axis=0)
    inner = grad * gain
    return scale * (inner - normed * jnp.mean(inner * normed, axis=-1, keepdims=True)), grad_gain


def layer_forward(hidden, weights, small, heads, layout):
    w_in, w_mix, w_qkv, w_attn, w_gate_up, w_down = weights
    gains, kernel, gain_inner = small
    position, inside, tables = layout
    scale = inverse_rms(hidden)
    normed = (hidden * scale * gains[0]).astype(BF16)
    inner = dot(normed, w_in)
    packed = dot(normed, w_qkv)
    core = functools.partial(mixer_core, position=position, inside=inside)
    gated, pull_core = jax.vjp(core, inner, kernel, heads)
    scale_inner = inverse_rms(gated)
    mixed = (gated * scale_inner * gain_inner).astype(BF16)
    context, kept_attn = attention_forward(packed, tables, inside)
    middle = hidden + dot(mixed, w_mix) + dot(context, w_attn)
    scale_two = inverse_rms(middle)
    normed_two = (middle * scale_two * gains[1]).astype(BF16)
    both = dot(normed_two, w_gate_up)
    active = (jax.nn.silu(both[:, :FF]) * both[:, FF:]).astype(BF16)
    out = middle + dot(active, w_down)
    kept = (
        hidden,
        scale,
        normed,
        pull_core,
        gated,
        scale_inner,
        mixed,
        context,
        kept_attn,
        middle,
        scale_two,
        normed_two,
        both,
        active,
    )
    return out, kept


def layer_backward(grad, kept, weights, small, layout):
    w_in, w_mix, w_qkv, w_attn, w_gate_up, w_down = weights
    gains, kernel, gain_inner = small
    position, inside, tables = layout
    (
        hidden,
        scale,
        normed,
        pull_core,
        gated,
        scale_inner,
        mixed,
        context,
        kept_attn,
        middle,
        scale_two,
        normed_two,
        both,
        active,
    ) = kept
    ddown = grad.astype(BF16)
    dactive = dot_rt(ddown, w_down)
    gate, up = both[:, :FF], both[:, FF:]
    sig = jax.nn.sigmoid(gate)
    dgate = dactive * up * (sig * (1.0 + gate * (1.0 - sig)))
    dboth = jnp.concatenate([dgate, dactive * (gate * sig)], axis=1).astype(BF16)
    dmiddle, dgain_two = norm_backward(dot_rt(dboth, w_gate_up), middle, scale_two, gains[1])
    dmiddle = grad + dmiddle
    dbranch = dmiddle.astype(BF16)
    dgated, dgain_inner = norm_backward(dot_rt(dbranch, w_mix), gated, scale_inner, gain_inner)
    dcontext = dot_rt(dbranch, w_attn).astype(BF16)
    dpacked = attention_backward(dcontext, kept_attn, tables)
    dinner, dkernel, dheads = pull_core(dgated)
    dinner = dinner.astype(BF16)
    dnormed = dot_rt(dinner, w_in) + dot_rt(dpacked, w_qkv)
    dhidden, dgain = norm_backward(dnormed, hidden, scale, gains[0])
    turned = [x.T for x in (normed, mixed, context, normed_two, active)]
    grads = [dinner, dpacked, dbranch, dboth, ddown]
    flat = [dgain, dgain_two, dkernel.reshape(-1), dgain_inner] + list(dheads)
    return dmiddle + dhidden, turned, grads, jnp.concatenate(flat)


def shards(
    tokens,
    cotangent,
    destination,
    lengths,
    norm_gains,
    in_proj,
    conv_weight,
    ssm_gain,
    mixer_out,
    qkv_proj,
    attn_out,
    gate_up,
    down_proj,
    a_log,
    d_skip,
    dt_bias,
):
    devices = lax.axis_size("dp")
    me = lax.axis_index("dp")
    rows_here, width = tokens.shape
    share = rows_here // devices
    own_kernels = devices == 32
    index = jnp.arange(rows_here, dtype=jnp.int32)
    slabs = destination.reshape(devices, rows_here)

    own = lax.dynamic_slice_in_dim(slabs, me, 1, 0)[0] // rows_here
    same = (own[:, None] == own[None, :]) & (index[None, :] < index[:, None])
    slot = own * share + jnp.sum(same.astype(jnp.int32), axis=1)
    leave = (slot[None, :] == index[:, None]).astype(BF16)
    outgoing = [dot(leave, x).astype(BF16) for x in (tokens, cotangent)]

    def exchange(rows):
        split = rows.reshape(devices, share, width)
        moved = lax.all_to_all(split, "dp", split_axis=0, concat_axis=0, tiled=True)
        return moved.reshape(rows_here, width)

    arrived = [exchange(x) for x in outgoing]

    local = slabs - me * rows_here
    mask = ((local >= 0) & (local < rows_here)).astype(BF16)
    below = (index[:, None] < index[None, :]).astype(BF16)
    rank = dot(mask, below).astype(jnp.int32)
    order = rank + share * jnp.arange(devices, dtype=jnp.int32)[:, None]
    hits = local.reshape(-1)[None, :] == index[:, None]
    taken = jnp.sum(jnp.where(hits, order.reshape(-1)[None, :], 0), axis=1)
    enter = (taken[:, None] == index[None, :]).astype(BF16)
    hidden = dot(enter, arrived[0])
    upstream = dot(enter, arrived[1])

    segment, position = doc_layout(lengths[0], rows_here)
    inside = (segment[:, None] == segment[None, :]) & (index[:, None] >= index[None, :])
    inverse = ROPE_BASE ** (-(jnp.arange(HD // 2, dtype=F32) * 2.0 / HD))
    angles = position.astype(F32)[:, None] * inverse[None, :]
    layout = (position, inside, (jnp.cos(angles), jnp.sin(angles)))

    matrices = (in_proj, mixer_out, qkv_proj, attn_out, gate_up, down_proj)
    gain_part, conv_part, inner_part = (x.shape[-1] for x in (norm_gains, conv_weight, ssm_gain))
    packed = jnp.concatenate(
        [norm_gains.reshape(LAYERS, -1), conv_weight.reshape(LAYERS, -1), ssm_gain], axis=1
    )
    used = packed.shape[1]
    if own_kernels:
        room = SMALL_ROWS * 128
        padded = jnp.pad(packed, ((0, 0), (0, room - used))).reshape(LAYERS, SMALL_ROWS, 128)
        gathered = gather_all(list(matrices) + [padded], devices)
        weights = [g[:-1] for g in gathered]
        smalls = [g[-1].reshape(devices, room)[:, :used] for g in gathered]
    else:
        weights = [
            [lax.all_gather(x[layer], "dp", axis=0, tiled=True) for x in matrices]
            for layer in range(LAYERS)
        ]
        every = lax.all_gather(packed, "dp", axis=0)
        smalls = [every[:, layer] for layer in range(LAYERS)]

    def spread(piece, count):
        shaped = piece.reshape(devices, count, -1)
        return jnp.swapaxes(shaped, 0, 1).reshape(count, -1).astype(F32)

    def small_of(layer):
        both = smalls[layer]
        mid = 2 * gain_part
        return (
            spread(both[:, :mid], 2),
            spread(both[:, mid : mid + TAPS * conv_part], TAPS),
            spread(both[:, mid + TAPS * conv_part :], 1)[0],
        )

    params = [small_of(layer) for layer in range(LAYERS)]
    heads = [(a_log[layer], d_skip[layer], dt_bias[layer]) for layer in range(LAYERS)]

    kept = [None] * LAYERS
    for layer in range(LAYERS):
        hidden, kept[layer] = layer_forward(
            hidden, weights[layer], params[layer], heads[layer], layout
        )
    leaving = lax.dot_general(
        enter, hidden.astype(BF16), (((0,), (0,)), ((), ())), preferred_element_type=F32
    ).astype(BF16)

    def come_home(rows):
        moved = exchange(rows)
        return lax.dot_general(
            leave, moved, (((0,), (0,)), ((), ())), preferred_element_type=F32
        )

    out_tokens = come_home(leaving).astype(BF16)

    flowing = upstream
    owned = [None] * LAYERS
    for layer in reversed(range(LAYERS)):
        flowing, turned, grads, flat = layer_backward(
            flowing, kept[layer], weights[layer], params[layer], layout
        )
        count = flat.shape[0]
        lines = -(-count // 1024) * 8
        small = jnp.pad(flat, (0, lines * 128 - count)).reshape(lines, 128)
        if own_kernels:
            owned[layer] = scatter_layer(turned, grads, small, devices, layer)
        else:
            owned[layer] = scatter_plain(turned, grads, small)
    sending = lax.dot_general(
        enter, flowing.astype(BF16), (((0,), (0,)), ((), ())), preferred_element_type=F32
    ).astype(BF16)
    in_grad = come_home(sending)

    big = [jnp.stack([owned[layer][k] for layer in range(LAYERS)]) for k in range(6)]
    totals = jnp.stack([owned[layer][6].reshape(-1) for layer in range(LAYERS)])
    model = gain_part * devices
    sizes = (2 * model, TAPS * CONVCH, INNER, HEADS, HEADS, HEADS)
    pieces, at = [], 0
    for size in sizes:
        pieces.append(totals[:, at : at + size])
        at += size

    def mine(piece, count, part):
        shaped = piece.reshape(LAYERS, count, devices * part)
        return lax.dynamic_slice_in_dim(shaped, me * part, part, 2)

    return (
        out_tokens,
        in_grad,
        mine(pieces[0], 2, gain_part),
        big[0],
        mine(pieces[1], TAPS, conv_part),
        mine(pieces[2], 1, inner_part)[:, 0],
        big[1],
        big[2],
        big[3],
        big[4],
        big[5],
        pieces[3],
        pieces[4],
        pieces[5],
    )


def solution(mesh):
    placed = (
        P("dp", None),
        P("dp", None),
        P(),
        P("dp", None),
        P(None, None, "dp"),
        P(None, "dp", None),
        P(None, None, "dp"),
        P(None, "dp"),
        P(None, "dp", None),
        P(None, "dp", None),
        P(None, "dp", None),
        P(None, "dp", None),
        P(None, "dp", None),
        P(),
        P(),
        P(),
    )
    return jax.shard_map(
        shards,
        mesh=mesh,
        in_specs=placed,
        out_specs=(
            P("dp", None),
            P("dp", None),
            P(None, None, "dp"),
            P(None, "dp", None),
            P(None, None, "dp"),
            P(None, "dp"),
            P(None, "dp", None),
            P(None, "dp", None),
            P(None, "dp", None),
            P(None, "dp", None),
            P(None, "dp", None),
            P(),
            P(),
            P(),
        ),
        check_vma=False,
    )
```

```python
import functools

import jax
import jax.numpy as jnp
from jax import lax
from jax.experimental import pallas as pl
from jax.experimental.pallas import tpu as pltpu
from jax.sharding import PartitionSpec as P

FF = 2048
HEADS = 24
HDIM = 64
STATE = 128
QH = 8
KVH = 2
HD = 64
LAYERS = 2
INNER = 1536
CONVCH = 1792
TAPS = 4
EPSILON = 1e-05
ROPE_BASE = 100000000000.0
SCORE_SCALE = 0.125
HIGHEST = lax.Precision.HIGHEST
F32 = jnp.float32
BF16 = jnp.bfloat16
MESH = pl.DeviceIdType.MESH

AG_CHUNKS = [(0, 6, (4, 3, 2, 1)), (1, 6, (4, 3, 2, 1)), (0, 1, (4, 3, 2, 1)), (1, 3, (4, 3, 1, 2)), (0, 2, (2, 4, 3, 1)), (1, 2, (4, 3, 1, 2)), (0, 5, (4, 3, 2, 1)), (1, 5, (1, 4, 3, 2)), (0, 3, (1, 2, 4, 3)), (0, 0, (1, 4, 3, 2)), (1, 1, (4, 3, 1, 2)), (1, 4, (1, 2, 4, 3)), (1, 0, (4, 3, 2, 1)), (0, 4, (4, 3, 2, 1))]
AG_EVENTS = [(0, 0), (1, 0), (4, 0), (7, 0), (8, 0), (2, 0), (3, 0), (8, 1), (5, 0), (9, 0), (6, 0), (11, 0), (10, 0), (0, 1), (1, 1), (12, 0), (11, 1), (0, 2), (1, 2), (2, 1), (3, 1), (0, 3), (1, 3), (5, 1), (3, 2), (13, 0), (2, 2), (4, 1), (5, 2), (3, 3), (6, 1), (7, 1), (10, 1), (5, 3), (8, 2), (2, 3), (12, 1), (6, 2), (10, 2), (9, 1), (12, 2), (6, 3), (13, 1), (4, 2), (10, 3), (7, 2), (8, 3), (11, 2), (13, 2), (12, 3), (4, 3), (9, 2), (7, 3), (13, 3), (11, 3), (9, 3)]
RS_CHUNKS = [(3, 512, 1024, (2, 1, 3, 4)), (4, 2048, 4096, (3, 4, 1, 2)), (5, 512, 1024, (2, 3, 4, 1)), (4, 0, 2048, (1, 2, 3, 4)), (1, 512, 1024, (2, 1, 3, 4)), (0, 0, 1792, (1, 2, 3, 4)), (0, 1792, 3352, (1, 2, 3, 4)), (3, 0, 512, (2, 1, 3, 4)), (1, 0, 512, (1, 2, 3, 4)), (5, 0, 512, (2, 3, 4, 1)), (2, 384, 768, (1, 2, 3, 4)), (2, 0, 384, (2, 3, 4, 1))]
RS_EVENTS = [(0, -1), (1, -1), (2, -1), (3, -1), (4, -1), (5, -1), (6, -1), (7, -1), (8, -1), (9, -1), (10, -1), (11, -1), (-1, 0), (0, 0), (-2, 0), (2, 0), (4, 0), (1, 0), (7, 0), (3, 0), (2, 1), (9, 0), (11, 0), (-2, 1), (5, 0), (9, 1), (11, 1), (1, 1), (-2, 2), (2, 2), (3, 1), (9, 2), (6, 0), (11, 2), (5, 1), (3, 2), (8, 0), (-2, 3), (6, 1), (10, 0), (5, 2), (-2, 4), (-1, 1), (0, 1), (8, 1), (3, 3), (10, 1), (4, 1), (-1, 2), (6, 2), (7, 1), (5, 3), (0, 2), (8, 2), (1, 2), (10, 2), (2, 3), (4, 2), (6, 3), (9, 3), (0, 3), (-1, 3), (11, 3), (8, 3), (7, 2), (1, 3), (10, 3), (4, 3), (-1, 4), (7, 3)]

SMALL_ROWS = 16
ROW_BITS = (1, 2, 3, 4, 0)


def dot(left, right):
    return jnp.dot(left, right, preferred_element_type=F32)


def dot_rt(left, right):
    return lax.dot_general(left, right, (((1,), (1,)), ((), ())), preferred_element_type=F32)


def flip(me, bit):
    step = 1 << bit
    return me + step * (1 - 2 * ((me // step) % 2))


def place(bits, free, mine, flipped=()):
    return tuple(
        slice(None) if b in free else 1 - mine[b] if b in flipped else mine[b]
        for b in reversed(range(bits))
    )


def greet(me, bits):
    barrier = pltpu.get_barrier_semaphore()
    for b in range(bits):
        pl.semaphore_signal(barrier, inc=1, device_id=(flip(me, b),), device_id_type=MESH)
    pl.semaphore_wait(barrier, bits)


def remote(me, src, dst, send, recv, bit):
    return pltpu.make_async_remote_copy(
        src_ref=src,
        dst_ref=dst,
        send_sem=send,
        recv_sem=recv,
        device_id=(flip(me, bit),),
        device_id_type=MESH,
    )


def gather_kernel(devices, chunks, events, layers, arrays, *refs):
    bits = devices.bit_length() - 1
    ins = refs[:arrays]
    outs = refs[arrays : arrays + layers * arrays]
    send_sem, recv_sem, csend_sem, crecv_sem, own_sem = refs[arrays + layers * arrays :]
    me = lax.axis_index("dp")
    mine = [(me // (1 << b)) % 2 for b in range(bits)]
    greet(me, bits)
    own, sends, cores, pending = [], [], [], {}
    for c, (l, a, order) in enumerate(chunks):
        here = outs[l * arrays + a].at[place(bits, (), mine)]
        src = ins[a].at[l]
        copy = remote(me, src, here, send_sem.at[c, 0], recv_sem.at[c, 0], order[0])
        copy.start()
        pending[c] = copy
        sends.append(copy)
        local = pltpu.make_async_copy(src, here, own_sem.at[c])
        local.start()
        own.append(local)
    for c, (l, a, order) in enumerate(chunks):
        here = outs[l * arrays + a].at[place(bits, (), mine)]
        copy = remote(me, ins[a].at[l], here, csend_sem.at[c, 0], crecv_sem.at[c, 0], 0)
        copy.start()
        sends.append(copy)
        cores.append(copy)
    for local in own:
        local.wait()
    for c, s in events:
        l, a, order = chunks[c]
        full = outs[l * arrays + a]
        pending[c].wait_recv()
        if s + 1 < bits - 1:
            view = full.at[place(bits, order[: s + 1], mine)]
            copy = remote(
                me, view, view, send_sem.at[c, s + 1], recv_sem.at[c, s + 1], order[s + 1]
            )
            copy.start()
            pending[c] = copy
            sends.append(copy)
        new = full.at[place(bits, order[:s], mine, (order[s],))]
        copy = remote(me, new, new, csend_sem.at[c, s + 1], crecv_sem.at[c, s + 1], 0)
        copy.start()
        sends.append(copy)
        cores.append(copy)
    for copy in sends:
        copy.wait_send()
    for copy in cores:
        copy.wait_recv()


def gather_all(shards, devices):
    bits = devices.bit_length() - 1
    layers = shards[0].shape[0]
    n = len(AG_CHUNKS)
    outs = [
        jax.ShapeDtypeStruct((2,) * bits + s.shape[1:], s.dtype)
        for _ in range(layers)
        for s in shards
    ]
    res = pl.pallas_call(
        functools.partial(gather_kernel, devices, AG_CHUNKS, AG_EVENTS, layers, len(shards)),
        out_shape=outs,
        in_specs=[pl.BlockSpec(memory_space=pltpu.VMEM)] * len(shards),
        out_specs=[pl.BlockSpec(memory_space=pl.ANY)] * len(outs),
        scratch_shapes=[pltpu.SemaphoreType.DMA((n, bits - 1))] * 2
        + [pltpu.SemaphoreType.DMA((n, bits))] * 2
        + [pltpu.SemaphoreType.DMA((n,))],
        compiler_params=pltpu.CompilerParams(collective_id=0, has_side_effects=True),
        name="gather_all",
    )(*shards)
    full = [r.reshape((devices * r.shape[-2], r.shape[-1])) for r in res]
    return [full[l * len(shards) : (l + 1) * len(shards)] for l in range(layers)]


PAIRS = ((0, 0), (1, 2), (0, 1), (2, 2), (3, 3), (4, 4))


def scatter_kernel(devices, arrs, nx, ny, *refs):
    bits = devices.bit_length() - 1
    chunks, events = RS_CHUNKS, RS_EVENTS
    half = devices // 2
    na, nc = len(arrs), len(chunks)
    groups, at = [], 0
    for size in (nx, ny, 2, na, 2, nx, ny, nc, nc * (bits - 1), bits - 1, bits, bits):
        groups.append(refs[at : at + size])
        at += size
    xs, ys, extra, outs, extra_out, xr, yr, sums, parts, small_mid, small_got, rows_got = groups
    small, rows_in = extra
    small_out, rows_out = extra_out
    xs_s, xs_r, ys_s, ys_r, st_s, st_r, sm_s, sm_r, ro_s, ro_r = refs[at:]
    me = lax.axis_index("dp")
    mine = [(me // (1 << b)) % 2 for b in range(bits)]
    greet(me, bits)
    core = mine[0]
    swaps_x, swaps_y, got_x, got_y = {}, {}, set(), set()
    for a, _, _, _ in chunks:
        xi, yi = PAIRS[a]
        if xi not in swaps_x:
            swaps_x[xi] = remote(
                me, xs[xi].at[:, 1 - core], xr[xi], xs_s.at[xi], xs_r.at[xi], 0
            )
            swaps_x[xi].start()
        if yi not in swaps_y:
            swaps_y[yi] = remote(me, ys[yi], yr[yi], ys_s.at[yi], ys_r.at[yi], 0)
            swaps_y[yi].start()
    sends, pending = [], {}

    def small_send(s):
        src = small if s == 0 else small_mid[s - 1]
        copy = remote(me, src, small_got[s], sm_s.at[s], sm_r.at[s], s)
        copy.start()
        pending["small"] = copy
        sends.append(copy)

    def small_receive(s):
        src = small if s == 0 else small_mid[s - 1]
        pending["small"].wait_recv()
        total = src[...] + small_got[s][...]
        if s + 1 < bits:
            small_mid[s][...] = total
            small_send(s + 1)
        else:
            small_out[...] = total

    def rows_index(s, j):
        index, pos = [], bits - 1
        for q in reversed(range(bits)):
            if q == ROW_BITS[s]:
                index.append(1 - mine[q])
            else:
                pos -= 1
                index.append((j // (1 << pos)) % 2)
        return tuple(index)

    def rows_send(s):
        bit = ROW_BITS[s]
        index = tuple(1 - mine[q] if q == bit else slice(None) for q in reversed(range(bits)))
        copy = remote(me, rows_out.at[index], rows_got[s], ro_s.at[s], ro_r.at[s], bit)
        copy.start()
        pending["rows"] = copy

    def rows_receive(s):
        pending["rows"].wait_send()
        pending["rows"].wait_recv()

        @pl.loop(0, 1 << (bits - 1))
        def _(j):
            index = rows_index(s, j)
            there = tuple(index[k] for k in range(bits) if k != bits - 1 - ROW_BITS[s])
            rows_out[index] = rows_got[s][there]

        if s + 1 < bits:
            rows_send(s + 1)

    def send(c, s):
        order = chunks[c][3]
        index = tuple(
            1 - mine[q] if q == order[s] else mine[q] if q in order[:s] else slice(None)
            for q in reversed(range(1, bits))
        )
        copy = remote(
            me,
            sums[c].at[index],
            parts[c * (bits - 1) + s],
            st_s.at[c, s],
            st_r.at[c, s],
            order[s],
        )
        copy.start()
        pending[c] = copy
        sends.append(copy)

    def compute(c):
        a, first, end, _ = chunks[c]
        xi, yi = PAIRS[a]
        rows = arrs[a][0]
        if xi not in got_x:
            swaps_x[xi].wait_recv()
            got_x.add(xi)
        if yi not in got_y:
            swaps_y[yi].wait_recv()
            got_y.add(yi)

        def tile(start, width, offset):
            left = xs[xi][:, core].reshape(half * rows, -1)
            other = xr[xi][...].reshape(half * rows, -1)
            value = dot(left, ys[yi][:, pl.ds(start, width)])
            value = value + dot(other, yr[yi][:, pl.ds(start, width)])
            sums[c][..., pl.ds(offset, width)] = value.astype(BF16).reshape(
                (2,) * (bits - 1) + (rows, width)
            )

        width, step = end - first, 256
        whole = width // step

        @pl.loop(0, whole)
        def _(i):
            tile(
                pl.multiple_of(first + i * step, 128), step, pl.multiple_of(i * step, 128)
            )

        if width % step:
            tile(first + whole * step, width % step, whole * step)
        send(c, 0)

    def receive(c, s):
        a, first, end, order = chunks[c]
        pending[c].wait_recv()
        fixed = order[: s + 1]
        free = [q for q in reversed(range(1, bits)) if q not in fixed]

        def add(j, last):
            here, there, pos = [], [], len(free)
            for q in reversed(range(1, bits)):
                if q in fixed:
                    here.append(mine[q])
                else:
                    pos -= 1
                    value = (j // (1 << pos)) % 2
                    here.append(value)
                    there.append(value)
            part = parts[c * (bits - 1) + s]
            total = part[tuple(there)].astype(F32) + sums[c][tuple(here)].astype(F32)
            if last:
                outs[a][:, first:end] = total
            else:
                sums[c][tuple(here)] = total.astype(BF16)

        if not free:
            add(0, True)
        else:

            @pl.loop(0, 1 << len(free))
            def _(j):
                add(j, False)

            send(c, s + 1)

    small_send(0)
    rows_out[...] = rows_in[...]
    rows_send(0)
    for c, s in events:
        if c == -1:
            small_receive(s)
        elif c == -2:
            rows_receive(s)
        elif s < 0:
            compute(c)
        else:
            receive(c, s)
    for copy in list(swaps_x.values()) + list(swaps_y.values()) + sends:
        copy.wait_send()


def scatter_layer(turned, grads, small, rows, devices):
    bits = devices.bit_length() - 1
    moved = rows.reshape((2,) * bits + (rows.shape[0] // devices, rows.shape[1]))
    nx, ny = len(turned), len(grads)
    half = devices // 2
    split = [x.reshape(half, 2, x.shape[0] // devices, x.shape[1]) for x in turned]
    arrs = [(turned[xi].shape[0] // devices, grads[yi].shape[1]) for xi, yi in PAIRS]
    scratch = [pltpu.VMEM((half, x.shape[0] // devices, x.shape[1]), BF16) for x in turned]
    scratch += [pltpu.VMEM(y.shape, BF16) for y in grads]
    for a, first, end, _ in RS_CHUNKS:
        scratch.append(pltpu.VMEM((2,) * (bits - 1) + (arrs[a][0], end - first), BF16))
    for a, first, end, _ in RS_CHUNKS:
        for s in range(bits - 1):
            scratch.append(pltpu.VMEM((2,) * (bits - 2 - s) + (arrs[a][0], end - first), BF16))
    scratch += [pltpu.VMEM(small.shape, F32)] * (2 * bits - 1)
    scratch += [pltpu.VMEM(moved.shape[1:], BF16)] * bits
    dma = pltpu.SemaphoreType.DMA
    scratch += [dma((nx,))] * 2 + [dma((ny,))] * 2 + [dma((len(RS_CHUNKS), bits - 1))] * 2
    scratch += [dma((bits,))] * 4
    vmem = pl.BlockSpec(memory_space=pltpu.VMEM)
    outs = [jax.ShapeDtypeStruct(shape, F32) for shape in arrs]
    outs.append(jax.ShapeDtypeStruct(small.shape, F32))
    outs.append(jax.ShapeDtypeStruct(moved.shape, BF16))
    *owned, back = pl.pallas_call(
        functools.partial(scatter_kernel, devices, arrs, nx, ny),
        out_shape=outs,
        in_specs=[vmem] * (nx + ny + 2),
        out_specs=[vmem] * len(outs),
        scratch_shapes=scratch,
        compiler_params=pltpu.CompilerParams(
            collective_id=1, has_side_effects=True, vmem_limit_bytes=60 * 1024 * 1024
        ),
        name="scatter_layer",
    )(*split, *grads, small, moved)
    return owned, back.reshape(rows.shape)


def scatter_plain(turned, grads, small):
    owned = [
        lax.psum_scatter(
            dot(turned[xi], grads[yi]).astype(BF16), "dp", scatter_dimension=0, tiled=True
        ).astype(F32)
        for xi, yi in PAIRS
    ]
    return owned + [lax.psum(small, "dp")]


def doc_layout(doc_lengths, rows_count):
    rows_index = jnp.arange(rows_count, dtype=jnp.int32)
    doc_ends = jnp.cumsum(doc_lengths, dtype=jnp.int32)
    later = (rows_index[:, None] >= doc_ends[None, :]).astype(jnp.int32)
    segment = jnp.sum(later, axis=1, dtype=jnp.int32)
    position = rows_index - jnp.sum(later * doc_lengths[None, :], axis=1, dtype=jnp.int32)
    return (segment, position)


PAIRS_OF_HEADS = HEADS // 2
LANES = 128
VMEM = pl.BlockSpec(memory_space=pltpu.VMEM)
BIG = pltpu.CompilerParams(vmem_limit_bytes=56 * 1024 * 1024)


def dot_exact(left, right):
    return jnp.dot(left, right, preferred_element_type=F32, precision=HIGHEST)


def dot_rt_exact(left, right):
    return lax.dot_general(
        left, right, (((1,), (1,)), ((), ())), preferred_element_type=F32, precision=HIGHEST
    )


def sigmoid(x):
    return 1.0 / (1.0 + jnp.exp(-x))


def column_index(shape):
    return lax.broadcasted_iota(jnp.int32, shape, len(shape) - 1)


def shifted_down(values, offset, position):
    return jnp.where(position >= offset, pltpu.roll(values, offset, 0), 0.0)


def conv_before(conv_in, taps, position):
    total = conv_in * taps[TAPS - 1 : TAPS]
    for offset in range(1, TAPS):
        total = total + shifted_down(conv_in, offset, position) * taps[
            TAPS - 1 - offset : TAPS - offset
        ]
    return total


def mixer_setup(inner_ref, taps_ref, heads_ref, position, inside, x_ref, qcol, qrow, dtpair):
    rows = inner_ref.shape[0]

    @pl.loop(0, CONVCH // LANES)
    def _(k):
        at = pl.multiple_of(k * LANES, LANES)
        before = conv_before(
            inner_ref[:, pl.ds(pl.multiple_of(INNER + at, LANES), LANES)],
            taps_ref[:, pl.ds(at, LANES)],
            position,
        )
        x_ref[:, pl.ds(at, LANES)] = before * sigmoid(before)

    raw = inner_ref[:, INNER + CONVCH :] + heads_ref[2:3, :HEADS]
    step = jnp.maximum(raw, 0.0) + jnp.log1p(jnp.exp(-jnp.abs(raw)))
    rates = -jnp.exp(heads_ref[0:1, :HEADS])
    sums = dot_exact(inside, step * rates)
    wide = jnp.concatenate([sums, jnp.zeros((rows, LANES - HEADS), F32)], axis=1)
    qrow[...] = wide.T[: qrow.shape[0]]
    first = column_index((rows, LANES)) < HDIM
    for p in range(PAIRS_OF_HEADS):
        both = []
        for h in (2 * p, 2 * p + 1):
            qcol[h] = jnp.broadcast_to(sums[:, h : h + 1], (rows, LANES))
            both.append(jnp.broadcast_to(step[:, h : h + 1], (rows, LANES)))
        dtpair[p] = jnp.where(first, both[0], both[1])
    return raw, step, rates


def mixer_forward_kernel(
    inner_ref, taps_ref, heads_ref, skip_ref, gain_ref, position_ref, inside_ref,
    mixed_ref, turned_ref, y_ref, x_ref, qcol, qrow, dtpair, aff_ref,
):
    rows = inner_ref.shape[0]
    position = position_ref[...]
    inside = inside_ref[...]
    mixer_setup(inner_ref, taps_ref, heads_ref, position, inside, x_ref, qcol, qrow, dtpair)
    b_all = x_ref[:, INNER : INNER + STATE]
    c_all = x_ref[:, INNER + STATE :]
    aff_ref[...] = dot_rt_exact(c_all, b_all) * inside
    first = column_index((rows, LANES)) < HDIM

    def pair(p, total):
        at = pl.multiple_of(p * LANES, LANES)
        x = x_ref[:, pl.ds(at, LANES)]
        scaled = (x * dtpair[p]).astype(BF16)
        outs = []
        for k in (0, 1):
            h = 2 * p + k
            column = qcol[h]
            gaps = jnp.concatenate([column, column], axis=1) - qrow[pl.ds(h, 1), :]
            prod = jnp.exp(jnp.minimum(gaps, 0.0)) * aff_ref[...]
            outs.append(dot(prod.astype(BF16), scaled))
        y = jnp.where(first, outs[0], outs[1]) + x * skip_ref[:, pl.ds(at, LANES)]
        y_ref[:, pl.ds(at, LANES)] = y
        z = inner_ref[:, pl.ds(at, LANES)]
        w = y * (z * sigmoid(z))
        return total + jnp.sum(w * w, axis=1, keepdims=True)

    total = lax.fori_loop(0, PAIRS_OF_HEADS, pair, jnp.zeros((rows, 1), F32))
    scale = lax.rsqrt(total / INNER + EPSILON)

    @pl.loop(0, PAIRS_OF_HEADS)
    def _(p):
        at = pl.multiple_of(p * LANES, LANES)
        z = inner_ref[:, pl.ds(at, LANES)]
        w = y_ref[:, pl.ds(at, LANES)] * (z * sigmoid(z))
        mixed = w * scale * gain_ref[:, pl.ds(at, LANES)]
        mixed_ref[:, pl.ds(at, LANES)] = mixed.astype(BF16)
        turned_ref[pl.ds(at, LANES), :] = mixed.T.astype(BF16)


def mixer_scratch(rows):
    return [
        pltpu.VMEM((rows, CONVCH), F32),
        pltpu.VMEM((HEADS, rows, LANES), F32),
        pltpu.VMEM((HEADS, rows), F32),
        pltpu.VMEM((PAIRS_OF_HEADS, rows, LANES), F32),
        pltpu.VMEM((rows, rows), F32),
    ]


def mixer_forward(inner, taps, heads, skip, gain, position, inside):
    rows = inner.shape[0]
    shape = jax.ShapeDtypeStruct
    return pl.pallas_call(
        mixer_forward_kernel,
        out_shape=[
            shape((rows, INNER), BF16),
            shape((INNER, rows), BF16),
            shape((rows, INNER), F32),
        ],
        in_specs=[VMEM] * 7,
        out_specs=[VMEM] * 3,
        scratch_shapes=mixer_scratch(rows),
        compiler_params=BIG,
        name="mixer_forward",
    )(inner, taps, heads, skip, gain, position, inside)


def mixer_backward_kernel(
    inner_ref, taps_ref, heads_ref, skip_ref, gain_ref, position_ref, inside_ref, y_ref, dmixed_ref,
    dinner_ref, dtaps_ref, dgain_ref, dskip_ref, dheads_ref,
    x_ref, qcol, qrow, dtpair, aff_ref, dx_ref, daff_ref, rowsum, stepgrad, colsum,
):
    rows = inner_ref.shape[0]
    position = position_ref[...]
    inside = inside_ref[...]
    raw, step, rates = mixer_setup(
        inner_ref, taps_ref, heads_ref, position, inside, x_ref, qcol, qrow, dtpair
    )
    turned_inside = inside.T
    aff_ref[...] = (
        dot_rt_exact(x_ref[:, INNER : INNER + STATE], x_ref[:, INNER + STATE :]) * turned_inside
    )
    daff_ref[...] = jnp.zeros_like(daff_ref)
    stepgrad[...] = jnp.zeros_like(stepgrad)
    colsum[...] = jnp.zeros_like(colsum)
    lane = column_index((rows, LANES))
    first = lane < HDIM

    def sums(p, carry):
        squares, product = carry
        at = pl.multiple_of(p * LANES, LANES)
        z = inner_ref[:, pl.ds(at, LANES)]
        w = y_ref[:, pl.ds(at, LANES)] * (z * sigmoid(z))
        g = dmixed_ref[:, pl.ds(at, LANES)] * gain_ref[:, pl.ds(at, LANES)]
        return (
            squares + jnp.sum(w * w, axis=1, keepdims=True),
            product + jnp.sum(w * g, axis=1, keepdims=True),
        )

    zero = jnp.zeros((rows, 1), F32)
    squares, product = lax.fori_loop(0, PAIRS_OF_HEADS, sums, (zero, zero))
    scale = lax.rsqrt(squares / INNER + EPSILON)
    pull = scale * scale * scale * product / INNER

    @pl.loop(0, PAIRS_OF_HEADS)
    def _(p):
        at = pl.multiple_of(p * LANES, LANES)
        here = pl.ds(at, LANES)
        z = inner_ref[:, here]
        y = y_ref[:, here]
        sig = sigmoid(z)
        silu = z * sig
        w = y * silu
        g = dmixed_ref[:, here]
        dgain_ref[:, here] = jnp.sum(g * w * scale, axis=0, keepdims=True)
        dw = scale * (g * gain_ref[:, here]) - w * pull
        dinner_ref[:, here] = (dw * y * (sig * (1.0 + z * (1.0 - sig)))).astype(BF16)
        dy = dw * silu
        x = x_ref[:, here]
        dskip_ref[:, here] = jnp.sum(dy * x, axis=0, keepdims=True)
        steps = dtpair[p]
        scaled = x * steps
        low = dy.astype(BF16)
        outs = []
        for k in (0, 1):
            h = 2 * p + k
            column = qcol[h]
            gaps = qrow[pl.ds(h, 1), :] - jnp.concatenate([column, column], axis=1)
            decay = jnp.exp(jnp.minimum(gaps, 0.0))
            prod = decay * aff_ref[...]
            own = first if k == 0 else jnp.logical_not(first)
            dprod = dot_rt(jnp.where(own, scaled, 0.0).astype(BF16), low)
            daff_ref[...] += dprod * decay
            both = dprod * prod
            rowsum[pl.ds(h, 1), :] = jnp.sum(both, axis=0, keepdims=True)
            away = jnp.sum(both, axis=1, keepdims=True)
            colsum[...] += jnp.where(lane == h, away, 0.0)
            outs.append(dot(prod.astype(BF16), low))
        dscaled = jnp.where(first, outs[0], outs[1])
        dx_ref[:, here] = dscaled * steps + dy * skip_ref[:, here]
        gain_step = dscaled * x
        left = jnp.sum(jnp.where(first, gain_step, 0.0), axis=1, keepdims=True)
        right = jnp.sum(jnp.where(first, 0.0, gain_step), axis=1, keepdims=True)
        stepgrad[...] += jnp.where(lane == 2 * p, left, 0.0) + jnp.where(
            lane == 2 * p + 1, right, 0.0
        )

    daff = daff_ref[...] * turned_inside
    dx_ref[:, INNER : INNER + STATE] = dot_exact(daff, x_ref[:, INNER + STATE :])
    dx_ref[:, INNER + STATE :] = dot_exact(daff.T, x_ref[:, INNER : INNER + STATE])
    pad = jnp.zeros((LANES - HEADS, rows), F32)
    dsums = jnp.concatenate([rowsum[...], pad], axis=0).T - colsum[...]
    dlog = dot_exact(turned_inside, dsums)[:, :HEADS]
    dstep = stepgrad[:, :HEADS] + dlog * rates
    draw = dstep * sigmoid(raw)
    dinner_ref[:, INNER + CONVCH :] = draw.astype(BF16)
    dheads_ref[0:1, :HEADS] = jnp.sum(dlog * step, axis=0, keepdims=True) * rates
    dheads_ref[1:2, :HEADS] = jnp.sum(draw, axis=0, keepdims=True)

    @pl.loop(0, CONVCH // LANES)
    def _(k):
        here = pl.ds(pl.multiple_of(k * LANES, LANES), LANES)
        there = pl.ds(pl.multiple_of(INNER + k * LANES, LANES), LANES)
        conv_in = inner_ref[:, there]
        taps = taps_ref[:, here]
        before = conv_before(conv_in, taps, position)
        sig = sigmoid(before)
        grad = dx_ref[:, here] * (sig * (1.0 + before * (1.0 - sig)))
        back = grad * taps[TAPS - 1 : TAPS]
        dtaps_ref[TAPS - 1 : TAPS, here] = jnp.sum(grad * conv_in, axis=0, keepdims=True)
        for offset in range(1, TAPS):
            t = TAPS - 1 - offset
            valid = jnp.where(position >= offset, grad, 0.0)
            dtaps_ref[t : t + 1, here] = jnp.sum(
                valid * pltpu.roll(conv_in, offset, 0), axis=0, keepdims=True
            )
            back = back + pltpu.roll(valid, rows - offset, 0) * taps[t : t + 1]
        dinner_ref[:, there] = back.astype(BF16)


def mixer_backward(inner, taps, heads, skip, gain, position, inside, y, dmixed):
    rows = inner.shape[0]
    shape = jax.ShapeDtypeStruct
    return pl.pallas_call(
        mixer_backward_kernel,
        out_shape=[
            shape(inner.shape, BF16),
            shape(taps.shape, F32),
            shape((1, INNER), F32),
            shape((1, INNER), F32),
            shape((8, LANES), F32),
        ],
        in_specs=[VMEM] * 9,
        out_specs=[VMEM] * 5,
        scratch_shapes=mixer_scratch(rows)
        + [
            pltpu.VMEM((rows, CONVCH), F32),
            pltpu.VMEM((rows, rows), F32),
            pltpu.VMEM((HEADS, rows), F32),
            pltpu.VMEM((rows, LANES), F32),
            pltpu.VMEM((rows, LANES), F32),
        ],
        compiler_params=BIG,
        name="mixer_backward",
    )(inner, taps, heads, skip, gain, position, inside, y, dmixed)


def rotate_rows(front, rear, cosine, sine):
    return front * cosine - rear * sine, rear * cosine + front * sine


def attention_setup(packed_ref, cosine_ref, sine_ref, query, key_rows):
    half = HD // 2
    for h in range(QH + KVH):
        at = h * HD
        turned = rotate_rows(
            packed_ref[at : at + half], packed_ref[at + half : at + HD],
            cosine_ref[...], sine_ref[...],
        )
        both = jnp.concatenate(turned, axis=0)
        if h < QH:
            query[at : at + HD] = both.astype(BF16)
        else:
            key_rows[at - QH * HD : at - (QH - 1) * HD] = both


def turned_probs(keys, query, outside):
    scores = dot(keys, query) * SCORE_SCALE + outside
    expo = jnp.exp(scores - jnp.max(scores, axis=0, keepdims=True))
    return expo / jnp.sum(expo, axis=0, keepdims=True)


def attention_forward_kernel(
    packed_ref, cosine_ref, sine_ref, outside_ref, context_ref, turned_ref, query, key_rows
):
    attention_setup(packed_ref, cosine_ref, sine_ref, query, key_rows)
    keys = key_rows[...].T.astype(BF16)
    values = packed_ref[(QH + KVH) * HD :].astype(BF16)
    for h in range(QH):
        kv = h * KVH // QH
        probs = turned_probs(
            keys[:, kv * HD : (kv + 1) * HD], query[h * HD : (h + 1) * HD], outside_ref[...]
        )
        turned = dot(values[kv * HD : (kv + 1) * HD], probs.astype(BF16))
        turned_ref[h * HD : (h + 1) * HD] = turned.astype(BF16)
    for k in range(QH * HD // LANES):
        here = slice(k * LANES, (k + 1) * LANES)
        context_ref[:, here] = turned_ref[here].astype(F32).T.astype(BF16)


def attention_forward(packed, cosine, sine, outside):
    rows = packed.shape[1]
    shape = jax.ShapeDtypeStruct
    return pl.pallas_call(
        attention_forward_kernel,
        out_shape=[shape((rows, QH * HD), BF16), shape((QH * HD, rows), BF16)],
        in_specs=[VMEM] * 4,
        out_specs=[VMEM] * 2,
        scratch_shapes=[pltpu.VMEM((QH * HD, rows), BF16), pltpu.VMEM((KVH * HD, rows), F32)],
        compiler_params=BIG,
        name="attention_forward",
    )(packed, cosine, sine, outside)


def attention_backward_kernel(
    packed_ref, cosine_ref, sine_ref, outside_ref, dcontext_ref, dpacked_ref,
    query, key_rows, grad_rows,
):
    half = HD // 2
    attention_setup(packed_ref, cosine_ref, sine_ref, query, key_rows)
    low_rows = key_rows[...].astype(BF16)
    keys = key_rows[...].T.astype(BF16)
    values = packed_ref[(QH + KVH) * HD :].T.astype(BF16)
    for k in range(QH * HD // LANES):
        here = slice(k * LANES, (k + 1) * LANES)
        grad_rows[here] = dcontext_ref[:, here].T
    for kv in range(KVH):
        of_kv = slice(kv * HD, (kv + 1) * HD)
        dkey = jnp.zeros((HD, keys.shape[0]), F32)
        dvalue = jnp.zeros((HD, keys.shape[0]), F32)
        for h in range(kv * QH // KVH, (kv + 1) * QH // KVH):
            here = slice(h * HD, (h + 1) * HD)
            probs = turned_probs(keys[:, of_kv], query[here], outside_ref[...])
            grad = grad_rows[here].astype(BF16)
            dprobs = dot(values[:, of_kv], grad)
            dvalue = dvalue + dot_rt(grad, probs.astype(BF16))
            inner = jnp.sum(probs * dprobs, axis=0, keepdims=True)
            dscores = (probs * (dprobs - inner) * SCORE_SCALE).astype(BF16)
            dquery = dot(low_rows[of_kv], dscores)
            dkey = dkey + dot_rt(query[here], dscores)
            turned = rotate_rows(dquery[:half], dquery[half:], cosine_ref[...], -sine_ref[...])
            grad_rows[here] = jnp.concatenate(turned, axis=0)
        turned = rotate_rows(dkey[:half], dkey[half:], cosine_ref[...], -sine_ref[...])
        at = QH * HD + kv * HD
        grad_rows[at : at + HD] = jnp.concatenate(turned, axis=0)
        at = (QH + KVH) * HD + kv * HD
        grad_rows[at : at + HD] = dvalue
    for k in range((QH + 2 * KVH) * HD // LANES):
        here = slice(k * LANES, (k + 1) * LANES)
        dpacked_ref[:, here] = grad_rows[here].T.astype(BF16)


def attention_backward(packed, cosine, sine, outside, dcontext):
    width, rows = packed.shape
    return pl.pallas_call(
        attention_backward_kernel,
        out_shape=jax.ShapeDtypeStruct((rows, width), BF16),
        in_specs=[VMEM] * 5,
        out_specs=VMEM,
        scratch_shapes=[
            pltpu.VMEM((QH * HD, rows), BF16),
            pltpu.VMEM((KVH * HD, rows), F32),
            pltpu.VMEM((width, rows), F32),
        ],
        compiler_params=BIG,
        name="attention_backward",
    )(packed, cosine, sine, outside, dcontext)


def inverse_rms(values):
    return lax.rsqrt(jnp.mean(values * values, axis=-1, keepdims=True) + EPSILON)


def norm_backward(grad, values, scale, gain):
    normed = values * scale
    grad_gain = jnp.sum(grad * normed, axis=0)
    inner = grad * gain
    return scale * (inner - normed * jnp.mean(inner * normed, axis=-1, keepdims=True)), grad_gain


def layer_forward(hidden, weights, small, layout):
    w_in, w_mix, w_qkv, w_attn, w_gate_up, w_down = weights
    gains, taps, gain_inner, heads, skip = small
    position, inside, outside, cosine, sine = layout
    scale = inverse_rms(hidden)
    normed = (hidden * scale * gains[0]).astype(BF16)
    inner = dot(normed, w_in)
    packed = lax.dot_general(
        w_qkv, normed, (((0,), (1,)), ((), ())), preferred_element_type=F32
    )
    mixed, mixed_rows, y = mixer_forward(inner, taps, heads, skip, gain_inner, position, inside)
    context, context_rows = attention_forward(packed, cosine, sine, outside)
    middle = hidden + dot(mixed, w_mix) + dot(context, w_attn)
    scale_two = inverse_rms(middle)
    normed_two = (middle * scale_two * gains[1]).astype(BF16)
    both = dot(normed_two, w_gate_up)
    active = (jax.nn.silu(both[:, :FF]) * both[:, FF:]).astype(BF16)
    out = middle + dot(active, w_down)
    turned = [normed.T, mixed_rows, context_rows, normed_two.T, active.T]
    return out, (hidden, scale, inner, packed, y, middle, scale_two, both, turned)


def layer_backward(grad, kept, weights, small, layout):
    w_in, w_mix, w_qkv, w_attn, w_gate_up, w_down = weights
    gains, taps, gain_inner, heads, skip = small
    position, inside, outside, cosine, sine = layout
    hidden, scale, inner, packed, y, middle, scale_two, both, turned = kept
    ddown = grad.astype(BF16)
    dactive = dot_rt(ddown, w_down)
    gate, up = both[:, :FF], both[:, FF:]
    sig = jax.nn.sigmoid(gate)
    dgate = dactive * up * (sig * (1.0 + gate * (1.0 - sig)))
    dboth = jnp.concatenate([dgate, dactive * (gate * sig)], axis=1).astype(BF16)
    dmiddle, dgain_two = norm_backward(dot_rt(dboth, w_gate_up), middle, scale_two, gains[1])
    dmiddle = grad + dmiddle
    dbranch = dmiddle.astype(BF16)
    dmixed = dot_rt(dbranch, w_mix)
    dcontext = dot_rt(dbranch, w_attn).astype(BF16).astype(F32)
    dpacked = attention_backward(packed, cosine, sine, outside, dcontext)
    dinner, dtaps, dgain_inner, dskip, dheads = mixer_backward(
        inner, taps, heads, skip, gain_inner, position, inside, y, dmixed
    )
    dnormed = dot_rt(dinner, w_in) + dot_rt(dpacked, w_qkv)
    dhidden, dgain = norm_backward(dnormed, hidden, scale, gains[0])
    grads = [dinner, dpacked, dbranch, dboth, ddown]
    flat = [dgain, dgain_two, dtaps.reshape(-1), dgain_inner[0], dheads[0, :HEADS]]
    flat += [jnp.sum(dskip.reshape(HEADS, HDIM), axis=1), dheads[1, :HEADS]]
    return dmiddle + dhidden, turned, grads, jnp.concatenate(flat)


def shards(
    tokens,
    cotangent,
    destination,
    lengths,
    norm_gains,
    in_proj,
    conv_weight,
    ssm_gain,
    mixer_out,
    qkv_proj,
    attn_out,
    gate_up,
    down_proj,
    a_log,
    d_skip,
    dt_bias,
):
    devices = lax.axis_size("dp")
    me = lax.axis_index("dp")
    rows_here, width = tokens.shape
    share = rows_here // devices
    own_kernels = devices == 32
    index = jnp.arange(rows_here, dtype=jnp.int32)
    slabs = destination.reshape(devices, rows_here)

    own = lax.dynamic_slice_in_dim(slabs, me, 1, 0)[0] // rows_here
    same = (own[:, None] == own[None, :]) & (index[None, :] < index[:, None])
    slot = own * share + jnp.sum(same.astype(jnp.int32), axis=1)
    leave = (slot[None, :] == index[:, None]).astype(BF16)
    outgoing = [dot(leave, x).astype(BF16) for x in (tokens, cotangent)]

    def exchange(rows):
        split = rows.reshape(devices, share, width)
        moved = lax.all_to_all(split, "dp", split_axis=0, concat_axis=0, tiled=True)
        return moved.reshape(rows_here, width)

    arrived = [exchange(x) for x in outgoing]

    local = slabs - me * rows_here
    mask = ((local >= 0) & (local < rows_here)).astype(BF16)
    below = (index[:, None] < index[None, :]).astype(BF16)
    rank = dot(mask, below).astype(jnp.int32)
    order = rank + share * jnp.arange(devices, dtype=jnp.int32)[:, None]
    hits = local.reshape(-1)[None, :] == index[:, None]
    taken = jnp.sum(jnp.where(hits, order.reshape(-1)[None, :], 0), axis=1)
    enter = (taken[:, None] == index[None, :]).astype(BF16)
    hidden = dot(enter, arrived[0])
    upstream = dot(enter, arrived[1])

    segment, position = doc_layout(lengths[0], rows_here)
    inside = (segment[:, None] == segment[None, :]) & (index[:, None] >= index[None, :])
    inverse = ROPE_BASE ** (-(jnp.arange(HD // 2, dtype=F32) * 2.0 / HD))
    angles = position.astype(F32)[:, None] * inverse[None, :]
    outside = jnp.where(inside.T, 0.0, -1e30)
    layout = (position[:, None], inside.astype(F32), outside, jnp.cos(angles).T, jnp.sin(angles).T)

    matrices = (in_proj, mixer_out, qkv_proj, attn_out, gate_up, down_proj)
    gain_part, conv_part, inner_part = (x.shape[-1] for x in (norm_gains, conv_weight, ssm_gain))
    packed = jnp.concatenate(
        [norm_gains.reshape(LAYERS, -1), conv_weight.reshape(LAYERS, -1), ssm_gain], axis=1
    )
    used = packed.shape[1]
    if own_kernels:
        room = SMALL_ROWS * 128
        padded = jnp.pad(packed, ((0, 0), (0, room - used))).reshape(LAYERS, SMALL_ROWS, 128)
        gathered = gather_all(list(matrices) + [padded], devices)
        weights = [g[:-1] for g in gathered]
        smalls = [g[-1].reshape(devices, room)[:, :used] for g in gathered]
    else:
        weights = [
            [lax.all_gather(x[layer], "dp", axis=0, tiled=True) for x in matrices]
            for layer in range(LAYERS)
        ]
        every = lax.all_gather(packed, "dp", axis=0)
        smalls = [every[:, layer] for layer in range(LAYERS)]

    def spread(piece, count):
        shaped = piece.reshape(devices, count, -1)
        return jnp.swapaxes(shaped, 0, 1).reshape(count, -1).astype(F32)

    def small_of(layer):
        both = smalls[layer]
        mid = 2 * gain_part
        heads = jnp.stack([a_log[layer], d_skip[layer], dt_bias[layer]])
        return (
            spread(both[:, :mid], 2),
            spread(both[:, mid : mid + TAPS * conv_part], TAPS),
            spread(both[:, mid + TAPS * conv_part :], 1),
            jnp.pad(heads, ((0, 5), (0, LANES - HEADS))),
            jnp.repeat(d_skip[layer], HDIM)[None],
        )

    params = [small_of(layer) for layer in range(LAYERS)]

    kept = [None] * LAYERS
    for layer in range(LAYERS):
        hidden, kept[layer] = layer_forward(hidden, weights[layer], params[layer], layout)

    def permute_back(choice, rows):
        return lax.dot_general(
            choice, rows.astype(BF16), (((0,), (0,)), ((), ())), preferred_element_type=F32
        )

    flowing = upstream
    owned = [None] * LAYERS
    back = [None] * LAYERS
    for layer in reversed(range(LAYERS)):
        flowing, turned, grads, flat = layer_backward(
            flowing, kept[layer], weights[layer], params[layer], layout
        )
        count = flat.shape[0]
        lines = -(-count // 1024) * 8
        small = jnp.pad(flat, (0, lines * 128 - count)).reshape(lines, 128)
        home = flowing if layer == 0 else hidden
        home = permute_back(enter, home).astype(BF16)
        if own_kernels:
            owned[layer], back[layer] = scatter_layer(turned, grads, small, home, devices)
        else:
            owned[layer], back[layer] = scatter_plain(turned, grads, small), exchange(home)
    out_tokens = permute_back(leave, back[LAYERS - 1]).astype(BF16)
    in_grad = permute_back(leave, back[0])

    big = [jnp.stack([owned[layer][k] for layer in range(LAYERS)]) for k in range(6)]
    totals = jnp.stack([owned[layer][6].reshape(-1) for layer in range(LAYERS)])
    model = gain_part * devices
    sizes = (2 * model, TAPS * CONVCH, INNER, HEADS, HEADS, HEADS)
    pieces, at = [], 0
    for size in sizes:
        pieces.append(totals[:, at : at + size])
        at += size

    def mine(piece, count, part):
        shaped = piece.reshape(LAYERS, count, devices * part)
        return lax.dynamic_slice_in_dim(shaped, me * part, part, 2)

    return (
        out_tokens,
        in_grad,
        mine(pieces[0], 2, gain_part),
        big[0],
        mine(pieces[1], TAPS, conv_part),
        mine(pieces[2], 1, inner_part)[:, 0],
        big[1],
        big[2],
        big[3],
        big[4],
        big[5],
        pieces[3],
        pieces[4],
        pieces[5],
    )


def solution(mesh):
    placed = (
        P("dp", None),
        P("dp", None),
        P(),
        P("dp", None),
        P(None, None, "dp"),
        P(None, "dp", None),
        P(None, None, "dp"),
        P(None, "dp"),
        P(None, "dp", None),
        P(None, "dp", None),
        P(None, "dp", None),
        P(None, "dp", None),
        P(None, "dp", None),
        P(),
        P(),
        P(),
    )
    return jax.shard_map(
        shards,
        mesh=mesh,
        in_specs=placed,
        out_specs=(
            P("dp", None),
            P("dp", None),
            P(None, None, "dp"),
            P(None, "dp", None),
            P(None, None, "dp"),
            P(None, "dp"),
            P(None, "dp", None),
            P(None, "dp", None),
            P(None, "dp", None),
            P(None, "dp", None),
            P(None, "dp", None),
            P(),
            P(),
            P(),
        ),
        check_vma=False,
    )
```

```python
import functools

import jax
import jax.numpy as jnp
from jax import lax
from jax.experimental import pallas as pl
from jax.experimental.pallas import tpu as pltpu
from jax.sharding import PartitionSpec as P

FF = 2048
HEADS = 24
HDIM = 64
STATE = 128
QH = 8
KVH = 2
HD = 64
LAYERS = 2
INNER = 1536
CONVCH = 1792
TAPS = 4
EPSILON = 1e-05
ROPE_BASE = 100000000000.0
SCORE_SCALE = 0.125
HIGHEST = lax.Precision.HIGHEST
F32 = jnp.float32
BF16 = jnp.bfloat16
MESH = pl.DeviceIdType.MESH

AG_CHUNKS = [(0, 6, (4, 3, 2, 1)), (1, 6, (4, 3, 2, 1)), (1, 0, (4, 3, 1, 2)), (1, 3, (4, 3, 2, 1)), (1, 2, (4, 3, 2, 1)), (0, 2, (4, 3, 2, 1)), (1, 5, (4, 3, 2, 1)), (0, 0, (4, 3, 1, 2)), (0, 3, (1, 4, 3, 2)), (0, 5, (4, 3, 2, 1)), (0, 4, (1, 2, 4, 3)), (0, 1, (1, 2, 4, 3)), (1, 1, (4, 3, 2, 1))]
AG_EVENTS = [(0, 0), (1, 0), (8, 0), (10, 0), (11, 0), (2, 0), (3, 0), (4, 0), (5, 0), (0, 1), (1, 1), (6, 0), (10, 1), (11, 1), (0, 2), (1, 2), (0, 3), (1, 3), (7, 0), (2, 1), (3, 1), (4, 1), (9, 0), (5, 1), (3, 2), (12, 0), (6, 1), (4, 2), (8, 1), (5, 2), (2, 2), (6, 2), (3, 3), (4, 3), (5, 3), (7, 1), (9, 1), (10, 2), (12, 1), (2, 3), (8, 2), (6, 3), (11, 2), (9, 2), (12, 2), (7, 2), (8, 3), (9, 3), (10, 3), (12, 3), (7, 3), (11, 3)]
PLAN_A = ([(1, 0, 256, (2, 1, 3, 4)), (1, 768, 1024, (3, 4, 1, 2)), (0, 0, 1024, (1, 2, 3, 4)), (0, 2048, 3072, (2, 3, 4, 1)), (0, 3072, 4096, (3, 4, 1, 2)), (0, 1024, 2048, (1, 2, 3, 4)), (1, 256, 512, (1, 2, 3, 4)), (1, 512, 768, (2, 1, 3, 4))], [(0, -1), (1, -1), (2, -1), (3, -1), (4, -1), (5, -1), (6, -1), (7, -1), (-3, 0), (0, 0), (1, 0), (-3, 0), (-3, 0), (-3, 0), (-3, 0), (-3, 0), (-3, 0), (-3, 0), (2, 0), (-3, 0), (1, 1), (3, 0), (4, 0), (-3, 0), (-3, 0), (7, 0), (-3, 0), (5, 0), (3, 1), (-3, 0), (2, 1), (-3, 0), (6, 0), (-3, 0), (-3, 0), (0, 1), (4, 1), (-3, 0), (5, 1), (1, 2), (-3, 0), (-3, 0), (7, 1), (6, 1), (2, 2), (-3, 0), (0, 2), (3, 2), (-3, 0), (1, 3), (-3, 0), (4, 2), (-3, 0), (-3, 0), (5, 2), (-3, 0), (-3, 0), (7, 2), (-3, 0), (-3, 0), (3, 3), (-3, 0), (6, 2), (2, 3), (-3, 0), (4, 3), (0, 3), (5, 3), (7, 3), (6, 3)], (1, 2, 3, 4, 0))
PLAN_B = ([(1, 512, 1024, (1, 2, 3, 4)), (4, 2688, 4096, (2, 1, 3, 4)), (0, 0, 1664, (3, 4, 2, 1)), (2, 0, 768, (3, 4, 2, 1)), (3, 0, 1024, (2, 1, 3, 4)), (4, 1408, 2688, (1, 3, 4, 2)), (0, 1664, 3352, (2, 1, 3, 4)), (4, 0, 1408, (1, 2, 3, 4)), (5, 512, 1024, (1, 3, 4, 2)), (5, 0, 512, (2, 1, 3, 4)), (1, 0, 512, (2, 1, 3, 4))], [(0, -1), (1, -1), (2, -1), (3, -1), (4, -1), (5, -1), (6, -1), (7, -1), (8, -1), (9, -1), (10, -1), (-1, 0), (0, 0), (-2, 0), (-3, 0), (-2, 1), (-3, 0), (-3, 0), (-3, 0), (-3, 0), (1, 0), (-3, 0), (-3, 0), (-3, 0), (-3, 0), (5, 0), (4, 0), (2, 0), (-3, 0), (-3, 0), (-3, 0), (3, 0), (-3, 0), (-3, 0), (-3, 0), (-3, 0), (7, 0), (5, 1), (-3, 0), (-3, 0), (-3, 0), (6, 0), (-3, 0), (-3, 0), (-3, 0), (-3, 0), (-3, 0), (-3, 0), (-3, 0), (-3, 0), (-3, 0), (2, 1), (-3, 0), (-3, 0), (8, 0), (-1, 1), (9, 0), (3, 1), (1, 1), (4, 1), (8, 1), (10, 0), (5, 2), (0, 1), (1, 2), (4, 2), (6, 1), (-2, 2), (8, 2), (0, 2), (1, 3), (9, 1), (4, 3), (0, 3), (7, 1), (6, 2), (10, 1), (9, 2), (2, 2), (-1, 2), (-2, 3), (3, 2), (7, 2), (6, 3), (5, 3), (2, 3), (8, 3), (3, 3), (9, 3), (10, 2), (-1, 3), (7, 3), (10, 3), (-2, 4), (-1, 4)], (4, 0, 2, 1, 3))
PLAN_C = ([(3, 512, 1024, (2, 1, 3, 4)), (1, 0, 512, (1, 2, 3, 4)), (0, 2560, 3352, (3, 4, 1, 2)), (2, 384, 768, (2, 3, 4, 1)), (0, 0, 896, (2, 1, 3, 4)), (0, 896, 1664, (3, 4, 2, 1)), (0, 1664, 2560, (2, 1, 3, 4)), (1, 512, 1024, (1, 2, 3, 4)), (2, 0, 384, (1, 2, 3, 4)), (3, 0, 512, (1, 2, 3, 4))], [(0, -1), (1, -1), (2, -1), (3, -1), (4, -1), (5, -1), (6, -1), (7, -1), (8, -1), (9, -1), (-1, 0), (0, 0), (3, 0), (1, 0), (-2, 0), (-2, 1), (2, 0), (4, 0), (7, 0), (5, 0), (8, 0), (3, 1), (9, 0), (-1, 1), (6, 0), (2, 1), (0, 1), (1, 1), (4, 1), (0, 2), (5, 1), (1, 2), (-2, 2), (6, 1), (3, 2), (4, 2), (0, 3), (2, 2), (7, 1), (1, 3), (8, 1), (6, 2), (9, 1), (-1, 2), (4, 3), (-2, 3), (3, 3), (7, 2), (5, 2), (8, 2), (2, 3), (9, 2), (6, 3), (-1, 3), (5, 3), (7, 3), (8, 3), (9, 3), (-2, 4), (-1, 4)], (4, 0, 2, 1, 3))

SMALL_ROWS = 16
LATE_ARRAY = 4


def dot(left, right):
    return jnp.dot(left, right, preferred_element_type=F32)


def dot_rt(left, right):
    return lax.dot_general(left, right, (((1,), (1,)), ((), ())), preferred_element_type=F32)


PAIRS_OF_HEADS = HEADS // 2
LANES = 128
VMEM = pl.BlockSpec(memory_space=pltpu.VMEM)
BIG = pltpu.CompilerParams(vmem_limit_bytes=56 * 1024 * 1024)


def dot_exact(left, right):
    return jnp.dot(left, right, preferred_element_type=F32, precision=HIGHEST)


def dot_rt_exact(left, right):
    return lax.dot_general(
        left, right, (((1,), (1,)), ((), ())), preferred_element_type=F32, precision=HIGHEST
    )


def sigmoid(x):
    return 1.0 / (1.0 + jnp.exp(-x))


def column_index(shape):
    return lax.broadcasted_iota(jnp.int32, shape, len(shape) - 1)


def shifted_down(values, offset, position):
    return jnp.where(position >= offset, pltpu.roll(values, offset, 0), 0.0)


def conv_before(conv_in, taps, position):
    total = conv_in * taps[TAPS - 1 : TAPS]
    for offset in range(1, TAPS):
        total = total + shifted_down(conv_in, offset, position) * taps[
            TAPS - 1 - offset : TAPS - offset
        ]
    return total


def spans(count, parts):
    edges = [count * k // parts for k in range(parts + 1)]
    return list(zip(edges[:-1], edges[1:]))


def run_steps(steps):
    for _ in steps:
        pass


def step_sizes(inner_ref, heads_ref):
    raw = inner_ref[:, INNER + CONVCH :] + heads_ref[2:3, :HEADS]
    step = jnp.maximum(raw, 0.0) + jnp.log1p(jnp.exp(-jnp.abs(raw)))
    return raw, step, -jnp.exp(heads_ref[0:1, :HEADS])


def mixer_setup(inner_ref, taps_ref, heads_ref, position, inside, x_ref, qcol, qrow, dtpair):
    rows = inner_ref.shape[0]
    for start, end in spans(CONVCH // LANES, 2):

        @pl.loop(start, end)
        def _(k):
            at = pl.multiple_of(k * LANES, LANES)
            before = conv_before(
                inner_ref[:, pl.ds(pl.multiple_of(INNER + at, LANES), LANES)],
                taps_ref[:, pl.ds(at, LANES)],
                position,
            )
            x_ref[:, pl.ds(at, LANES)] = before * sigmoid(before)

        yield

    raw, step, rates = step_sizes(inner_ref, heads_ref)
    sums = dot_exact(inside, step * rates)
    wide = jnp.concatenate([sums, jnp.zeros((rows, LANES - HEADS), F32)], axis=1)
    qrow[...] = wide.T[: qrow.shape[0]]
    first = column_index((rows, LANES)) < HDIM
    yield
    for p in range(PAIRS_OF_HEADS):
        for source, target in ((sums, qcol), (step, dtpair)):
            both = [
                jnp.broadcast_to(source[:, h : h + 1], (rows, LANES)) for h in (2 * p, 2 * p + 1)
            ]
            target[p] = jnp.where(first, both[0], both[1])
        if p % 4 == 3:
            yield


def mixer_forward_kernel(
    inner_ref, taps_ref, heads_ref, skip_ref, gain_ref, position_ref, inside_ref,
    mixed_ref, turned_ref, y_ref, x_ref, qcol, qrow, dtpair, aff_ref,
):
    rows = inner_ref.shape[0]
    position = position_ref[...]
    inside = inside_ref[...]
    run_steps(
        mixer_setup(inner_ref, taps_ref, heads_ref, position, inside, x_ref, qcol, qrow, dtpair)
    )
    b_all = x_ref[:, INNER : INNER + STATE]
    c_all = x_ref[:, INNER + STATE :]
    aff_ref[...] = dot_rt_exact(c_all, b_all) * inside
    first = column_index((rows, LANES)) < HDIM

    def pair(p, total):
        at = pl.multiple_of(p * LANES, LANES)
        x = x_ref[:, pl.ds(at, LANES)]
        scaled = (x * dtpair[p]).astype(BF16)
        outs = []
        columns = qcol[p]
        for k in (0, 1):
            h = 2 * p + k
            gaps = columns[:, k * HDIM : k * HDIM + 1] - qrow[pl.ds(h, 1), :]
            prod = jnp.exp(jnp.minimum(gaps, 0.0)) * aff_ref[...]
            outs.append(dot(prod.astype(BF16), scaled))
        y = jnp.where(first, outs[0], outs[1]) + x * skip_ref[:, pl.ds(at, LANES)]
        y_ref[:, pl.ds(at, LANES)] = y
        z = inner_ref[:, pl.ds(at, LANES)]
        w = y * (z * sigmoid(z))
        return total + jnp.sum(w * w, axis=1, keepdims=True)

    total = lax.fori_loop(0, PAIRS_OF_HEADS, pair, jnp.zeros((rows, 1), F32))
    scale = lax.rsqrt(total / INNER + EPSILON)

    @pl.loop(0, PAIRS_OF_HEADS)
    def _(p):
        at = pl.multiple_of(p * LANES, LANES)
        z = inner_ref[:, pl.ds(at, LANES)]
        w = y_ref[:, pl.ds(at, LANES)] * (z * sigmoid(z))
        mixed = w * scale * gain_ref[:, pl.ds(at, LANES)]
        mixed_ref[:, pl.ds(at, LANES)] = mixed.astype(BF16)
        turned_ref[pl.ds(at, LANES), :] = mixed.T.astype(BF16)


def mixer_scratch(rows):
    return [
        pltpu.VMEM((rows, CONVCH), F32),
        pltpu.VMEM((PAIRS_OF_HEADS, rows, LANES), F32),
        pltpu.VMEM((HEADS, rows), F32),
        pltpu.VMEM((PAIRS_OF_HEADS, rows, LANES), F32),
        pltpu.VMEM((rows, rows), F32),
    ]


def mixer_forward(inner, taps, heads, skip, gain, position, inside):
    rows = inner.shape[0]
    shape = jax.ShapeDtypeStruct
    return pl.pallas_call(
        mixer_forward_kernel,
        out_shape=[
            shape((rows, INNER), BF16),
            shape((INNER, rows), BF16),
            shape((rows, INNER), F32),
        ],
        in_specs=[VMEM] * 7,
        out_specs=[VMEM] * 3,
        scratch_shapes=mixer_scratch(rows),
        compiler_params=BIG,
        name="mixer_forward",
    )(inner, taps, heads, skip, gain, position, inside)


def mixer_backward_steps(
    inner_ref, taps_ref, heads_ref, skip_ref, gain_ref, position_ref, inside_ref, y_ref, dmixed_ref,
    dinner_ref, dtaps_ref, dgain_ref, dskip_ref, dheads_ref,
    x_ref, qcol, qrow, dtpair, aff_ref, dx_ref, daff_ref, rowsum, stepgrad, colsum,
):
    rows = inner_ref.shape[0]
    position = position_ref[...]
    yield from mixer_setup(
        inner_ref, taps_ref, heads_ref, position, inside_ref[...], x_ref, qcol, qrow, dtpair
    )
    aff_ref[...] = (
        dot_rt_exact(x_ref[:, INNER : INNER + STATE], x_ref[:, INNER + STATE :]) * inside_ref[...].T
    )
    daff_ref[...] = jnp.zeros_like(daff_ref)
    stepgrad[...] = jnp.zeros_like(stepgrad)
    colsum[...] = jnp.zeros_like(colsum)
    lane = column_index((rows, LANES))
    first = lane < HDIM
    yield

    def sums(p, carry):
        squares, product = carry
        at = pl.multiple_of(p * LANES, LANES)
        z = inner_ref[:, pl.ds(at, LANES)]
        w = y_ref[:, pl.ds(at, LANES)] * (z * sigmoid(z))
        g = dmixed_ref[:, pl.ds(at, LANES)] * gain_ref[:, pl.ds(at, LANES)]
        return (
            squares + jnp.sum(w * w, axis=1, keepdims=True),
            product + jnp.sum(w * g, axis=1, keepdims=True),
        )

    zero = jnp.zeros((rows, 1), F32)
    squares, product = lax.fori_loop(0, PAIRS_OF_HEADS, sums, (zero, zero))
    scale = lax.rsqrt(squares / INNER + EPSILON)
    pull = scale * scale * scale * product / INNER
    yield

    def pair(p):
        at = pl.multiple_of(p * LANES, LANES)
        here = pl.ds(at, LANES)
        z = inner_ref[:, here]
        y = y_ref[:, here]
        sig = sigmoid(z)
        silu = z * sig
        w = y * silu
        g = dmixed_ref[:, here]
        dgain_ref[:, here] = jnp.sum(g * w * scale, axis=0, keepdims=True)
        dw = scale * (g * gain_ref[:, here]) - w * pull
        dinner_ref[:, here] = (dw * y * (sig * (1.0 + z * (1.0 - sig)))).astype(BF16)
        dy = dw * silu
        x = x_ref[:, here]
        dskip_ref[:, here] = jnp.sum(dy * x, axis=0, keepdims=True)
        steps = dtpair[p]
        scaled = x * steps
        low = dy.astype(BF16)
        outs = []
        columns = qcol[p]
        for k in (0, 1):
            h = 2 * p + k
            gaps = qrow[pl.ds(h, 1), :] - columns[:, k * HDIM : k * HDIM + 1]
            decay = jnp.exp(jnp.minimum(gaps, 0.0))
            prod = decay * aff_ref[...]
            own = first if k == 0 else jnp.logical_not(first)
            dprod = dot_rt(jnp.where(own, scaled, 0.0).astype(BF16), low)
            daff_ref[...] += dprod * decay
            both = dprod * prod
            rowsum[pl.ds(h, 1), :] = jnp.sum(both, axis=0, keepdims=True)
            away = jnp.sum(both, axis=1, keepdims=True)
            colsum[...] += jnp.where(lane == h, away, 0.0)
            outs.append(dot(prod.astype(BF16), low))
        dscaled = jnp.where(first, outs[0], outs[1])
        dx_ref[:, here] = dscaled * steps + dy * skip_ref[:, here]
        gain_step = dscaled * x
        left = jnp.sum(jnp.where(first, gain_step, 0.0), axis=1, keepdims=True)
        right = jnp.sum(jnp.where(first, 0.0, gain_step), axis=1, keepdims=True)
        stepgrad[...] += jnp.where(lane == 2 * p, left, 0.0) + jnp.where(
            lane == 2 * p + 1, right, 0.0
        )

    for start, end in spans(PAIRS_OF_HEADS, 6):
        pl.loop(start, end)(pair)
        yield

    daff = daff_ref[...] * inside_ref[...].T
    dx_ref[:, INNER : INNER + STATE] = dot_exact(daff, x_ref[:, INNER + STATE :])
    dx_ref[:, INNER + STATE :] = dot_exact(daff.T, x_ref[:, INNER : INNER + STATE])
    yield
    pad = jnp.zeros((LANES - HEADS, rows), F32)
    dsums = jnp.concatenate([rowsum[...], pad], axis=0).T - colsum[...]
    dlog = dot_exact(inside_ref[...].T, dsums)[:, :HEADS]
    raw, step, rates = step_sizes(inner_ref, heads_ref)
    dstep = stepgrad[:, :HEADS] + dlog * rates
    draw = dstep * sigmoid(raw)
    dinner_ref[:, INNER + CONVCH :] = draw.astype(BF16)
    dheads_ref[0:1, :HEADS] = jnp.sum(dlog * step, axis=0, keepdims=True) * rates
    dheads_ref[1:2, :HEADS] = jnp.sum(draw, axis=0, keepdims=True)
    yield

    def conv_back(k):
        here = pl.ds(pl.multiple_of(k * LANES, LANES), LANES)
        there = pl.ds(pl.multiple_of(INNER + k * LANES, LANES), LANES)
        conv_in = inner_ref[:, there]
        taps = taps_ref[:, here]
        before = conv_before(conv_in, taps, position)
        sig = sigmoid(before)
        grad = dx_ref[:, here] * (sig * (1.0 + before * (1.0 - sig)))
        back = grad * taps[TAPS - 1 : TAPS]
        dtaps_ref[TAPS - 1 : TAPS, here] = jnp.sum(grad * conv_in, axis=0, keepdims=True)
        for offset in range(1, TAPS):
            t = TAPS - 1 - offset
            valid = jnp.where(position >= offset, grad, 0.0)
            dtaps_ref[t : t + 1, here] = jnp.sum(
                valid * pltpu.roll(conv_in, offset, 0), axis=0, keepdims=True
            )
            back = back + pltpu.roll(valid, rows - offset, 0) * taps[t : t + 1]
        dinner_ref[:, there] = back.astype(BF16)

    for start, end in spans(CONVCH // LANES, 4):
        pl.loop(start, end)(conv_back)
        yield


def mixer_backward_scratch(rows):
    return mixer_scratch(rows) + [
        pltpu.VMEM((rows, CONVCH), F32),
        pltpu.VMEM((rows, rows), F32),
        pltpu.VMEM((HEADS, rows), F32),
        pltpu.VMEM((rows, LANES), F32),
        pltpu.VMEM((rows, LANES), F32),
    ]


def mixer_backward_shapes(inner, taps):
    shape = jax.ShapeDtypeStruct
    return [
        shape(inner.shape, BF16),
        shape(taps.shape, F32),
        shape((1, INNER), F32),
        shape((1, INNER), F32),
        shape((8, LANES), F32),
    ]


def rotate_rows(front, rear, cosine, sine):
    return front * cosine - rear * sine, rear * cosine + front * sine


def attention_setup(packed_ref, cosine_ref, sine_ref, query, key_rows):
    half = HD // 2
    for h in range(QH + KVH):
        at = h * HD
        turned = rotate_rows(
            packed_ref[at : at + half], packed_ref[at + half : at + HD],
            cosine_ref[...], sine_ref[...],
        )
        both = jnp.concatenate(turned, axis=0)
        if h < QH:
            query[at : at + HD] = both.astype(BF16)
        else:
            key_rows[at - QH * HD : at - (QH - 1) * HD] = both


def turned_probs(keys, query, outside):
    scores = dot(keys, query) * SCORE_SCALE + outside
    expo = jnp.exp(scores - jnp.max(scores, axis=0, keepdims=True))
    return expo / jnp.sum(expo, axis=0, keepdims=True)


def attention_forward_kernel(
    packed_ref, cosine_ref, sine_ref, outside_ref, context_ref, turned_ref, query, key_rows
):
    attention_setup(packed_ref, cosine_ref, sine_ref, query, key_rows)
    keys = key_rows[...].T.astype(BF16)
    values = packed_ref[(QH + KVH) * HD :].astype(BF16)
    for h in range(QH):
        kv = h * KVH // QH
        probs = turned_probs(
            keys[:, kv * HD : (kv + 1) * HD], query[h * HD : (h + 1) * HD], outside_ref[...]
        )
        turned = dot(values[kv * HD : (kv + 1) * HD], probs.astype(BF16))
        turned_ref[h * HD : (h + 1) * HD] = turned.astype(BF16)
    for k in range(QH * HD // LANES):
        here = slice(k * LANES, (k + 1) * LANES)
        context_ref[:, here] = turned_ref[here].astype(F32).T.astype(BF16)


def attention_forward(packed, cosine, sine, outside):
    rows = packed.shape[1]
    shape = jax.ShapeDtypeStruct
    return pl.pallas_call(
        attention_forward_kernel,
        out_shape=[shape((rows, QH * HD), BF16), shape((QH * HD, rows), BF16)],
        in_specs=[VMEM] * 4,
        out_specs=[VMEM] * 2,
        scratch_shapes=[pltpu.VMEM((QH * HD, rows), BF16), pltpu.VMEM((KVH * HD, rows), F32)],
        compiler_params=BIG,
        name="attention_forward",
    )(packed, cosine, sine, outside)


def attention_backward_steps(
    packed_ref, cosine_ref, sine_ref, outside_ref, dcontext_ref, dpacked_ref,
    query, key_rows, grad_rows,
):
    half = HD // 2
    attention_setup(packed_ref, cosine_ref, sine_ref, query, key_rows)
    low_rows = key_rows[...].astype(BF16)
    keys = key_rows[...].T.astype(BF16)
    values = packed_ref[(QH + KVH) * HD :].T.astype(BF16)
    for k in range(QH * HD // LANES):
        here = slice(k * LANES, (k + 1) * LANES)
        grad_rows[here] = dcontext_ref[:, here].astype(F32).T
    yield
    for kv in range(KVH):
        of_kv = slice(kv * HD, (kv + 1) * HD)
        dkey = jnp.zeros((HD, keys.shape[0]), F32)
        dvalue = jnp.zeros((HD, keys.shape[0]), F32)
        for h in range(kv * QH // KVH, (kv + 1) * QH // KVH):
            here = slice(h * HD, (h + 1) * HD)
            probs = turned_probs(keys[:, of_kv], query[here], outside_ref[...])
            grad = grad_rows[here].astype(BF16)
            dprobs = dot(values[:, of_kv], grad)
            dvalue = dvalue + dot_rt(grad, probs.astype(BF16))
            inner = jnp.sum(probs * dprobs, axis=0, keepdims=True)
            dscores = (probs * (dprobs - inner) * SCORE_SCALE).astype(BF16)
            dquery = dot(low_rows[of_kv], dscores)
            dkey = dkey + dot_rt(query[here], dscores)
            turned = rotate_rows(dquery[:half], dquery[half:], cosine_ref[...], -sine_ref[...])
            grad_rows[here] = jnp.concatenate(turned, axis=0)
            yield
        turned = rotate_rows(dkey[:half], dkey[half:], cosine_ref[...], -sine_ref[...])
        at = QH * HD + kv * HD
        grad_rows[at : at + HD] = jnp.concatenate(turned, axis=0)
        at = (QH + KVH) * HD + kv * HD
        grad_rows[at : at + HD] = dvalue
    for k in range((QH + 2 * KVH) * HD // LANES):
        here = slice(k * LANES, (k + 1) * LANES)
        dpacked_ref[:, here] = grad_rows[here].T.astype(BF16)
    yield


def attention_backward_scratch(rows):
    return [
        pltpu.VMEM((QH * HD, rows), BF16),
        pltpu.VMEM((KVH * HD, rows), F32),
        pltpu.VMEM(((QH + 2 * KVH) * HD, rows), F32),
    ]


def host_steps(ins, outs, scratch):
    yield from mixer_backward_steps(*ins[:9], *outs[:5], *scratch[:10])
    yield from attention_backward_steps(*ins[9:], outs[5], *scratch[10:])


def host_shapes(ins):
    rows, wide = ins[0].shape[0], ins[9].shape[0]
    return mixer_backward_shapes(ins[0], ins[1]) + [jax.ShapeDtypeStruct((rows, wide), BF16)]


def host_scratch(ins):
    rows = ins[0].shape[0]
    return mixer_backward_scratch(rows) + attention_backward_scratch(rows)


def host_plain(ins):
    shapes, scratch = host_shapes(ins), host_scratch(ins)

    def kernel(*refs):
        one, two = len(ins), len(ins) + len(shapes)
        run_steps(host_steps(refs[:one], refs[one:two], refs[two:]))

    return pl.pallas_call(
        kernel,
        out_shape=shapes,
        in_specs=[VMEM] * len(ins),
        out_specs=[VMEM] * len(shapes),
        scratch_shapes=scratch,
        compiler_params=BIG,
        name="mixer_attention_backward",
    )(*ins)


def flip(me, bit):
    step = 1 << bit
    return me + step * (1 - 2 * ((me // step) % 2))


def place(bits, free, mine, flipped=()):
    return tuple(
        slice(None) if b in free else 1 - mine[b] if b in flipped else mine[b]
        for b in reversed(range(bits))
    )


def greet(me, bits):
    barrier = pltpu.get_barrier_semaphore()
    for b in range(bits):
        pl.semaphore_signal(barrier, inc=1, device_id=(flip(me, b),), device_id_type=MESH)
    pl.semaphore_wait(barrier, bits)


def remote(me, src, dst, send, recv, bit):
    return pltpu.make_async_remote_copy(
        src_ref=src,
        dst_ref=dst,
        send_sem=send,
        recv_sem=recv,
        device_id=(flip(me, bit),),
        device_id_type=MESH,
    )


def gather_kernel(devices, chunks, events, layers, arrays, *refs):
    bits = devices.bit_length() - 1
    ins = refs[:arrays]
    outs = refs[arrays : arrays + layers * arrays]
    send_sem, recv_sem, csend_sem, crecv_sem, own_sem = refs[arrays + layers * arrays :]
    me = lax.axis_index("dp")
    mine = [(me // (1 << b)) % 2 for b in range(bits)]
    greet(me, bits)
    own, sends, cores, pending = [], [], [], {}
    for c, (l, a, order) in enumerate(chunks):
        here = outs[l * arrays + a].at[place(bits, (), mine)]
        src = ins[a].at[l]
        copy = remote(me, src, here, send_sem.at[c, 0], recv_sem.at[c, 0], order[0])
        copy.start()
        pending[c] = copy
        sends.append(copy)
        local = pltpu.make_async_copy(src, here, own_sem.at[c])
        local.start()
        own.append(local)
    for c, (l, a, order) in enumerate(chunks):
        here = outs[l * arrays + a].at[place(bits, (), mine)]
        copy = remote(me, ins[a].at[l], here, csend_sem.at[c, 0], crecv_sem.at[c, 0], 0)
        copy.start()
        sends.append(copy)
        cores.append(copy)
    for local in own:
        local.wait()
    for c, s in events:
        l, a, order = chunks[c]
        full = outs[l * arrays + a]
        pending[c].wait_recv()
        if s + 1 < bits - 1:
            view = full.at[place(bits, order[: s + 1], mine)]
            copy = remote(
                me, view, view, send_sem.at[c, s + 1], recv_sem.at[c, s + 1], order[s + 1]
            )
            copy.start()
            pending[c] = copy
            sends.append(copy)
        new = full.at[place(bits, order[:s], mine, (order[s],))]
        copy = remote(me, new, new, csend_sem.at[c, s + 1], crecv_sem.at[c, s + 1], 0)
        copy.start()
        sends.append(copy)
        cores.append(copy)
    for copy in sends:
        copy.wait_send()
    for copy in cores:
        copy.wait_recv()


def gather_all(shards, devices):
    bits = devices.bit_length() - 1
    layers = shards[0].shape[0]
    n = len(AG_CHUNKS)
    sent = {(layer, a) for layer, a, _ in AG_CHUNKS}
    outs = [
        jax.ShapeDtypeStruct(
            (2,) * bits + (s.shape[1:] if (layer, a) in sent else (8, 128)), s.dtype
        )
        for layer in range(layers)
        for a, s in enumerate(shards)
    ]
    res = pl.pallas_call(
        functools.partial(gather_kernel, devices, AG_CHUNKS, AG_EVENTS, layers, len(shards)),
        out_shape=outs,
        in_specs=[pl.BlockSpec(memory_space=pltpu.VMEM)] * len(shards),
        out_specs=[pl.BlockSpec(memory_space=pl.ANY)] * len(outs),
        scratch_shapes=[pltpu.SemaphoreType.DMA((n, bits - 1))] * 2
        + [pltpu.SemaphoreType.DMA((n, bits))] * 2
        + [pltpu.SemaphoreType.DMA((n,))],
        compiler_params=pltpu.CompilerParams(collective_id=0, has_side_effects=True),
        name="gather_all",
    )(*shards)
    full = [r.reshape((devices * r.shape[-2], r.shape[-1])) for r in res]
    return [full[l * len(shards) : (l + 1) * len(shards)] for l in range(layers)]


PAIRS = ((0, 0), (1, 2), (0, 1), (2, 2), (3, 3), (4, 4))


def take(refs, *sizes):
    groups, at = [], 0
    for size in sizes:
        groups.append(refs[at : at + size])
        at += size
    return groups + [refs[at:]]


def scatter_kernel(devices, plan, jobs, arrs, counts, *refs):
    chunks, events, row_bits = plan
    bits = devices.bit_length() - 1
    half = devices // 2
    nx, ny, nsmall, nrows, nhost, nhost_out = counts
    na, nc = len(arrs), len(chunks)
    xs, ys, small_in, rows_in, host_in, refs = take(refs, nx, ny, nsmall, nrows, nhost)
    outs, small_out, rows_out, host_out, refs = take(refs, na, nsmall, nrows, nhost_out)
    xr, yr, sums, parts, refs = take(refs, nx, ny, nc, nc * (bits - 1))
    small_mid, small_got, rows_got, refs = take(
        refs, nsmall * (bits - 1), nsmall * bits, nrows * bits
    )
    host_scratch_refs, sems = refs[:-10], refs[-10:]
    xs_s, xs_r, ys_s, ys_r, st_s, st_r, sm_s, sm_r, ro_s, ro_r = sems
    me = lax.axis_index("dp")
    mine = [(me // (1 << b)) % 2 for b in range(bits)]
    greet(me, bits)
    core = mine[0]
    swaps_x, swaps_y, got_x, got_y = {}, {}, set(), set()
    for a, _, _, _ in chunks:
        xi, yi = jobs[a]
        if xi not in swaps_x:
            swaps_x[xi] = remote(
                me, xs[xi].at[:, 1 - core], xr[xi], xs_s.at[xi], xs_r.at[xi], 0
            )
            swaps_x[xi].start()
        if yi not in swaps_y:
            swaps_y[yi] = remote(me, ys[yi], yr[yi], ys_s.at[yi], ys_r.at[yi], 0)
            swaps_y[yi].start()
    sends, pending = [], {}

    def small_send(s):
        src = small_in[0] if s == 0 else small_mid[s - 1]
        copy = remote(me, src, small_got[s], sm_s.at[s], sm_r.at[s], s)
        copy.start()
        pending["small"] = copy
        sends.append(copy)

    def small_receive(s):
        src = small_in[0] if s == 0 else small_mid[s - 1]
        pending["small"].wait_recv()
        total = src[...] + small_got[s][...]
        if s + 1 < bits:
            small_mid[s][...] = total
            small_send(s + 1)
        else:
            small_out[0][...] = total

    def rows_send(s):
        bit = row_bits[s]
        index = tuple(1 - mine[q] if q == bit else slice(None) for q in reversed(range(bits)))
        copy = remote(me, rows_out[0].at[index], rows_got[s], ro_s.at[s], ro_r.at[s], bit)
        copy.start()
        pending["rows"] = copy

    def rows_receive(s):
        pending["rows"].wait_send()
        pending["rows"].wait_recv()

        @pl.loop(0, 1 << (bits - 1))
        def _(j):
            here, there, pos = [], [], bits - 1
            for q in reversed(range(bits)):
                if q == row_bits[s]:
                    here.append(1 - mine[q])
                else:
                    pos -= 1
                    value = (j // (1 << pos)) % 2
                    here.append(value)
                    there.append(value)
            rows_out[0][tuple(here)] = rows_got[s][tuple(there)]

        if s + 1 < bits:
            rows_send(s + 1)

    def send(c, s):
        order = chunks[c][3]
        index = tuple(
            1 - mine[q] if q == order[s] else mine[q] if q in order[:s] else slice(None)
            for q in reversed(range(1, bits))
        )
        copy = remote(
            me,
            sums[c].at[index],
            parts[c * (bits - 1) + s],
            st_s.at[c, s],
            st_r.at[c, s],
            order[s],
        )
        copy.start()
        pending[c] = copy
        sends.append(copy)

    def compute(c):
        a, first, end, _ = chunks[c]
        xi, yi = jobs[a]
        rows = arrs[a][0]
        if xi not in got_x:
            swaps_x[xi].wait_recv()
            got_x.add(xi)
        if yi not in got_y:
            swaps_y[yi].wait_recv()
            got_y.add(yi)

        def tile(start, width, offset):
            left = xs[xi][:, core].reshape(half * rows, -1)
            other = xr[xi][...].reshape(half * rows, -1)
            value = dot(left, ys[yi][:, pl.ds(start, width)])
            value = value + dot(other, yr[yi][:, pl.ds(start, width)])
            sums[c][..., pl.ds(offset, width)] = value.astype(BF16).reshape(
                (2,) * (bits - 1) + (rows, width)
            )

        width, step = end - first, 256
        whole = width // step

        @pl.loop(0, whole)
        def _(i):
            tile(
                pl.multiple_of(first + i * step, 128), step, pl.multiple_of(i * step, 128)
            )

        if width % step:
            tile(first + whole * step, width % step, whole * step)
        send(c, 0)

    def receive(c, s):
        a, first, end, order = chunks[c]
        pending[c].wait_recv()
        fixed = order[: s + 1]
        free = [q for q in reversed(range(1, bits)) if q not in fixed]

        def add(j, last):
            here, there, pos = [], [], len(free)
            for q in reversed(range(1, bits)):
                if q in fixed:
                    here.append(mine[q])
                else:
                    pos -= 1
                    value = (j // (1 << pos)) % 2
                    here.append(value)
                    there.append(value)
            part = parts[c * (bits - 1) + s]
            total = part[tuple(there)].astype(F32) + sums[c][tuple(here)].astype(F32)
            if last:
                outs[a][:, first:end] = total
            else:
                sums[c][tuple(here)] = total.astype(BF16)

        if not free:
            add(0, True)
        else:

            @pl.loop(0, 1 << len(free))
            def _(j):
                add(j, False)

            send(c, s + 1)

    steps = host_steps(host_in, host_out, host_scratch_refs) if nhost else iter(())
    if nsmall:
        small_send(0)
    if nrows:
        fetch = pltpu.make_async_copy(rows_in[0], rows_out[0], ro_s.at[0])
        fetch.start()
        fetch.wait()
        rows_send(0)
    for c, s in events:
        if c == -1:
            small_receive(s)
        elif c == -2:
            rows_receive(s)
        elif c == -3:
            next(steps, None)
        elif s < 0:
            compute(c)
        else:
            receive(c, s)
    run_steps(steps)
    for copy in list(swaps_x.values()) + list(swaps_y.values()) + sends:
        copy.wait_send()


def scatter(plan, jobs, turned, grads, devices, number, small=None, rows=None, host=()):
    chunks = plan[0]
    bits = devices.bit_length() - 1
    nx, ny = len(turned), len(grads)
    half = devices // 2
    split = [x.reshape(half, 2, x.shape[0] // devices, x.shape[1]) for x in turned]
    arrs = [(turned[xi].shape[0] // devices, grads[yi].shape[1]) for xi, yi in jobs]
    smalls = [] if small is None else [small]
    moved = []
    if rows is not None:
        moved.append(rows.reshape((2,) * bits + (rows.shape[0] // devices, rows.shape[1])))
    shape = jax.ShapeDtypeStruct
    extra = host_shapes(host) if host else []
    outs = [shape(size, F32) for size in arrs] + [shape(x.shape, F32) for x in smalls]
    outs += [shape(x.shape, BF16) for x in moved] + extra
    scratch = [pltpu.VMEM((half, x.shape[0] // devices, x.shape[1]), BF16) for x in turned]
    scratch += [pltpu.VMEM(y.shape, BF16) for y in grads]
    for a, first, end, _ in chunks:
        scratch.append(pltpu.VMEM((2,) * (bits - 1) + (arrs[a][0], end - first), BF16))
    for a, first, end, _ in chunks:
        for s in range(bits - 1):
            scratch.append(pltpu.VMEM((2,) * (bits - 2 - s) + (arrs[a][0], end - first), BF16))
    for x in smalls:
        scratch += [pltpu.VMEM(x.shape, F32)] * (2 * bits - 1)
    for x in moved:
        scratch += [pltpu.VMEM(x.shape[1:], BF16)] * bits
    if host:
        scratch += host_scratch(host)
    dma = pltpu.SemaphoreType.DMA
    scratch += [dma((nx,))] * 2 + [dma((ny,))] * 2 + [dma((len(chunks), bits - 1))] * 2
    scratch += [dma((bits,))] * 4
    counts = (nx, ny, len(smalls), len(moved), len(host), len(extra))
    res = pl.pallas_call(
        functools.partial(scatter_kernel, devices, plan, jobs, arrs, counts),
        out_shape=outs,
        in_specs=[VMEM] * (nx + ny + len(smalls))
        + [pl.BlockSpec(memory_space=pl.ANY)] * len(moved)
        + [VMEM] * len(host),
        out_specs=[VMEM] * len(outs),
        scratch_shapes=scratch,
        compiler_params=pltpu.CompilerParams(
            collective_id=number, has_side_effects=True, vmem_limit_bytes=67043328
        ),
        name="scatter",
    )(*split, *grads, *smalls, *moved, *host)
    owned, small_total, back, own_work = take(res, len(arrs), len(smalls), len(moved))
    return owned, small_total, [x.reshape(rows.shape) for x in back], own_work


def scatter_plain(turned, grads, small):
    owned = [
        lax.psum_scatter(
            dot(turned[xi], grads[yi]).astype(BF16), "dp", scatter_dimension=0, tiled=True
        ).astype(F32)
        for xi, yi in PAIRS
    ]
    return owned + [lax.psum(small, "dp")]


def doc_layout(doc_lengths, rows_count):
    rows_index = jnp.arange(rows_count, dtype=jnp.int32)
    doc_ends = jnp.cumsum(doc_lengths, dtype=jnp.int32)
    later = (rows_index[:, None] >= doc_ends[None, :]).astype(jnp.int32)
    segment = jnp.sum(later, axis=1, dtype=jnp.int32)
    position = rows_index - jnp.sum(later * doc_lengths[None, :], axis=1, dtype=jnp.int32)
    return (segment, position)


def inverse_rms(values):
    return lax.rsqrt(jnp.mean(values * values, axis=-1, keepdims=True) + EPSILON)


def norm_backward(grad, values, scale, gain):
    normed = values * scale
    grad_gain = jnp.sum(grad * normed, axis=0)
    inner = grad * gain
    return scale * (inner - normed * jnp.mean(inner * normed, axis=-1, keepdims=True)), grad_gain


def layer_forward(hidden, weights, small, layout):
    w_in, w_mix, w_qkv, w_attn, w_gate_up, w_down = weights
    gains, taps, gain_inner, heads, skip = small
    position, inside, outside, cosine, sine = layout
    scale = inverse_rms(hidden)
    normed = (hidden * scale * gains[0]).astype(BF16)
    inner = dot(normed, w_in)
    packed = lax.dot_general(
        w_qkv, normed, (((0,), (1,)), ((), ())), preferred_element_type=F32
    )
    mixed, mixed_rows, y = mixer_forward(inner, taps, heads, skip, gain_inner, position, inside)
    context, context_rows = attention_forward(packed, cosine, sine, outside)
    middle = hidden + dot(mixed, w_mix) + dot(context, w_attn)
    scale_two = inverse_rms(middle)
    normed_two = (middle * scale_two * gains[1]).astype(BF16)
    both = dot(normed_two, w_gate_up)
    active = (jax.nn.silu(both[:, :FF]) * both[:, FF:]).astype(BF16)
    out = middle + dot(active, w_down)
    turned = [normed.T, mixed_rows, context_rows, normed_two.T, active.T]
    return out, (hidden, scale, inner, packed, y, middle, scale_two, both, turned)


def backward_start(grad, kept, weights, small, layout):
    w_in, w_mix, w_qkv, w_attn, w_gate_up, w_down = weights
    gains, taps, gain_inner, heads, skip = small
    position, inside, outside, cosine, sine = layout
    hidden, scale, inner, packed, y, middle, scale_two, both, turned = kept
    ddown = grad.astype(BF16)
    dactive = dot_rt(ddown, w_down)
    gate, up = both[:, :FF], both[:, FF:]
    sig = jax.nn.sigmoid(gate)
    dgate = dactive * up * (sig * (1.0 + gate * (1.0 - sig)))
    dboth = jnp.concatenate([dgate, dactive * (gate * sig)], axis=1).astype(BF16)
    dmiddle, dgain_two = norm_backward(dot_rt(dboth, w_gate_up), middle, scale_two, gains[1])
    dmiddle = grad + dmiddle
    dbranch = dmiddle.astype(BF16)
    dmixed = dot_rt(dbranch, w_mix)
    dcontext = dot_rt(dbranch, w_attn).astype(BF16)
    host = (inner, taps, heads, skip, gain_inner, position, inside, y, dmixed)
    host += (packed, cosine, sine, outside, dcontext)
    return dmiddle, dgain_two, dbranch, dboth, ddown, host


def backward_end(dmiddle, dgain_two, kept, weights, small, done):
    w_in, w_qkv = weights[0], weights[2]
    hidden, scale = kept[:2]
    dinner, dtaps, dgain_inner, dskip, dheads, dpacked = done
    dnormed = dot_rt(dinner, w_in) + dot_rt(dpacked, w_qkv)
    dhidden, dgain = norm_backward(dnormed, hidden, scale, small[0][0])
    flat = [dgain, dgain_two, dtaps.reshape(-1), dgain_inner[0], dheads[0, :HEADS]]
    flat += [jnp.sum(dskip.reshape(HEADS, HDIM), axis=1), dheads[1, :HEADS]]
    flat = jnp.concatenate(flat)
    lines = -(-flat.shape[0] // 1024) * 8
    small_sum = jnp.pad(flat, (0, lines * 128 - flat.shape[0])).reshape(lines, 128)
    return dmiddle + dhidden, small_sum


def shards(
    tokens,
    cotangent,
    destination,
    lengths,
    norm_gains,
    in_proj,
    conv_weight,
    ssm_gain,
    mixer_out,
    qkv_proj,
    attn_out,
    gate_up,
    down_proj,
    a_log,
    d_skip,
    dt_bias,
):
    devices = lax.axis_size("dp")
    me = lax.axis_index("dp")
    rows_here, width = tokens.shape
    share = rows_here // devices
    own_kernels = devices == 32
    index = jnp.arange(rows_here, dtype=jnp.int32)
    slabs = destination.reshape(devices, rows_here)

    own = lax.dynamic_slice_in_dim(slabs, me, 1, 0)[0] // rows_here
    same = (own[:, None] == own[None, :]) & (index[None, :] < index[:, None])
    slot = own * share + jnp.sum(same.astype(jnp.int32), axis=1)
    leave = (slot[None, :] == index[:, None]).astype(BF16)
    outgoing = [dot(leave, x).astype(BF16) for x in (tokens, cotangent)]

    def exchange(rows):
        split = rows.reshape(devices, share, width)
        moved = lax.all_to_all(split, "dp", split_axis=0, concat_axis=0, tiled=True)
        return moved.reshape(rows_here, width)

    arrived = [exchange(x) for x in outgoing]

    local = slabs - me * rows_here
    mask = ((local >= 0) & (local < rows_here)).astype(BF16)
    below = (index[:, None] < index[None, :]).astype(BF16)
    rank = dot(mask, below).astype(jnp.int32)
    order = rank + share * jnp.arange(devices, dtype=jnp.int32)[:, None]
    hits = local.reshape(-1)[None, :] == index[:, None]
    taken = jnp.sum(jnp.where(hits, order.reshape(-1)[None, :], 0), axis=1)
    enter = (taken[:, None] == index[None, :]).astype(BF16)
    hidden = dot(enter, arrived[0])
    upstream = dot(enter, arrived[1])

    segment, position = doc_layout(lengths[0], rows_here)
    inside = (segment[:, None] == segment[None, :]) & (index[:, None] >= index[None, :])
    inverse = ROPE_BASE ** (-(jnp.arange(HD // 2, dtype=F32) * 2.0 / HD))
    angles = position.astype(F32)[:, None] * inverse[None, :]
    outside = jnp.where(inside.T, 0.0, -1e30)
    layout = (position[:, None], inside.astype(F32), outside, jnp.cos(angles).T, jnp.sin(angles).T)

    matrices = (in_proj, mixer_out, qkv_proj, attn_out, gate_up, down_proj)
    gain_part, conv_part, inner_part = (x.shape[-1] for x in (norm_gains, conv_weight, ssm_gain))
    packed = jnp.concatenate(
        [norm_gains.reshape(LAYERS, -1), conv_weight.reshape(LAYERS, -1), ssm_gain], axis=1
    )
    used = packed.shape[1]
    if own_kernels:
        room = SMALL_ROWS * 128
        padded = jnp.pad(packed, ((0, 0), (0, room - used))).reshape(LAYERS, SMALL_ROWS, 128)
        gathered = gather_all(list(matrices) + [padded], devices)
        weights = [g[:-1] for g in gathered]
        late = LATE_ARRAY
        tied = matrices[late][1] + gathered[0][-1][:1, :1] * 0
        weights[1][late] = lax.all_gather(tied, "dp", axis=0, tiled=True)
        smalls = [g[-1].reshape(devices, room)[:, :used] for g in gathered]
    else:
        weights = [
            [lax.all_gather(x[layer], "dp", axis=0, tiled=True) for x in matrices]
            for layer in range(LAYERS)
        ]
        every = lax.all_gather(packed, "dp", axis=0)
        smalls = [every[:, layer] for layer in range(LAYERS)]

    def spread(piece, count):
        shaped = piece.reshape(devices, count, -1)
        return jnp.swapaxes(shaped, 0, 1).reshape(count, -1).astype(F32)

    def small_of(layer):
        both = smalls[layer]
        mid = 2 * gain_part
        heads = jnp.stack([a_log[layer], d_skip[layer], dt_bias[layer]])
        return (
            spread(both[:, :mid], 2),
            spread(both[:, mid : mid + TAPS * conv_part], TAPS),
            spread(both[:, mid + TAPS * conv_part :], 1),
            jnp.pad(heads, ((0, 5), (0, LANES - HEADS))),
            jnp.repeat(d_skip[layer], HDIM)[None],
        )

    params = [small_of(layer) for layer in range(LAYERS)]

    kept = [None] * LAYERS
    for layer in range(LAYERS):
        hidden, kept[layer] = layer_forward(hidden, weights[layer], params[layer], layout)

    def permute_back(choice, rows):
        return lax.dot_general(
            choice, rows.astype(BF16), (((0,), (0,)), ((), ())), preferred_element_type=F32
        )

    top, low = 1, 0
    start = backward_start(upstream, kept[top], weights[top], params[top], layout)
    dmiddle, dgain_two, dbranch, dboth, ddown, host = start
    if own_kernels:
        up_down, _, _, done = scatter(
            PLAN_A, ((0, 0), (1, 1)), kept[top][-1][3:], [dboth, ddown], devices, 1, host=host
        )
    else:
        done = host_plain(host)
    flowing, small_top = backward_end(
        dmiddle, dgain_two, kept[top], weights[top], params[top], done
    )
    turned_top = kept[top][-1]
    grads_top = [done[0], done[5], dbranch, dboth, ddown]

    start = backward_start(flowing, kept[low], weights[low], params[low], layout)
    dmiddle, dgain_two, dbranch, dboth, ddown, host = start
    leaving = permute_back(enter, hidden).astype(BF16)
    turned_low = kept[low][-1]
    if own_kernels:
        second, sum_top, home, done = scatter(
            PLAN_B,
            ((0, 0), (1, 2), (0, 1), (2, 2), (3, 3), (4, 4)),
            turned_top[:3] + turned_low[3:],
            grads_top[:3] + [dboth, ddown],
            devices,
            2,
            small=small_top,
            rows=leaving,
            host=host,
        )
    else:
        done = host_plain(host)
    flowing, small_low = backward_end(
        dmiddle, dgain_two, kept[low], weights[low], params[low], done
    )
    grads_low = [done[0], done[5], dbranch, dboth, ddown]
    leaving_grad = permute_back(enter, flowing).astype(BF16)
    if own_kernels:
        third, sum_low, home_grad, _ = scatter(
            PLAN_C,
            ((0, 0), (1, 2), (0, 1), (2, 2)),
            turned_low[:3],
            grads_low[:3],
            devices,
            3,
            small=small_low,
            rows=leaving_grad,
        )
        home, home_grad = home[0], home_grad[0]
        owned = [third + second[4:] + sum_low, second[:4] + up_down + sum_top]
    else:
        owned = [
            scatter_plain(turned_low, grads_low, small_low),
            scatter_plain(turned_top, grads_top, small_top),
        ]
        home, home_grad = exchange(leaving), exchange(leaving_grad)
    out_tokens = permute_back(leave, home).astype(BF16)
    in_grad = permute_back(leave, home_grad)

    big = [jnp.stack([owned[layer][k] for layer in range(LAYERS)]) for k in range(6)]
    totals = jnp.stack([owned[layer][6].reshape(-1) for layer in range(LAYERS)])
    model = gain_part * devices
    sizes = (2 * model, TAPS * CONVCH, INNER, HEADS, HEADS, HEADS)
    pieces, at = [], 0
    for size in sizes:
        pieces.append(totals[:, at : at + size])
        at += size

    def mine(piece, count, part):
        shaped = piece.reshape(LAYERS, count, devices * part)
        return lax.dynamic_slice_in_dim(shaped, me * part, part, 2)

    return (
        out_tokens,
        in_grad,
        mine(pieces[0], 2, gain_part),
        big[0],
        mine(pieces[1], TAPS, conv_part),
        mine(pieces[2], 1, inner_part)[:, 0],
        big[1],
        big[2],
        big[3],
        big[4],
        big[5],
        pieces[3],
        pieces[4],
        pieces[5],
    )


def solution(mesh):
    placed = (
        P("dp", None),
        P("dp", None),
        P(),
        P("dp", None),
        P(None, None, "dp"),
        P(None, "dp", None),
        P(None, None, "dp"),
        P(None, "dp"),
        P(None, "dp", None),
        P(None, "dp", None),
        P(None, "dp", None),
        P(None, "dp", None),
        P(None, "dp", None),
        P(),
        P(),
        P(),
    )
    return jax.shard_map(
        shards,
        mesh=mesh,
        in_specs=placed,
        out_specs=(
            P("dp", None),
            P("dp", None),
            P(None, None, "dp"),
            P(None, "dp", None),
            P(None, None, "dp"),
            P(None, "dp"),
            P(None, "dp", None),
            P(None, "dp", None),
            P(None, "dp", None),
            P(None, "dp", None),
            P(None, "dp", None),
            P(),
            P(),
            P(),
        ),
        check_vma=False,
    )
```

```python
import functools

import jax
import jax.numpy as jnp
from jax import lax
from jax.experimental import pallas as pl
from jax.experimental.pallas import tpu as pltpu
from jax.sharding import PartitionSpec as P

FF = 2048
HEADS = 24
HDIM = 64
STATE = 128
QH = 8
KVH = 2
HD = 64
LAYERS = 2
INNER = 1536
CONVCH = 1792
TAPS = 4
EPSILON = 1e-05
ROPE_BASE = 100000000000.0
SCORE_SCALE = 0.125
HIGHEST = lax.Precision.HIGHEST
F32 = jnp.float32
BF16 = jnp.bfloat16
MESH = pl.DeviceIdType.MESH

AG_CHUNKS = [(0, 6, (4, 3, 2, 1)), (1, 6, (4, 3, 2, 1)), (1, 0, (4, 3, 1, 2)), (1, 3, (4, 3, 2, 1)), (1, 2, (4, 3, 2, 1)), (0, 2, (4, 3, 2, 1)), (1, 5, (4, 3, 2, 1)), (0, 0, (4, 3, 1, 2)), (0, 3, (1, 4, 3, 2)), (0, 5, (4, 3, 2, 1)), (0, 4, (1, 2, 4, 3)), (0, 1, (1, 2, 4, 3)), (1, 1, (4, 3, 2, 1))]
AG_EVENTS = [(0, 0), (1, 0), (8, 0), (10, 0), (11, 0), (2, 0), (3, 0), (4, 0), (5, 0), (0, 1), (1, 1), (6, 0), (10, 1), (11, 1), (0, 2), (1, 2), (0, 3), (1, 3), (7, 0), (2, 1), (3, 1), (4, 1), (9, 0), (5, 1), (3, 2), (12, 0), (6, 1), (4, 2), (8, 1), (5, 2), (2, 2), (6, 2), (3, 3), (4, 3), (5, 3), (7, 1), (9, 1), (10, 2), (12, 1), (2, 3), (8, 2), (6, 3), (11, 2), (9, 2), (12, 2), (7, 2), (8, 3), (9, 3), (10, 3), (12, 3), (7, 3), (11, 3)]
PLAN_B = ([(3, 0, 1024, (2, 3, 1, 4)), (0, 0, 1664, (1, 3, 4, 2)), (0, 1664, 3352, (2, 1, 3, 4)), (4, 0, 1408, (2, 1, 3, 4)), (1, 0, 512, (2, 3, 1, 4)), (5, 512, 1024, (1, 3, 2, 4)), (2, 0, 768, (3, 2, 1, 4)), (4, 2688, 4096, (2, 1, 3, 4)), (4, 1408, 2688, (1, 3, 2, 4)), (5, 0, 512, (2, 1, 3, 4)), (1, 512, 1024, (2, 1, 3, 4))], [(0, -1), (1, -1), (2, -1), (3, -1), (4, -1), (5, -1), (6, -1), (7, -1), (8, -1), (9, -1), (10, -1), (-1, 0), (0, 0), (-2, 0), (-3, 0), (-3, 0), (-3, 0), (-3, 0), (-3, 0), (-3, 0), (-3, 0), (-3, 0), (6, 0), (1, 0), (0, 1), (-3, 0), (2, 0), (-3, 0), (-2, 1), (-3, 0), (-2, 2), (5, 0), (-3, 0), (-3, 0), (1, 1), (-3, 0), (-3, 0), (3, 0), (-3, 0), (-3, 0), (5, 1), (-3, 0), (-3, 0), (-3, 0), (8, 0), (-3, 0), (-1, 1), (-3, 0), (-3, 0), (0, 2), (4, 0), (-3, 0), (-3, 0), (-3, 0), (-3, 0), (-3, 0), (-3, 0), (-3, 0), (1, 2), (2, 1), (8, 1), (0, 3), (7, 0), (4, 1), (3, 1), (2, 2), (3, 2), (9, 0), (7, 1), (4, 2), (2, 3), (3, 3), (10, 0), (9, 1), (7, 2), (6, 1), (4, 3), (9, 2), (10, 1), (6, 2), (-2, 3), (7, 3), (5, 2), (-1, 2), (9, 3), (10, 2), (1, 3), (6, 3), (-2, 4), (8, 2), (-1, 3), (5, 3), (10, 3), (8, 3), (-1, 4)], (4, 3, 0, 2, 1))
PLAN_C = ([(0, 0, 896, (1, 2, 3, 4)), (3, 0, 512, (2, 3, 1, 4)), (0, 1664, 2560, (1, 2, 3, 4)), (1, 512, 1024, (2, 3, 4, 1)), (1, 0, 512, (1, 2, 3, 4)), (0, 2560, 3352, (1, 2, 3, 4)), (0, 896, 1664, (2, 3, 1, 4)), (2, 0, 384, (1, 2, 3, 4)), (2, 384, 768, (3, 1, 2, 4)), (3, 512, 1024, (1, 2, 3, 4))], [(0, -1), (1, -1), (2, -1), (3, -1), (4, -1), (5, -1), (6, -1), (7, -1), (8, -1), (9, -1), (-1, 0), (1, 0), (0, 0), (-2, 0), (3, 0), (-2, 1), (8, 0), (1, 1), (2, 0), (3, 1), (6, 0), (0, 1), (-2, 2), (4, 0), (2, 1), (3, 2), (6, 1), (4, 1), (0, 2), (5, 0), (2, 2), (7, 0), (4, 2), (9, 0), (0, 3), (5, 1), (-1, 1), (7, 1), (8, 1), (2, 3), (1, 2), (9, 1), (4, 3), (-1, 2), (5, 2), (8, 2), (7, 2), (9, 2), (1, 3), (-2, 3), (-1, 3), (3, 3), (6, 2), (5, 3), (8, 3), (7, 3), (9, 3), (-1, 4), (-2, 4), (6, 3)], (4, 0, 3, 1, 2))
PLAN_A = ([(1, 0, 256, (2, 1, 3, 4)), (1, 768, 1024, (3, 4, 1, 2)), (0, 0, 1024, (1, 2, 3, 4)), (0, 2048, 3072, (2, 3, 4, 1)), (0, 3072, 4096, (3, 4, 1, 2)), (0, 1024, 2048, (1, 2, 3, 4)), (1, 256, 512, (1, 2, 3, 4)), (1, 512, 768, (2, 1, 3, 4))], [(0, -1), (1, -1), (2, -1), (3, -1), (4, -1), (5, -1), (6, -1), (7, -1), (-3, 0), (0, 0), (1, 0), (-3, 0), (-3, 0), (-3, 0), (-3, 0), (-3, 0), (-3, 0), (-3, 0), (2, 0), (-3, 0), (1, 1), (3, 0), (4, 0), (-3, 0), (-3, 0), (7, 0), (-3, 0), (5, 0), (3, 1), (-3, 0), (2, 1), (-3, 0), (6, 0), (-3, 0), (-3, 0), (0, 1), (4, 1), (-3, 0), (5, 1), (1, 2), (-3, 0), (-3, 0), (7, 1), (6, 1), (2, 2), (-3, 0), (0, 2), (3, 2), (-3, 0), (1, 3), (-3, 0), (4, 2), (-3, 0), (-3, 0), (5, 2), (-3, 0), (-3, 0), (7, 2), (-3, 0), (-3, 0), (3, 3), (-3, 0), (6, 2), (2, 3), (-3, 0), (4, 3), (0, 3), (5, 3), (7, 3), (6, 3)], (1, 2, 3, 4, 0))

SMALL_ROWS = 16
LATE_ARRAY = 4


def dot(left, right):
    return jnp.dot(left, right, preferred_element_type=F32)


def dot_rt(left, right):
    return lax.dot_general(left, right, (((1,), (1,)), ((), ())), preferred_element_type=F32)


PAIRS_OF_HEADS = HEADS // 2
LANES = 128
VMEM = pl.BlockSpec(memory_space=pltpu.VMEM)
BIG = pltpu.CompilerParams(vmem_limit_bytes=56 * 1024 * 1024)


def dot_exact(left, right):
    return jnp.dot(left, right, preferred_element_type=F32, precision=HIGHEST)


def dot_rt_exact(left, right):
    return lax.dot_general(
        left, right, (((1,), (1,)), ((), ())), preferred_element_type=F32, precision=HIGHEST
    )


def sigmoid(x):
    return 1.0 / (1.0 + jnp.exp(-x))


def column_index(shape):
    return lax.broadcasted_iota(jnp.int32, shape, len(shape) - 1)


def shifted_down(values, offset, position):
    return jnp.where(position >= offset, pltpu.roll(values, offset, 0), 0.0)


def conv_before(conv_in, taps, position):
    total = conv_in * taps[TAPS - 1 : TAPS]
    for offset in range(1, TAPS):
        total = total + shifted_down(conv_in, offset, position) * taps[
            TAPS - 1 - offset : TAPS - offset
        ]
    return total


def spans(count, parts):
    edges = [count * k // parts for k in range(parts + 1)]
    return list(zip(edges[:-1], edges[1:]))


def run_steps(steps):
    for _ in steps:
        pass


def step_sizes(inner_ref, heads_ref):
    raw = inner_ref[:, INNER + CONVCH :] + heads_ref[2:3, :HEADS]
    step = jnp.maximum(raw, 0.0) + jnp.log1p(jnp.exp(-jnp.abs(raw)))
    return raw, step, -jnp.exp(heads_ref[0:1, :HEADS])


def mixer_setup(
    inner_ref, taps_ref, heads_ref, position, inside, x_ref, qcol, qrow, dtpair, unroll=1
):
    rows = inner_ref.shape[0]
    for start, end in spans(CONVCH // LANES, 2):

        @pl.loop(start, end, unroll=unroll)
        def _(k):
            at = pl.multiple_of(k * LANES, LANES)
            before = conv_before(
                inner_ref[:, pl.ds(pl.multiple_of(INNER + at, LANES), LANES)],
                taps_ref[:, pl.ds(at, LANES)],
                position,
            )
            x_ref[:, pl.ds(at, LANES)] = before * sigmoid(before)

        yield

    raw, step, rates = step_sizes(inner_ref, heads_ref)
    sums = dot_exact(inside, step * rates)
    wide = jnp.concatenate([sums, jnp.zeros((rows, LANES - HEADS), F32)], axis=1)
    qrow[...] = wide.T[: qrow.shape[0]]
    first = column_index((rows, LANES)) < HDIM
    yield
    for p in range(PAIRS_OF_HEADS):
        for source, target in ((sums, qcol), (step, dtpair)):
            both = [
                jnp.broadcast_to(source[:, h : h + 1], (rows, LANES)) for h in (2 * p, 2 * p + 1)
            ]
            target[p] = jnp.where(first, both[0], both[1])
        if p % 4 == 3:
            yield


def mixer_forward_kernel(
    inner_ref, taps_ref, heads_ref, skip_ref, gain_ref, position_ref, inside_ref,
    mixed_ref, turned_ref, y_ref, x_ref, qcol, qrow, dtpair, aff_ref,
):
    rows = inner_ref.shape[0]
    position = position_ref[...]
    inside = inside_ref[...]
    run_steps(
        mixer_setup(
            inner_ref, taps_ref, heads_ref, position, inside, x_ref, qcol, qrow, dtpair, unroll=7
        )
    )
    b_all = x_ref[:, INNER : INNER + STATE]
    c_all = x_ref[:, INNER + STATE :]
    aff_ref[...] = dot_rt_exact(c_all, b_all) * inside
    first = column_index((rows, LANES)) < HDIM

    def pair(p, total):
        at = pl.multiple_of(p * LANES, LANES)
        x = x_ref[:, pl.ds(at, LANES)]
        scaled = (x * dtpair[p]).astype(BF16)
        outs = []
        columns = qcol[p]
        for k in (0, 1):
            h = 2 * p + k
            column, row = columns[:, k * HDIM : k * HDIM + 1], qrow[pl.ds(h, 1), :]
            halves = []
            for low, high in ((0, rows // 2), (rows // 2, rows)):
                gaps = column[low:high] - row[:, :high]
                prod = jnp.exp(jnp.minimum(gaps, 0.0)) * aff_ref[low:high, :high]
                halves.append(dot(prod.astype(BF16), scaled[:high]))
            outs.append(jnp.concatenate(halves, axis=0))
        y = jnp.where(first, outs[0], outs[1]) + x * skip_ref[:, pl.ds(at, LANES)]
        y_ref[:, pl.ds(at, LANES)] = y
        z = inner_ref[:, pl.ds(at, LANES)]
        w = y * (z * sigmoid(z))
        return total + jnp.sum(w * w, axis=1, keepdims=True)

    total = lax.fori_loop(0, PAIRS_OF_HEADS, pair, jnp.zeros((rows, 1), F32), unroll=2)
    scale = lax.rsqrt(total / INNER + EPSILON)

    @pl.loop(0, PAIRS_OF_HEADS, unroll=2)
    def _(p):
        at = pl.multiple_of(p * LANES, LANES)
        z = inner_ref[:, pl.ds(at, LANES)]
        w = y_ref[:, pl.ds(at, LANES)] * (z * sigmoid(z))
        mixed = w * scale * gain_ref[:, pl.ds(at, LANES)]
        mixed_ref[:, pl.ds(at, LANES)] = mixed.astype(BF16)
        turned_ref[pl.ds(at, LANES), :] = mixed.T.astype(BF16)


def mixer_scratch(rows):
    return [
        pltpu.VMEM((rows, CONVCH), F32),
        pltpu.VMEM((PAIRS_OF_HEADS, rows, LANES), F32),
        pltpu.VMEM((HEADS, rows), F32),
        pltpu.VMEM((PAIRS_OF_HEADS, rows, LANES), F32),
        pltpu.VMEM((rows, rows), F32),
    ]


def mixer_forward(inner, taps, heads, skip, gain, position, inside):
    rows = inner.shape[0]
    shape = jax.ShapeDtypeStruct
    return pl.pallas_call(
        mixer_forward_kernel,
        out_shape=[
            shape((rows, INNER), BF16),
            shape((INNER, rows), BF16),
            shape((rows, INNER), F32),
        ],
        in_specs=[VMEM] * 7,
        out_specs=[VMEM] * 3,
        scratch_shapes=mixer_scratch(rows),
        compiler_params=BIG,
        name="mixer_forward",
    )(inner, taps, heads, skip, gain, position, inside)


def mixer_backward_steps(
    inner_ref, taps_ref, heads_ref, skip_ref, gain_ref, position_ref, inside_ref, y_ref, dmixed_ref,
    dinner_ref, dtaps_ref, dgain_ref, dskip_ref, dheads_ref,
    x_ref, qcol, qrow, dtpair, aff_ref, dx_ref, daff_ref, rowsum, stepgrad, colsum,
):
    rows = inner_ref.shape[0]
    position = position_ref[...]
    yield from mixer_setup(
        inner_ref, taps_ref, heads_ref, position, inside_ref[...], x_ref, qcol, qrow, dtpair
    )
    aff_ref[...] = (
        dot_rt_exact(x_ref[:, INNER : INNER + STATE], x_ref[:, INNER + STATE :]) * inside_ref[...].T
    )
    daff_ref[...] = jnp.zeros_like(daff_ref)
    stepgrad[...] = jnp.zeros_like(stepgrad)
    colsum[...] = jnp.zeros_like(colsum)
    lane = column_index((rows, LANES))
    first = lane < HDIM
    yield

    def sums(p, carry):
        squares, product = carry
        at = pl.multiple_of(p * LANES, LANES)
        z = inner_ref[:, pl.ds(at, LANES)]
        w = y_ref[:, pl.ds(at, LANES)] * (z * sigmoid(z))
        g = dmixed_ref[:, pl.ds(at, LANES)] * gain_ref[:, pl.ds(at, LANES)]
        return (
            squares + jnp.sum(w * w, axis=1, keepdims=True),
            product + jnp.sum(w * g, axis=1, keepdims=True),
        )

    zero = jnp.zeros((rows, 1), F32)
    squares, product = lax.fori_loop(0, PAIRS_OF_HEADS, sums, (zero, zero))
    scale = lax.rsqrt(squares / INNER + EPSILON)
    pull = scale * scale * scale * product / INNER
    yield

    def pair(p):
        at = pl.multiple_of(p * LANES, LANES)
        here = pl.ds(at, LANES)
        z = inner_ref[:, here]
        y = y_ref[:, here]
        sig = sigmoid(z)
        silu = z * sig
        w = y * silu
        g = dmixed_ref[:, here]
        dgain_ref[:, here] = jnp.sum(g * w * scale, axis=0, keepdims=True)
        dw = scale * (g * gain_ref[:, here]) - w * pull
        dinner_ref[:, here] = (dw * y * (sig * (1.0 + z * (1.0 - sig)))).astype(BF16)
        dy = dw * silu
        x = x_ref[:, here]
        dskip_ref[:, here] = jnp.sum(dy * x, axis=0, keepdims=True)
        steps = dtpair[p]
        scaled = x * steps
        low = dy.astype(BF16)
        outs = []
        columns = qcol[p]
        for k in (0, 1):
            h = 2 * p + k
            gaps = qrow[pl.ds(h, 1), :] - columns[:, k * HDIM : k * HDIM + 1]
            decay = jnp.exp(jnp.minimum(gaps, 0.0))
            prod = decay * aff_ref[...]
            own = first if k == 0 else jnp.logical_not(first)
            dprod = dot_rt(jnp.where(own, scaled, 0.0).astype(BF16), low)
            daff_ref[...] += dprod * decay
            both = dprod * prod
            rowsum[pl.ds(h, 1), :] = jnp.sum(both, axis=0, keepdims=True)
            away = jnp.sum(both, axis=1, keepdims=True)
            colsum[...] += jnp.where(lane == h, away, 0.0)
            outs.append(dot(prod.astype(BF16), low))
        dscaled = jnp.where(first, outs[0], outs[1])
        dx_ref[:, here] = dscaled * steps + dy * skip_ref[:, here]
        gain_step = dscaled * x
        left = jnp.sum(jnp.where(first, gain_step, 0.0), axis=1, keepdims=True)
        right = jnp.sum(jnp.where(first, 0.0, gain_step), axis=1, keepdims=True)
        stepgrad[...] += jnp.where(lane == 2 * p, left, 0.0) + jnp.where(
            lane == 2 * p + 1, right, 0.0
        )

    for start, end in spans(PAIRS_OF_HEADS, 6):
        pl.loop(start, end)(pair)
        yield

    daff = daff_ref[...] * inside_ref[...].T
    dx_ref[:, INNER : INNER + STATE] = dot_exact(daff, x_ref[:, INNER + STATE :])
    dx_ref[:, INNER + STATE :] = dot_exact(daff.T, x_ref[:, INNER : INNER + STATE])
    yield
    pad = jnp.zeros((LANES - HEADS, rows), F32)
    dsums = jnp.concatenate([rowsum[...], pad], axis=0).T - colsum[...]
    dlog = dot_exact(inside_ref[...].T, dsums)[:, :HEADS]
    raw, step, rates = step_sizes(inner_ref, heads_ref)
    dstep = stepgrad[:, :HEADS] + dlog * rates
    draw = dstep * sigmoid(raw)
    dinner_ref[:, INNER + CONVCH :] = draw.astype(BF16)
    dheads_ref[0:1, :HEADS] = jnp.sum(dlog * step, axis=0, keepdims=True) * rates
    dheads_ref[1:2, :HEADS] = jnp.sum(draw, axis=0, keepdims=True)
    yield

    def conv_back(k):
        here = pl.ds(pl.multiple_of(k * LANES, LANES), LANES)
        there = pl.ds(pl.multiple_of(INNER + k * LANES, LANES), LANES)
        conv_in = inner_ref[:, there]
        taps = taps_ref[:, here]
        before = conv_before(conv_in, taps, position)
        sig = sigmoid(before)
        grad = dx_ref[:, here] * (sig * (1.0 + before * (1.0 - sig)))
        back = grad * taps[TAPS - 1 : TAPS]
        dtaps_ref[TAPS - 1 : TAPS, here] = jnp.sum(grad * conv_in, axis=0, keepdims=True)
        for offset in range(1, TAPS):
            t = TAPS - 1 - offset
            valid = jnp.where(position >= offset, grad, 0.0)
            dtaps_ref[t : t + 1, here] = jnp.sum(
                valid * pltpu.roll(conv_in, offset, 0), axis=0, keepdims=True
            )
            back = back + pltpu.roll(valid, rows - offset, 0) * taps[t : t + 1]
        dinner_ref[:, there] = back.astype(BF16)

    for start, end in spans(CONVCH // LANES, 4):
        pl.loop(start, end)(conv_back)
        yield


def mixer_backward_scratch(rows):
    return mixer_scratch(rows) + [
        pltpu.VMEM((rows, CONVCH), F32),
        pltpu.VMEM((rows, rows), F32),
        pltpu.VMEM((HEADS, rows), F32),
        pltpu.VMEM((rows, LANES), F32),
        pltpu.VMEM((rows, LANES), F32),
    ]


def mixer_backward_shapes(inner, taps):
    shape = jax.ShapeDtypeStruct
    return [
        shape(inner.shape, BF16),
        shape(taps.shape, F32),
        shape((1, INNER), F32),
        shape((1, INNER), F32),
        shape((8, LANES), F32),
    ]


def rotate_rows(front, rear, cosine, sine):
    return front * cosine - rear * sine, rear * cosine + front * sine


def attention_setup(packed_ref, cosine_ref, sine_ref, query, key_rows):
    half = HD // 2
    for h in range(QH + KVH):
        at = h * HD
        turned = rotate_rows(
            packed_ref[at : at + half], packed_ref[at + half : at + HD],
            cosine_ref[...], sine_ref[...],
        )
        both = jnp.concatenate(turned, axis=0)
        if h < QH:
            query[at : at + HD] = both.astype(BF16)
        else:
            key_rows[at - QH * HD : at - (QH - 1) * HD] = both


def turned_probs(keys, query, outside):
    scores = dot(keys, query) * SCORE_SCALE + outside
    expo = jnp.exp(scores - jnp.max(scores, axis=0, keepdims=True))
    return expo / jnp.sum(expo, axis=0, keepdims=True)


def attention_forward_kernel(
    packed_ref, cosine_ref, sine_ref, outside_ref, context_ref, turned_ref, query, key_rows
):
    attention_setup(packed_ref, cosine_ref, sine_ref, query, key_rows)
    keys = key_rows[...].T.astype(BF16)
    values = packed_ref[(QH + KVH) * HD :].astype(BF16)
    for h in range(QH):
        kv = h * KVH // QH
        probs = turned_probs(
            keys[:, kv * HD : (kv + 1) * HD], query[h * HD : (h + 1) * HD], outside_ref[...]
        )
        turned = dot(values[kv * HD : (kv + 1) * HD], probs.astype(BF16))
        turned_ref[h * HD : (h + 1) * HD] = turned.astype(BF16)
    for k in range(QH * HD // LANES):
        here = slice(k * LANES, (k + 1) * LANES)
        context_ref[:, here] = turned_ref[here].astype(F32).T.astype(BF16)


def attention_forward(packed, cosine, sine, outside):
    rows = packed.shape[1]
    shape = jax.ShapeDtypeStruct
    return pl.pallas_call(
        attention_forward_kernel,
        out_shape=[shape((rows, QH * HD), BF16), shape((QH * HD, rows), BF16)],
        in_specs=[VMEM] * 4,
        out_specs=[VMEM] * 2,
        scratch_shapes=[pltpu.VMEM((QH * HD, rows), BF16), pltpu.VMEM((KVH * HD, rows), F32)],
        compiler_params=BIG,
        name="attention_forward",
    )(packed, cosine, sine, outside)


def attention_backward_steps(
    packed_ref, cosine_ref, sine_ref, outside_ref, dcontext_ref, dpacked_ref,
    query, key_rows, grad_rows,
):
    half = HD // 2
    attention_setup(packed_ref, cosine_ref, sine_ref, query, key_rows)
    low_rows = key_rows[...].astype(BF16)
    keys = key_rows[...].T.astype(BF16)
    values = packed_ref[(QH + KVH) * HD :].T.astype(BF16)
    for k in range(QH * HD // LANES):
        here = slice(k * LANES, (k + 1) * LANES)
        grad_rows[here] = dcontext_ref[:, here].astype(F32).T
    yield
    for kv in range(KVH):
        of_kv = slice(kv * HD, (kv + 1) * HD)
        dkey = jnp.zeros((HD, keys.shape[0]), F32)
        dvalue = jnp.zeros((HD, keys.shape[0]), F32)
        for h in range(kv * QH // KVH, (kv + 1) * QH // KVH):
            here = slice(h * HD, (h + 1) * HD)
            probs = turned_probs(keys[:, of_kv], query[here], outside_ref[...])
            grad = grad_rows[here].astype(BF16)
            dprobs = dot(values[:, of_kv], grad)
            dvalue = dvalue + dot_rt(grad, probs.astype(BF16))
            inner = jnp.sum(probs * dprobs, axis=0, keepdims=True)
            dscores = (probs * (dprobs - inner) * SCORE_SCALE).astype(BF16)
            dquery = dot(low_rows[of_kv], dscores)
            dkey = dkey + dot_rt(query[here], dscores)
            turned = rotate_rows(dquery[:half], dquery[half:], cosine_ref[...], -sine_ref[...])
            grad_rows[here] = jnp.concatenate(turned, axis=0)
            yield
        turned = rotate_rows(dkey[:half], dkey[half:], cosine_ref[...], -sine_ref[...])
        at = QH * HD + kv * HD
        grad_rows[at : at + HD] = jnp.concatenate(turned, axis=0)
        at = (QH + KVH) * HD + kv * HD
        grad_rows[at : at + HD] = dvalue
    for k in range((QH + 2 * KVH) * HD // LANES):
        here = slice(k * LANES, (k + 1) * LANES)
        dpacked_ref[:, here] = grad_rows[here].T.astype(BF16)
    yield


def attention_backward_scratch(rows):
    return [
        pltpu.VMEM((QH * HD, rows), BF16),
        pltpu.VMEM((KVH * HD, rows), F32),
        pltpu.VMEM(((QH + 2 * KVH) * HD, rows), F32),
    ]


def host_steps(ins, outs, scratch):
    yield from mixer_backward_steps(*ins[:9], *outs[:5], *scratch[:10])
    yield from attention_backward_steps(*ins[9:], outs[5], *scratch[10:])


def host_shapes(ins):
    rows, wide = ins[0].shape[0], ins[9].shape[0]
    return mixer_backward_shapes(ins[0], ins[1]) + [jax.ShapeDtypeStruct((rows, wide), BF16)]


def host_scratch(ins):
    rows = ins[0].shape[0]
    return mixer_backward_scratch(rows) + attention_backward_scratch(rows)


def host_plain(ins):
    shapes, scratch = host_shapes(ins), host_scratch(ins)

    def kernel(*refs):
        one, two = len(ins), len(ins) + len(shapes)
        run_steps(host_steps(refs[:one], refs[one:two], refs[two:]))

    return pl.pallas_call(
        kernel,
        out_shape=shapes,
        in_specs=[VMEM] * len(ins),
        out_specs=[VMEM] * len(shapes),
        scratch_shapes=scratch,
        compiler_params=BIG,
        name="mixer_attention_backward",
    )(*ins)


def flip(me, bit):
    step = 1 << bit
    return me + step * (1 - 2 * ((me // step) % 2))


def place(bits, free, mine, flipped=()):
    return tuple(
        slice(None) if b in free else 1 - mine[b] if b in flipped else mine[b]
        for b in reversed(range(bits))
    )


def greet(me, bits):
    barrier = pltpu.get_barrier_semaphore()
    for b in range(bits):
        pl.semaphore_signal(barrier, inc=1, device_id=(flip(me, b),), device_id_type=MESH)
    pl.semaphore_wait(barrier, bits)


def remote(me, src, dst, send, recv, bit):
    return pltpu.make_async_remote_copy(
        src_ref=src,
        dst_ref=dst,
        send_sem=send,
        recv_sem=recv,
        device_id=(flip(me, bit),),
        device_id_type=MESH,
    )


def gather_kernel(devices, chunks, events, layers, arrays, *refs):
    bits = devices.bit_length() - 1
    ins = refs[:arrays]
    outs = refs[arrays : arrays + layers * arrays]
    send_sem, recv_sem, csend_sem, crecv_sem, own_sem = refs[arrays + layers * arrays :]
    me = lax.axis_index("dp")
    mine = [(me // (1 << b)) % 2 for b in range(bits)]
    greet(me, bits)
    own, sends, cores, pending = [], [], [], {}
    for c, (l, a, order) in enumerate(chunks):
        here = outs[l * arrays + a].at[place(bits, (), mine)]
        src = ins[a].at[l]
        copy = remote(me, src, here, send_sem.at[c, 0], recv_sem.at[c, 0], order[0])
        copy.start()
        pending[c] = copy
        sends.append(copy)
        local = pltpu.make_async_copy(src, here, own_sem.at[c])
        local.start()
        own.append(local)
    for c, (l, a, order) in enumerate(chunks):
        here = outs[l * arrays + a].at[place(bits, (), mine)]
        copy = remote(me, ins[a].at[l], here, csend_sem.at[c, 0], crecv_sem.at[c, 0], 0)
        copy.start()
        sends.append(copy)
        cores.append(copy)
    for local in own:
        local.wait()
    for c, s in events:
        l, a, order = chunks[c]
        full = outs[l * arrays + a]
        pending[c].wait_recv()
        if s + 1 < bits - 1:
            view = full.at[place(bits, order[: s + 1], mine)]
            copy = remote(
                me, view, view, send_sem.at[c, s + 1], recv_sem.at[c, s + 1], order[s + 1]
            )
            copy.start()
            pending[c] = copy
            sends.append(copy)
        new = full.at[place(bits, order[:s], mine, (order[s],))]
        copy = remote(me, new, new, csend_sem.at[c, s + 1], crecv_sem.at[c, s + 1], 0)
        copy.start()
        sends.append(copy)
        cores.append(copy)
    for copy in sends:
        copy.wait_send()
    for copy in cores:
        copy.wait_recv()


def gather_all(shards, devices):
    bits = devices.bit_length() - 1
    layers = shards[0].shape[0]
    n = len(AG_CHUNKS)
    sent = {(layer, a) for layer, a, _ in AG_CHUNKS}
    outs = [
        jax.ShapeDtypeStruct(
            (2,) * bits + (s.shape[1:] if (layer, a) in sent else (8, 128)), s.dtype
        )
        for layer in range(layers)
        for a, s in enumerate(shards)
    ]
    res = pl.pallas_call(
        functools.partial(gather_kernel, devices, AG_CHUNKS, AG_EVENTS, layers, len(shards)),
        out_shape=outs,
        in_specs=[pl.BlockSpec(memory_space=pltpu.VMEM)] * len(shards),
        out_specs=[pl.BlockSpec(memory_space=pl.ANY)] * len(outs),
        scratch_shapes=[pltpu.SemaphoreType.DMA((n, bits - 1))] * 2
        + [pltpu.SemaphoreType.DMA((n, bits))] * 2
        + [pltpu.SemaphoreType.DMA((n,))],
        compiler_params=pltpu.CompilerParams(collective_id=0, has_side_effects=True),
        name="gather_all",
    )(*shards)
    full = [r.reshape((devices * r.shape[-2], r.shape[-1])) for r in res]
    return [full[l * len(shards) : (l + 1) * len(shards)] for l in range(layers)]


PAIRS = ((0, 0), (1, 2), (0, 1), (2, 2), (3, 3), (4, 4))


def take(refs, *sizes):
    groups, at = [], 0
    for size in sizes:
        groups.append(refs[at : at + size])
        at += size
    return groups + [refs[at:]]


def scatter_kernel(devices, plan, jobs, arrs, counts, *refs):
    chunks, events, row_bits = plan
    bits = devices.bit_length() - 1
    half = devices // 2
    nx, ny, nsmall, nrows, nhost, nhost_out = counts
    na, nc = len(arrs), len(chunks)
    xs, ys, small_in, rows_in, host_in, refs = take(refs, nx, ny, nsmall, nrows, nhost)
    outs, small_out, rows_out, host_out, refs = take(refs, na, nsmall, nrows, nhost_out)
    xr, yr, sums, parts, refs = take(refs, nx, ny, nc, nc * (bits - 1))
    small_mid, small_got, rows_got, refs = take(
        refs, nsmall * (bits - 1), nsmall * bits, nrows * bits
    )
    host_scratch_refs, sems = refs[:-10], refs[-10:]
    xs_s, xs_r, ys_s, ys_r, st_s, st_r, sm_s, sm_r, ro_s, ro_r = sems
    me = lax.axis_index("dp")
    mine = [(me // (1 << b)) % 2 for b in range(bits)]
    greet(me, bits)
    core = mine[0]
    swaps_x, swaps_y, got_x, got_y = {}, {}, set(), set()
    for a, _, _, _ in chunks:
        xi, yi = jobs[a]
        if xi not in swaps_x:
            swaps_x[xi] = remote(
                me, xs[xi].at[:, 1 - core], xr[xi], xs_s.at[xi], xs_r.at[xi], 0
            )
            swaps_x[xi].start()
        if yi not in swaps_y:
            swaps_y[yi] = remote(me, ys[yi], yr[yi], ys_s.at[yi], ys_r.at[yi], 0)
            swaps_y[yi].start()
    sends, pending = [], {}

    def small_send(s):
        src = small_in[0] if s == 0 else small_mid[s - 1]
        copy = remote(me, src, small_got[s], sm_s.at[s], sm_r.at[s], s)
        copy.start()
        pending["small"] = copy
        sends.append(copy)

    def small_receive(s):
        src = small_in[0] if s == 0 else small_mid[s - 1]
        pending["small"].wait_recv()
        total = src[...] + small_got[s][...]
        if s + 1 < bits:
            small_mid[s][...] = total
            small_send(s + 1)
        else:
            small_out[0][...] = total

    def rows_send(s):
        bit = row_bits[s]
        index = tuple(1 - mine[q] if q == bit else slice(None) for q in reversed(range(bits)))
        copy = remote(me, rows_out[0].at[index], rows_got[s], ro_s.at[s], ro_r.at[s], bit)
        copy.start()
        pending["rows"] = copy

    def rows_receive(s):
        pending["rows"].wait_send()
        pending["rows"].wait_recv()

        @pl.loop(0, 1 << (bits - 1))
        def _(j):
            here, there, pos = [], [], bits - 1
            for q in reversed(range(bits)):
                if q == row_bits[s]:
                    here.append(1 - mine[q])
                else:
                    pos -= 1
                    value = (j // (1 << pos)) % 2
                    here.append(value)
                    there.append(value)
            rows_out[0][tuple(here)] = rows_got[s][tuple(there)]

        if s + 1 < bits:
            rows_send(s + 1)

    def send(c, s):
        order = chunks[c][3]
        index = tuple(
            1 - mine[q] if q == order[s] else mine[q] if q in order[:s] else slice(None)
            for q in reversed(range(1, bits))
        )
        copy = remote(
            me,
            sums[c].at[index],
            parts[c * (bits - 1) + s],
            st_s.at[c, s],
            st_r.at[c, s],
            order[s],
        )
        copy.start()
        pending[c] = copy
        sends.append(copy)

    def compute(c):
        a, first, end, _ = chunks[c]
        xi, yi = jobs[a]
        rows = arrs[a][0]
        if xi not in got_x:
            swaps_x[xi].wait_recv()
            got_x.add(xi)
        if yi not in got_y:
            swaps_y[yi].wait_recv()
            got_y.add(yi)

        def tile(start, width, offset):
            left = xs[xi][:, core].reshape(half * rows, -1)
            other = xr[xi][...].reshape(half * rows, -1)
            value = dot(left, ys[yi][:, pl.ds(start, width)])
            value = value + dot(other, yr[yi][:, pl.ds(start, width)])
            sums[c][..., pl.ds(offset, width)] = value.astype(BF16).reshape(
                (2,) * (bits - 1) + (rows, width)
            )

        width, step = end - first, 256
        whole = width // step

        @pl.loop(0, whole)
        def _(i):
            tile(
                pl.multiple_of(first + i * step, 128), step, pl.multiple_of(i * step, 128)
            )

        if width % step:
            tile(first + whole * step, width % step, whole * step)
        send(c, 0)

    def receive(c, s):
        a, first, end, order = chunks[c]
        pending[c].wait_recv()
        fixed = order[: s + 1]
        free = [q for q in reversed(range(1, bits)) if q not in fixed]

        def add(j, last):
            here, there, pos = [], [], len(free)
            for q in reversed(range(1, bits)):
                if q in fixed:
                    here.append(mine[q])
                else:
                    pos -= 1
                    value = (j // (1 << pos)) % 2
                    here.append(value)
                    there.append(value)
            part = parts[c * (bits - 1) + s]
            total = part[tuple(there)].astype(F32) + sums[c][tuple(here)].astype(F32)
            if last:
                outs[a][:, first:end] = total
            else:
                sums[c][tuple(here)] = total.astype(BF16)

        if not free:
            add(0, True)
        else:

            @pl.loop(0, 1 << len(free))
            def _(j):
                add(j, False)

            send(c, s + 1)

    steps = host_steps(host_in, host_out, host_scratch_refs) if nhost else iter(())
    if nsmall:
        small_send(0)
    if nrows:
        fetch = pltpu.make_async_copy(rows_in[0], rows_out[0], ro_s.at[0])
        fetch.start()
        fetch.wait()
        rows_send(0)
    for c, s in events:
        if c == -1:
            small_receive(s)
        elif c == -2:
            rows_receive(s)
        elif c == -3:
            next(steps, None)
        elif s < 0:
            compute(c)
        else:
            receive(c, s)
    run_steps(steps)
    for copy in list(swaps_x.values()) + list(swaps_y.values()) + sends:
        copy.wait_send()


def scatter(plan, jobs, turned, grads, devices, number, small=None, rows=None, host=()):
    chunks = plan[0]
    bits = devices.bit_length() - 1
    nx, ny = len(turned), len(grads)
    half = devices // 2
    split = [x.reshape(half, 2, x.shape[0] // devices, x.shape[1]) for x in turned]
    arrs = [(turned[xi].shape[0] // devices, grads[yi].shape[1]) for xi, yi in jobs]
    smalls = [] if small is None else [small]
    moved = []
    if rows is not None:
        moved.append(rows.reshape((2,) * bits + (rows.shape[0] // devices, rows.shape[1])))
    shape = jax.ShapeDtypeStruct
    extra = host_shapes(host) if host else []
    outs = [shape(size, F32) for size in arrs] + [shape(x.shape, F32) for x in smalls]
    outs += [shape(x.shape, BF16) for x in moved] + extra
    scratch = [pltpu.VMEM((half, x.shape[0] // devices, x.shape[1]), BF16) for x in turned]
    scratch += [pltpu.VMEM(y.shape, BF16) for y in grads]
    for a, first, end, _ in chunks:
        scratch.append(pltpu.VMEM((2,) * (bits - 1) + (arrs[a][0], end - first), BF16))
    for a, first, end, _ in chunks:
        for s in range(bits - 1):
            scratch.append(pltpu.VMEM((2,) * (bits - 2 - s) + (arrs[a][0], end - first), BF16))
    for x in smalls:
        scratch += [pltpu.VMEM(x.shape, F32)] * (2 * bits - 1)
    for x in moved:
        scratch += [pltpu.VMEM(x.shape[1:], BF16)] * bits
    if host:
        scratch += host_scratch(host)
    dma = pltpu.SemaphoreType.DMA
    scratch += [dma((nx,))] * 2 + [dma((ny,))] * 2 + [dma((len(chunks), bits - 1))] * 2
    scratch += [dma((bits,))] * 4
    counts = (nx, ny, len(smalls), len(moved), len(host), len(extra))
    res = pl.pallas_call(
        functools.partial(scatter_kernel, devices, plan, jobs, arrs, counts),
        out_shape=outs,
        in_specs=[VMEM] * (nx + ny + len(smalls))
        + [pl.BlockSpec(memory_space=pl.ANY)] * len(moved)
        + [VMEM] * len(host),
        out_specs=[VMEM] * len(outs),
        scratch_shapes=scratch,
        compiler_params=pltpu.CompilerParams(
            collective_id=number, has_side_effects=True, vmem_limit_bytes=67043328
        ),
        name="scatter",
    )(*split, *grads, *smalls, *moved, *host)
    owned, small_total, back, own_work = take(res, len(arrs), len(smalls), len(moved))
    return owned, small_total, [x.reshape(rows.shape) for x in back], own_work


def scatter_plain(turned, grads, small):
    owned = [
        lax.psum_scatter(
            dot(turned[xi], grads[yi]).astype(BF16), "dp", scatter_dimension=0, tiled=True
        ).astype(F32)
        for xi, yi in PAIRS
    ]
    return owned + [lax.psum(small, "dp")]


def doc_layout(doc_lengths, rows_count):
    rows_index = jnp.arange(rows_count, dtype=jnp.int32)
    doc_ends = jnp.cumsum(doc_lengths, dtype=jnp.int32)
    later = (rows_index[:, None] >= doc_ends[None, :]).astype(jnp.int32)
    segment = jnp.sum(later, axis=1, dtype=jnp.int32)
    position = rows_index - jnp.sum(later * doc_lengths[None, :], axis=1, dtype=jnp.int32)
    return (segment, position)


def inverse_rms(values):
    return lax.rsqrt(jnp.mean(values * values, axis=-1, keepdims=True) + EPSILON)


def norm_backward(grad, values, scale, gain):
    normed = values * scale
    grad_gain = jnp.sum(grad * normed, axis=0)
    inner = grad * gain
    return scale * (inner - normed * jnp.mean(inner * normed, axis=-1, keepdims=True)), grad_gain


def layer_forward(hidden, weights, small, layout):
    w_in, w_mix, w_qkv, w_attn, w_gate_up, w_down = weights
    gains, taps, gain_inner, heads, skip = small
    position, inside, outside, cosine, sine = layout
    scale = inverse_rms(hidden)
    normed = (hidden * scale * gains[0]).astype(BF16)
    inner = dot(normed, w_in)
    packed = lax.dot_general(
        w_qkv, normed, (((0,), (1,)), ((), ())), preferred_element_type=F32
    )
    mixed, mixed_rows, y = mixer_forward(inner, taps, heads, skip, gain_inner, position, inside)
    context, context_rows = attention_forward(packed, cosine, sine, outside)
    middle = hidden + dot(mixed, w_mix) + dot(context, w_attn)
    scale_two = inverse_rms(middle)
    normed_two = (middle * scale_two * gains[1]).astype(BF16)
    both = dot(normed_two, w_gate_up)
    active = (jax.nn.silu(both[:, :FF]) * both[:, FF:]).astype(BF16)
    out = middle + dot(active, w_down)
    turned = [normed.T, mixed_rows, context_rows, normed_two.T, active.T]
    return out, (hidden, scale, inner, packed, y, middle, scale_two, both, turned)


def backward_start(grad, kept, weights, small, layout):
    w_in, w_mix, w_qkv, w_attn, w_gate_up, w_down = weights
    gains, taps, gain_inner, heads, skip = small
    position, inside, outside, cosine, sine = layout
    hidden, scale, inner, packed, y, middle, scale_two, both, turned = kept
    ddown = grad.astype(BF16)
    dactive = dot_rt(ddown, w_down)
    gate, up = both[:, :FF], both[:, FF:]
    sig = jax.nn.sigmoid(gate)
    dgate = dactive * up * (sig * (1.0 + gate * (1.0 - sig)))
    dboth = jnp.concatenate([dgate, dactive * (gate * sig)], axis=1).astype(BF16)
    dmiddle, dgain_two = norm_backward(dot_rt(dboth, w_gate_up), middle, scale_two, gains[1])
    dmiddle = grad + dmiddle
    dbranch = dmiddle.astype(BF16)
    dmixed = dot_rt(dbranch, w_mix)
    dcontext = dot_rt(dbranch, w_attn).astype(BF16)
    host = (inner, taps, heads, skip, gain_inner, position, inside, y, dmixed)
    host += (packed, cosine, sine, outside, dcontext)
    return dmiddle, dgain_two, dbranch, dboth, ddown, host


def backward_end(dmiddle, dgain_two, kept, weights, small, done):
    w_in, w_qkv = weights[0], weights[2]
    hidden, scale = kept[:2]
    dinner, dtaps, dgain_inner, dskip, dheads, dpacked = done
    dnormed = dot_rt(dinner, w_in) + dot_rt(dpacked, w_qkv)
    dhidden, dgain = norm_backward(dnormed, hidden, scale, small[0][0])
    flat = [dgain, dgain_two, dtaps.reshape(-1), dgain_inner[0], dheads[0, :HEADS]]
    flat += [jnp.sum(dskip.reshape(HEADS, HDIM), axis=1), dheads[1, :HEADS]]
    flat = jnp.concatenate(flat)
    lines = -(-flat.shape[0] // 1024) * 8
    small_sum = jnp.pad(flat, (0, lines * 128 - flat.shape[0])).reshape(lines, 128)
    return dmiddle + dhidden, small_sum


def shards(
    tokens,
    cotangent,
    destination,
    lengths,
    norm_gains,
    in_proj,
    conv_weight,
    ssm_gain,
    mixer_out,
    qkv_proj,
    attn_out,
    gate_up,
    down_proj,
    a_log,
    d_skip,
    dt_bias,
):
    devices = lax.axis_size("dp")
    me = lax.axis_index("dp")
    rows_here, width = tokens.shape
    share = rows_here // devices
    own_kernels = devices == 32
    index = jnp.arange(rows_here, dtype=jnp.int32)
    slabs = destination.reshape(devices, rows_here)

    own = lax.dynamic_slice_in_dim(slabs, me, 1, 0)[0] // rows_here
    same = (own[:, None] == own[None, :]) & (index[None, :] < index[:, None])
    slot = own * share + jnp.sum(same.astype(jnp.int32), axis=1)
    leave = (slot[None, :] == index[:, None]).astype(BF16)
    outgoing = [dot(leave, x).astype(BF16) for x in (tokens, cotangent)]

    def exchange(rows):
        split = rows.reshape(devices, share, width)
        moved = lax.all_to_all(split, "dp", split_axis=0, concat_axis=0, tiled=True)
        return moved.reshape(rows_here, width)

    arrived = [exchange(x) for x in outgoing]

    local = slabs - me * rows_here
    mask = ((local >= 0) & (local < rows_here)).astype(BF16)
    below = (index[:, None] < index[None, :]).astype(BF16)
    rank = dot(mask, below).astype(jnp.int32)
    order = rank + share * jnp.arange(devices, dtype=jnp.int32)[:, None]
    hits = local.reshape(-1)[None, :] == index[:, None]
    taken = jnp.sum(jnp.where(hits, order.reshape(-1)[None, :], 0), axis=1)
    enter = (taken[:, None] == index[None, :]).astype(BF16)
    hidden = dot(enter, arrived[0])
    upstream = dot(enter, arrived[1])

    segment, position = doc_layout(lengths[0], rows_here)
    inside = (segment[:, None] == segment[None, :]) & (index[:, None] >= index[None, :])
    inverse = ROPE_BASE ** (-(jnp.arange(HD // 2, dtype=F32) * 2.0 / HD))
    angles = position.astype(F32)[:, None] * inverse[None, :]
    outside = jnp.where(inside.T, 0.0, -1e30)
    layout = (position[:, None], inside.astype(F32), outside, jnp.cos(angles).T, jnp.sin(angles).T)

    matrices = (in_proj, mixer_out, qkv_proj, attn_out, gate_up, down_proj)
    gain_part, conv_part, inner_part = (x.shape[-1] for x in (norm_gains, conv_weight, ssm_gain))
    packed = jnp.concatenate(
        [norm_gains.reshape(LAYERS, -1), conv_weight.reshape(LAYERS, -1), ssm_gain], axis=1
    )
    used = packed.shape[1]
    if own_kernels:
        room = SMALL_ROWS * 128
        padded = jnp.pad(packed, ((0, 0), (0, room - used))).reshape(LAYERS, SMALL_ROWS, 128)
        gathered = gather_all(list(matrices) + [padded], devices)
        weights = [g[:-1] for g in gathered]
        late = LATE_ARRAY
        tied = matrices[late][1] + gathered[0][-1][:1, :1] * 0
        weights[1][late] = lax.all_gather(tied, "dp", axis=0, tiled=True)
        smalls = [g[-1].reshape(devices, room)[:, :used] for g in gathered]
    else:
        weights = [
            [lax.all_gather(x[layer], "dp", axis=0, tiled=True) for x in matrices]
            for layer in range(LAYERS)
        ]
        every = lax.all_gather(packed, "dp", axis=0)
        smalls = [every[:, layer] for layer in range(LAYERS)]

    def spread(piece, count):
        shaped = piece.reshape(devices, count, -1)
        return jnp.swapaxes(shaped, 0, 1).reshape(count, -1).astype(F32)

    def small_of(layer):
        both = smalls[layer]
        mid = 2 * gain_part
        heads = jnp.stack([a_log[layer], d_skip[layer], dt_bias[layer]])
        return (
            spread(both[:, :mid], 2),
            spread(both[:, mid : mid + TAPS * conv_part], TAPS),
            spread(both[:, mid + TAPS * conv_part :], 1),
            jnp.pad(heads, ((0, 5), (0, LANES - HEADS))),
            jnp.repeat(d_skip[layer], HDIM)[None],
        )

    params = [small_of(layer) for layer in range(LAYERS)]

    kept = [None] * LAYERS
    for layer in range(LAYERS):
        hidden, kept[layer] = layer_forward(hidden, weights[layer], params[layer], layout)

    def permute_back(choice, rows):
        return lax.dot_general(
            choice, rows.astype(BF16), (((0,), (0,)), ((), ())), preferred_element_type=F32
        )

    top, low = 1, 0
    start = backward_start(upstream, kept[top], weights[top], params[top], layout)
    dmiddle, dgain_two, dbranch, dboth, ddown, host = start
    if own_kernels:
        up_down, _, _, done = scatter(
            PLAN_A, ((0, 0), (1, 1)), kept[top][-1][3:], [dboth, ddown], devices, 1, host=host
        )
    else:
        done = host_plain(host)
    flowing, small_top = backward_end(
        dmiddle, dgain_two, kept[top], weights[top], params[top], done
    )
    turned_top = kept[top][-1]
    grads_top = [done[0], done[5], dbranch, dboth, ddown]

    start = backward_start(flowing, kept[low], weights[low], params[low], layout)
    dmiddle, dgain_two, dbranch, dboth, ddown, host = start
    leaving = permute_back(enter, hidden).astype(BF16)
    turned_low = kept[low][-1]
    if own_kernels:
        second, sum_top, home, done = scatter(
            PLAN_B,
            ((0, 0), (1, 2), (0, 1), (2, 2), (3, 3), (4, 4)),
            turned_top[:3] + turned_low[3:],
            grads_top[:3] + [dboth, ddown],
            devices,
            2,
            small=small_top,
            rows=leaving,
            host=host,
        )
    else:
        done = host_plain(host)
    flowing, small_low = backward_end(
        dmiddle, dgain_two, kept[low], weights[low], params[low], done
    )
    grads_low = [done[0], done[5], dbranch, dboth, ddown]
    leaving_grad = permute_back(enter, flowing).astype(BF16)
    if own_kernels:
        third, sum_low, home_grad, _ = scatter(
            PLAN_C,
            ((0, 0), (1, 2), (0, 1), (2, 2)),
            turned_low[:3],
            grads_low[:3],
            devices,
            3,
            small=small_low,
            rows=leaving_grad,
        )
        home, home_grad = home[0], home_grad[0]
        owned = [third + second[4:] + sum_low, second[:4] + up_down + sum_top]
    else:
        owned = [
            scatter_plain(turned_low, grads_low, small_low),
            scatter_plain(turned_top, grads_top, small_top),
        ]
        home, home_grad = exchange(leaving), exchange(leaving_grad)
    out_tokens = permute_back(leave, home).astype(BF16)
    in_grad = permute_back(leave, home_grad)

    big = [jnp.stack([owned[layer][k] for layer in range(LAYERS)]) for k in range(6)]
    totals = jnp.stack([owned[layer][6].reshape(-1) for layer in range(LAYERS)])
    model = gain_part * devices
    sizes = (2 * model, TAPS * CONVCH, INNER, HEADS, HEADS, HEADS)
    pieces, at = [], 0
    for size in sizes:
        pieces.append(totals[:, at : at + size])
        at += size

    def mine(piece, count, part):
        shaped = piece.reshape(LAYERS, count, devices * part)
        return lax.dynamic_slice_in_dim(shaped, me * part, part, 2)

    return (
        out_tokens,
        in_grad,
        mine(pieces[0], 2, gain_part),
        big[0],
        mine(pieces[1], TAPS, conv_part),
        mine(pieces[2], 1, inner_part)[:, 0],
        big[1],
        big[2],
        big[3],
        big[4],
        big[5],
        pieces[3],
        pieces[4],
        pieces[5],
    )


def solution(mesh):
    placed = (
        P("dp", None),
        P("dp", None),
        P(),
        P("dp", None),
        P(None, None, "dp"),
        P(None, "dp", None),
        P(None, None, "dp"),
        P(None, "dp"),
        P(None, "dp", None),
        P(None, "dp", None),
        P(None, "dp", None),
        P(None, "dp", None),
        P(None, "dp", None),
        P(),
        P(),
        P(),
    )
    return jax.shard_map(
        shards,
        mesh=mesh,
        in_specs=placed,
        out_specs=(
            P("dp", None),
            P("dp", None),
            P(None, None, "dp"),
            P(None, "dp", None),
            P(None, None, "dp"),
            P(None, "dp"),
            P(None, "dp", None),
            P(None, "dp", None),
            P(None, "dp", None),
            P(None, "dp", None),
            P(None, "dp", None),
            P(),
            P(),
            P(),
        ),
        check_vma=False,
    )
```

```python
import functools

import jax
import jax.numpy as jnp
from jax import lax
from jax.experimental import pallas as pl
from jax.experimental.pallas import tpu as pltpu
from jax.sharding import PartitionSpec as P

FF = 2048
HEADS = 24
HDIM = 64
STATE = 128
QH = 8
KVH = 2
HD = 64
LAYERS = 2
INNER = 1536
CONVCH = 1792
TAPS = 4
EPSILON = 1e-05
ROPE_BASE = 100000000000.0
SCORE_SCALE = 0.125
HIGHEST = lax.Precision.HIGHEST
F32 = jnp.float32
BF16 = jnp.bfloat16
MESH = pl.DeviceIdType.MESH

AG_CHUNKS = [(0, 6, (4, 3, 2, 1)), (1, 6, (4, 3, 2, 1)), (1, 0, (4, 3, 1, 2)), (1, 3, (4, 3, 2, 1)), (1, 2, (4, 3, 2, 1)), (0, 2, (4, 3, 2, 1)), (1, 5, (4, 3, 2, 1)), (0, 0, (4, 3, 1, 2)), (0, 3, (1, 4, 3, 2)), (0, 5, (4, 3, 2, 1)), (0, 4, (1, 2, 4, 3)), (0, 1, (1, 2, 4, 3)), (1, 1, (4, 3, 2, 1))]
AG_EVENTS = [(0, 0), (1, 0), (8, 0), (-2, 0), (10, 0), (11, 0), (2, 0), (3, 0), (4, 0), (-2, 1), (5, 0), (6, 0), (10, 1), (0, 1), (1, 1), (11, 1), (7, 0), (-2, 2), (0, 2), (1, 2), (0, 3), (2, 1), (1, 3), (9, 0), (3, 1), (4, 1), (12, 0), (5, 1), (8, 1), (3, 2), (6, 1), (4, 2), (5, 2), (2, 2), (6, 2), (3, 3), (4, 3), (5, 3), (7, 1), (10, 2), (9, 1), (2, 3), (6, 3), (12, 1), (11, 2), (8, 2), (9, 2), (-2, 3), (-2, 4), (7, 2), (12, 2), (8, 3), (9, 3), (10, 3), (12, 3), (7, 3), (11, 3)]
AG_ROW_BITS = (3, 1, 2, 4, 0)
PLAN_B = ([(3, 0, 1024, (2, 3, 1, 4)), (0, 0, 1664, (1, 3, 4, 2)), (0, 1664, 3352, (2, 1, 3, 4)), (4, 0, 1408, (2, 1, 3, 4)), (1, 0, 512, (2, 3, 1, 4)), (5, 512, 1024, (1, 3, 2, 4)), (2, 0, 768, (3, 2, 1, 4)), (4, 2688, 4096, (2, 1, 3, 4)), (4, 1408, 2688, (1, 3, 2, 4)), (5, 0, 512, (2, 1, 3, 4)), (1, 512, 1024, (2, 1, 3, 4))], [(0, -1), (1, -1), (2, -1), (3, -1), (4, -1), (5, -1), (6, -1), (7, -1), (8, -1), (9, -1), (10, -1), (-1, 0), (0, 0), (-2, 0), (-3, 0), (-3, 0), (-3, 0), (-3, 0), (-3, 0), (-3, 0), (-3, 0), (-3, 0), (6, 0), (1, 0), (0, 1), (-3, 0), (2, 0), (-3, 0), (-2, 1), (-3, 0), (-2, 2), (5, 0), (-3, 0), (-3, 0), (1, 1), (-3, 0), (-3, 0), (3, 0), (-3, 0), (-3, 0), (5, 1), (-3, 0), (-3, 0), (-3, 0), (8, 0), (-3, 0), (-1, 1), (-3, 0), (-3, 0), (0, 2), (4, 0), (-3, 0), (-3, 0), (-3, 0), (-3, 0), (-3, 0), (-3, 0), (-3, 0), (1, 2), (2, 1), (8, 1), (0, 3), (7, 0), (4, 1), (3, 1), (2, 2), (3, 2), (9, 0), (7, 1), (4, 2), (2, 3), (3, 3), (10, 0), (9, 1), (7, 2), (6, 1), (4, 3), (9, 2), (10, 1), (6, 2), (-2, 3), (7, 3), (5, 2), (-1, 2), (9, 3), (10, 2), (1, 3), (6, 3), (-2, 4), (8, 2), (-1, 3), (5, 3), (10, 3), (8, 3), (-1, 4)], (4, 3, 0, 2, 1))
PLAN_C = ([(0, 0, 896, (1, 2, 3, 4)), (3, 0, 512, (2, 3, 1, 4)), (0, 1664, 2560, (1, 2, 3, 4)), (1, 512, 1024, (2, 3, 4, 1)), (1, 0, 512, (1, 2, 3, 4)), (0, 2560, 3352, (1, 2, 3, 4)), (0, 896, 1664, (2, 3, 1, 4)), (2, 0, 384, (1, 2, 3, 4)), (2, 384, 768, (3, 1, 2, 4)), (3, 512, 1024, (1, 2, 3, 4))], [(0, -1), (1, -1), (2, -1), (3, -1), (4, -1), (5, -1), (6, -1), (7, -1), (8, -1), (9, -1), (-1, 0), (1, 0), (0, 0), (-2, 0), (3, 0), (-2, 1), (8, 0), (1, 1), (2, 0), (3, 1), (6, 0), (0, 1), (-2, 2), (4, 0), (2, 1), (3, 2), (6, 1), (4, 1), (0, 2), (5, 0), (2, 2), (7, 0), (4, 2), (9, 0), (0, 3), (5, 1), (-1, 1), (7, 1), (8, 1), (2, 3), (1, 2), (9, 1), (4, 3), (-1, 2), (5, 2), (8, 2), (7, 2), (9, 2), (1, 3), (-2, 3), (-1, 3), (3, 3), (6, 2), (5, 3), (8, 3), (7, 3), (9, 3), (-1, 4), (-2, 4), (6, 3)], (4, 0, 3, 1, 2))
PLAN_A = ([(1, 0, 256, (2, 1, 3, 4)), (1, 768, 1024, (3, 4, 1, 2)), (0, 0, 1024, (1, 2, 3, 4)), (0, 2048, 3072, (2, 3, 4, 1)), (0, 3072, 4096, (3, 4, 1, 2)), (0, 1024, 2048, (1, 2, 3, 4)), (1, 256, 512, (1, 2, 3, 4)), (1, 512, 768, (2, 1, 3, 4))], [(0, -1), (1, -1), (2, -1), (3, -1), (4, -1), (5, -1), (6, -1), (7, -1), (-3, 0), (0, 0), (1, 0), (-3, 0), (-3, 0), (-3, 0), (-3, 0), (-3, 0), (-3, 0), (-3, 0), (2, 0), (-3, 0), (1, 1), (3, 0), (4, 0), (-3, 0), (-3, 0), (7, 0), (-3, 0), (5, 0), (3, 1), (-3, 0), (2, 1), (-3, 0), (6, 0), (-3, 0), (-3, 0), (0, 1), (4, 1), (-3, 0), (5, 1), (1, 2), (-3, 0), (-3, 0), (7, 1), (6, 1), (2, 2), (-3, 0), (0, 2), (3, 2), (-3, 0), (1, 3), (-3, 0), (4, 2), (-3, 0), (-3, 0), (5, 2), (-3, 0), (-3, 0), (7, 2), (-3, 0), (-3, 0), (3, 3), (-3, 0), (6, 2), (2, 3), (-3, 0), (4, 3), (0, 3), (5, 3), (7, 3), (6, 3)], (1, 2, 3, 4, 0))

SMALL_ROWS = 16
LATE_ARRAY = 4


def dot(left, right):
    return jnp.dot(left, right, preferred_element_type=F32)


def dot_rt(left, right):
    return lax.dot_general(left, right, (((1,), (1,)), ((), ())), preferred_element_type=F32)


PAIRS_OF_HEADS = HEADS // 2
LANES = 128
VMEM = pl.BlockSpec(memory_space=pltpu.VMEM)
BIG = pltpu.CompilerParams(vmem_limit_bytes=56 * 1024 * 1024)


def dot_exact(left, right):
    return jnp.dot(left, right, preferred_element_type=F32, precision=HIGHEST)


def dot_rt_exact(left, right):
    return lax.dot_general(
        left, right, (((1,), (1,)), ((), ())), preferred_element_type=F32, precision=HIGHEST
    )


def sigmoid(x):
    return 1.0 / (1.0 + jnp.exp(-x))


def column_index(shape):
    return lax.broadcasted_iota(jnp.int32, shape, len(shape) - 1)


def shifted_down(values, offset, position):
    return jnp.where(position >= offset, pltpu.roll(values, offset, 0), 0.0)


def conv_before(conv_in, taps, position):
    total = conv_in * taps[TAPS - 1 : TAPS]
    for offset in range(1, TAPS):
        total = total + shifted_down(conv_in, offset, position) * taps[
            TAPS - 1 - offset : TAPS - offset
        ]
    return total


def spans(count, parts):
    edges = [count * k // parts for k in range(parts + 1)]
    return list(zip(edges[:-1], edges[1:]))


def run_steps(steps):
    for _ in steps:
        pass


def step_sizes(inner_ref, heads_ref):
    raw = inner_ref[:, INNER + CONVCH :] + heads_ref[2:3, :HEADS]
    step = jnp.maximum(raw, 0.0) + jnp.log1p(jnp.exp(-jnp.abs(raw)))
    return raw, step, -jnp.exp(heads_ref[0:1, :HEADS])


def mixer_setup(
    inner_ref, taps_ref, heads_ref, position, inside, x_ref, qcol, qrow, dtpair, unroll=1
):
    rows = inner_ref.shape[0]
    for start, end in spans(CONVCH // LANES, 2):

        @pl.loop(start, end, unroll=unroll)
        def _(k):
            at = pl.multiple_of(k * LANES, LANES)
            before = conv_before(
                inner_ref[:, pl.ds(pl.multiple_of(INNER + at, LANES), LANES)],
                taps_ref[:, pl.ds(at, LANES)],
                position,
            )
            x_ref[:, pl.ds(at, LANES)] = before * sigmoid(before)

        yield

    raw, step, rates = step_sizes(inner_ref, heads_ref)
    sums = dot_exact(inside, step * rates)
    wide = jnp.concatenate([sums, jnp.zeros((rows, LANES - HEADS), F32)], axis=1)
    qrow[...] = wide.T[: qrow.shape[0]]
    first = column_index((rows, LANES)) < HDIM
    yield
    for p in range(PAIRS_OF_HEADS):
        for source, target in ((sums, qcol), (step, dtpair)):
            both = [
                jnp.broadcast_to(source[:, h : h + 1], (rows, LANES)) for h in (2 * p, 2 * p + 1)
            ]
            target[p] = jnp.where(first, both[0], both[1])
        if p % 4 == 3:
            yield


def mixer_forward_kernel(
    inner_ref, taps_ref, heads_ref, skip_ref, gain_ref, position_ref, inside_ref,
    mixed_ref, turned_ref, y_ref, x_ref, qcol, qrow, dtpair, aff_ref,
):
    rows = inner_ref.shape[0]
    position = position_ref[...]
    inside = inside_ref[...]
    run_steps(
        mixer_setup(
            inner_ref, taps_ref, heads_ref, position, inside, x_ref, qcol, qrow, dtpair, unroll=7
        )
    )
    b_all = x_ref[:, INNER : INNER + STATE]
    c_all = x_ref[:, INNER + STATE :]
    aff_ref[...] = dot_rt_exact(c_all, b_all) * inside
    first = column_index((rows, LANES)) < HDIM

    def pair(p, total):
        at = pl.multiple_of(p * LANES, LANES)
        x = x_ref[:, pl.ds(at, LANES)]
        scaled = (x * dtpair[p]).astype(BF16)
        outs = []
        columns = qcol[p]
        for k in (0, 1):
            h = 2 * p + k
            column, row = columns[:, k * HDIM : k * HDIM + 1], qrow[pl.ds(h, 1), :]
            halves = []
            for low, high in ((0, rows // 2), (rows // 2, rows)):
                gaps = column[low:high] - row[:, :high]
                prod = jnp.exp(jnp.minimum(gaps, 0.0)) * aff_ref[low:high, :high]
                halves.append(dot(prod.astype(BF16), scaled[:high]))
            outs.append(jnp.concatenate(halves, axis=0))
        y = jnp.where(first, outs[0], outs[1]) + x * skip_ref[:, pl.ds(at, LANES)]
        y_ref[:, pl.ds(at, LANES)] = y
        z = inner_ref[:, pl.ds(at, LANES)]
        w = y * (z * sigmoid(z))
        return total + jnp.sum(w * w, axis=1, keepdims=True)

    total = lax.fori_loop(0, PAIRS_OF_HEADS, pair, jnp.zeros((rows, 1), F32), unroll=2)
    scale = lax.rsqrt(total / INNER + EPSILON)

    @pl.loop(0, PAIRS_OF_HEADS, unroll=2)
    def _(p):
        at = pl.multiple_of(p * LANES, LANES)
        z = inner_ref[:, pl.ds(at, LANES)]
        w = y_ref[:, pl.ds(at, LANES)] * (z * sigmoid(z))
        mixed = w * scale * gain_ref[:, pl.ds(at, LANES)]
        mixed_ref[:, pl.ds(at, LANES)] = mixed.astype(BF16)
        turned_ref[pl.ds(at, LANES), :] = mixed.T.astype(BF16)


def mixer_scratch(rows):
    return [
        pltpu.VMEM((rows, CONVCH), F32),
        pltpu.VMEM((PAIRS_OF_HEADS, rows, LANES), F32),
        pltpu.VMEM((HEADS, rows), F32),
        pltpu.VMEM((PAIRS_OF_HEADS, rows, LANES), F32),
        pltpu.VMEM((rows, rows), F32),
    ]


def mixer_forward(inner, taps, heads, skip, gain, position, inside):
    rows = inner.shape[0]
    shape = jax.ShapeDtypeStruct
    return pl.pallas_call(
        mixer_forward_kernel,
        out_shape=[
            shape((rows, INNER), BF16),
            shape((INNER, rows), BF16),
            shape((rows, INNER), F32),
        ],
        in_specs=[VMEM] * 7,
        out_specs=[VMEM] * 3,
        scratch_shapes=mixer_scratch(rows),
        compiler_params=BIG,
        name="mixer_forward",
    )(inner, taps, heads, skip, gain, position, inside)


def mixer_backward_steps(
    inner_ref, taps_ref, heads_ref, skip_ref, gain_ref, position_ref, inside_ref, y_ref, dmixed_ref,
    dinner_ref, dtaps_ref, dgain_ref, dskip_ref, dheads_ref,
    x_ref, qcol, qrow, dtpair, aff_ref, dx_ref, daff_ref, rowsum, stepgrad, colsum,
):
    rows = inner_ref.shape[0]
    position = position_ref[...]
    yield from mixer_setup(
        inner_ref, taps_ref, heads_ref, position, inside_ref[...], x_ref, qcol, qrow, dtpair
    )
    aff_ref[...] = (
        dot_rt_exact(x_ref[:, INNER : INNER + STATE], x_ref[:, INNER + STATE :]) * inside_ref[...].T
    )
    daff_ref[...] = jnp.zeros_like(daff_ref)
    stepgrad[...] = jnp.zeros_like(stepgrad)
    colsum[...] = jnp.zeros_like(colsum)
    lane = column_index((rows, LANES))
    first = lane < HDIM
    yield

    def sums(p, carry):
        squares, product = carry
        at = pl.multiple_of(p * LANES, LANES)
        z = inner_ref[:, pl.ds(at, LANES)]
        w = y_ref[:, pl.ds(at, LANES)] * (z * sigmoid(z))
        g = dmixed_ref[:, pl.ds(at, LANES)] * gain_ref[:, pl.ds(at, LANES)]
        return (
            squares + jnp.sum(w * w, axis=1, keepdims=True),
            product + jnp.sum(w * g, axis=1, keepdims=True),
        )

    zero = jnp.zeros((rows, 1), F32)
    squares, product = lax.fori_loop(0, PAIRS_OF_HEADS, sums, (zero, zero))
    scale = lax.rsqrt(squares / INNER + EPSILON)
    pull = scale * scale * scale * product / INNER
    yield

    def pair(p):
        at = pl.multiple_of(p * LANES, LANES)
        here = pl.ds(at, LANES)
        z = inner_ref[:, here]
        y = y_ref[:, here]
        sig = sigmoid(z)
        silu = z * sig
        w = y * silu
        g = dmixed_ref[:, here]
        dgain_ref[:, here] = jnp.sum(g * w * scale, axis=0, keepdims=True)
        dw = scale * (g * gain_ref[:, here]) - w * pull
        dinner_ref[:, here] = (dw * y * (sig * (1.0 + z * (1.0 - sig)))).astype(BF16)
        dy = dw * silu
        x = x_ref[:, here]
        dskip_ref[:, here] = jnp.sum(dy * x, axis=0, keepdims=True)
        steps = dtpair[p]
        scaled = x * steps
        low = dy.astype(BF16)
        outs = []
        columns = qcol[p]
        for k in (0, 1):
            h = 2 * p + k
            gaps = qrow[pl.ds(h, 1), :] - columns[:, k * HDIM : k * HDIM + 1]
            decay = jnp.exp(jnp.minimum(gaps, 0.0))
            prod = decay * aff_ref[...]
            own = first if k == 0 else jnp.logical_not(first)
            dprod = dot_rt(jnp.where(own, scaled, 0.0).astype(BF16), low)
            daff_ref[...] += dprod * decay
            both = dprod * prod
            rowsum[pl.ds(h, 1), :] = jnp.sum(both, axis=0, keepdims=True)
            away = jnp.sum(both, axis=1, keepdims=True)
            colsum[...] += jnp.where(lane == h, away, 0.0)
            outs.append(dot(prod.astype(BF16), low))
        dscaled = jnp.where(first, outs[0], outs[1])
        dx_ref[:, here] = dscaled * steps + dy * skip_ref[:, here]
        gain_step = dscaled * x
        left = jnp.sum(jnp.where(first, gain_step, 0.0), axis=1, keepdims=True)
        right = jnp.sum(jnp.where(first, 0.0, gain_step), axis=1, keepdims=True)
        stepgrad[...] += jnp.where(lane == 2 * p, left, 0.0) + jnp.where(
            lane == 2 * p + 1, right, 0.0
        )

    for start, end in spans(PAIRS_OF_HEADS, 6):
        pl.loop(start, end)(pair)
        yield

    daff = daff_ref[...] * inside_ref[...].T
    dx_ref[:, INNER : INNER + STATE] = dot_exact(daff, x_ref[:, INNER + STATE :])
    dx_ref[:, INNER + STATE :] = dot_exact(daff.T, x_ref[:, INNER : INNER + STATE])
    yield
    pad = jnp.zeros((LANES - HEADS, rows), F32)
    dsums = jnp.concatenate([rowsum[...], pad], axis=0).T - colsum[...]
    dlog = dot_exact(inside_ref[...].T, dsums)[:, :HEADS]
    raw, step, rates = step_sizes(inner_ref, heads_ref)
    dstep = stepgrad[:, :HEADS] + dlog * rates
    draw = dstep * sigmoid(raw)
    dinner_ref[:, INNER + CONVCH :] = draw.astype(BF16)
    dheads_ref[0:1, :HEADS] = jnp.sum(dlog * step, axis=0, keepdims=True) * rates
    dheads_ref[1:2, :HEADS] = jnp.sum(draw, axis=0, keepdims=True)
    yield

    def conv_back(k):
        here = pl.ds(pl.multiple_of(k * LANES, LANES), LANES)
        there = pl.ds(pl.multiple_of(INNER + k * LANES, LANES), LANES)
        conv_in = inner_ref[:, there]
        taps = taps_ref[:, here]
        before = conv_before(conv_in, taps, position)
        sig = sigmoid(before)
        grad = dx_ref[:, here] * (sig * (1.0 + before * (1.0 - sig)))
        back = grad * taps[TAPS - 1 : TAPS]
        dtaps_ref[TAPS - 1 : TAPS, here] = jnp.sum(grad * conv_in, axis=0, keepdims=True)
        for offset in range(1, TAPS):
            t = TAPS - 1 - offset
            valid = jnp.where(position >= offset, grad, 0.0)
            dtaps_ref[t : t + 1, here] = jnp.sum(
                valid * pltpu.roll(conv_in, offset, 0), axis=0, keepdims=True
            )
            back = back + pltpu.roll(valid, rows - offset, 0) * taps[t : t + 1]
        dinner_ref[:, there] = back.astype(BF16)

    for start, end in spans(CONVCH // LANES, 4):
        pl.loop(start, end)(conv_back)
        yield


def mixer_backward_scratch(rows):
    return mixer_scratch(rows) + [
        pltpu.VMEM((rows, CONVCH), F32),
        pltpu.VMEM((rows, rows), F32),
        pltpu.VMEM((HEADS, rows), F32),
        pltpu.VMEM((rows, LANES), F32),
        pltpu.VMEM((rows, LANES), F32),
    ]


def mixer_backward_shapes(inner, taps):
    shape = jax.ShapeDtypeStruct
    return [
        shape(inner.shape, BF16),
        shape(taps.shape, F32),
        shape((1, INNER), F32),
        shape((1, INNER), F32),
        shape((8, LANES), F32),
    ]


def rotate_rows(front, rear, cosine, sine):
    return front * cosine - rear * sine, rear * cosine + front * sine


def attention_setup(packed_ref, cosine_ref, sine_ref, query, key_rows):
    half = HD // 2
    for h in range(QH + KVH):
        at = h * HD
        turned = rotate_rows(
            packed_ref[at : at + half], packed_ref[at + half : at + HD],
            cosine_ref[...], sine_ref[...],
        )
        both = jnp.concatenate(turned, axis=0)
        if h < QH:
            query[at : at + HD] = both.astype(BF16)
        else:
            key_rows[at - QH * HD : at - (QH - 1) * HD] = both


def turned_probs(keys, query, outside):
    scores = dot(keys, query) * SCORE_SCALE + outside
    expo = jnp.exp(scores - jnp.max(scores, axis=0, keepdims=True))
    return expo / jnp.sum(expo, axis=0, keepdims=True)


def attention_forward_kernel(
    packed_ref, cosine_ref, sine_ref, outside_ref, context_ref, turned_ref, query, key_rows
):
    attention_setup(packed_ref, cosine_ref, sine_ref, query, key_rows)
    keys = key_rows[...].T.astype(BF16)
    values = packed_ref[(QH + KVH) * HD :].astype(BF16)
    for h in range(QH):
        kv = h * KVH // QH
        probs = turned_probs(
            keys[:, kv * HD : (kv + 1) * HD], query[h * HD : (h + 1) * HD], outside_ref[...]
        )
        turned = dot(values[kv * HD : (kv + 1) * HD], probs.astype(BF16))
        turned_ref[h * HD : (h + 1) * HD] = turned.astype(BF16)
    for k in range(QH * HD // LANES):
        here = slice(k * LANES, (k + 1) * LANES)
        context_ref[:, here] = turned_ref[here].astype(F32).T.astype(BF16)


def attention_forward(packed, cosine, sine, outside):
    rows = packed.shape[1]
    shape = jax.ShapeDtypeStruct
    return pl.pallas_call(
        attention_forward_kernel,
        out_shape=[shape((rows, QH * HD), BF16), shape((QH * HD, rows), BF16)],
        in_specs=[VMEM] * 4,
        out_specs=[VMEM] * 2,
        scratch_shapes=[pltpu.VMEM((QH * HD, rows), BF16), pltpu.VMEM((KVH * HD, rows), F32)],
        compiler_params=BIG,
        name="attention_forward",
    )(packed, cosine, sine, outside)


def attention_backward_steps(
    packed_ref, cosine_ref, sine_ref, outside_ref, dcontext_ref, dpacked_ref,
    query, key_rows, grad_rows,
):
    half = HD // 2
    attention_setup(packed_ref, cosine_ref, sine_ref, query, key_rows)
    low_rows = key_rows[...].astype(BF16)
    keys = key_rows[...].T.astype(BF16)
    values = packed_ref[(QH + KVH) * HD :].T.astype(BF16)
    for k in range(QH * HD // LANES):
        here = slice(k * LANES, (k + 1) * LANES)
        grad_rows[here] = dcontext_ref[:, here].astype(F32).T
    yield
    for kv in range(KVH):
        of_kv = slice(kv * HD, (kv + 1) * HD)
        dkey = jnp.zeros((HD, keys.shape[0]), F32)
        dvalue = jnp.zeros((HD, keys.shape[0]), F32)
        for h in range(kv * QH // KVH, (kv + 1) * QH // KVH):
            here = slice(h * HD, (h + 1) * HD)
            probs = turned_probs(keys[:, of_kv], query[here], outside_ref[...])
            grad = grad_rows[here].astype(BF16)
            dprobs = dot(values[:, of_kv], grad)
            dvalue = dvalue + dot_rt(grad, probs.astype(BF16))
            inner = jnp.sum(probs * dprobs, axis=0, keepdims=True)
            dscores = (probs * (dprobs - inner) * SCORE_SCALE).astype(BF16)
            dquery = dot(low_rows[of_kv], dscores)
            dkey = dkey + dot_rt(query[here], dscores)
            turned = rotate_rows(dquery[:half], dquery[half:], cosine_ref[...], -sine_ref[...])
            grad_rows[here] = jnp.concatenate(turned, axis=0)
            yield
        turned = rotate_rows(dkey[:half], dkey[half:], cosine_ref[...], -sine_ref[...])
        at = QH * HD + kv * HD
        grad_rows[at : at + HD] = jnp.concatenate(turned, axis=0)
        at = (QH + KVH) * HD + kv * HD
        grad_rows[at : at + HD] = dvalue
    for k in range((QH + 2 * KVH) * HD // LANES):
        here = slice(k * LANES, (k + 1) * LANES)
        dpacked_ref[:, here] = grad_rows[here].T.astype(BF16)
    yield


def attention_backward_scratch(rows):
    return [
        pltpu.VMEM((QH * HD, rows), BF16),
        pltpu.VMEM((KVH * HD, rows), F32),
        pltpu.VMEM(((QH + 2 * KVH) * HD, rows), F32),
    ]


def host_steps(ins, outs, scratch):
    yield from mixer_backward_steps(*ins[:9], *outs[:5], *scratch[:10])
    yield from attention_backward_steps(*ins[9:], outs[5], *scratch[10:])


def host_shapes(ins):
    rows, wide = ins[0].shape[0], ins[9].shape[0]
    return mixer_backward_shapes(ins[0], ins[1]) + [jax.ShapeDtypeStruct((rows, wide), BF16)]


def host_scratch(ins):
    rows = ins[0].shape[0]
    return mixer_backward_scratch(rows) + attention_backward_scratch(rows)


def host_plain(ins):
    shapes, scratch = host_shapes(ins), host_scratch(ins)

    def kernel(*refs):
        one, two = len(ins), len(ins) + len(shapes)
        run_steps(host_steps(refs[:one], refs[one:two], refs[two:]))

    return pl.pallas_call(
        kernel,
        out_shape=shapes,
        in_specs=[VMEM] * len(ins),
        out_specs=[VMEM] * len(shapes),
        scratch_shapes=scratch,
        compiler_params=BIG,
        name="mixer_attention_backward",
    )(*ins)


def flip(me, bit):
    step = 1 << bit
    return me + step * (1 - 2 * ((me // step) % 2))


def place(bits, free, mine, flipped=()):
    return tuple(
        slice(None) if b in free else 1 - mine[b] if b in flipped else mine[b]
        for b in reversed(range(bits))
    )


def greet(me, bits):
    barrier = pltpu.get_barrier_semaphore()
    for b in range(bits):
        pl.semaphore_signal(barrier, inc=1, device_id=(flip(me, b),), device_id_type=MESH)
    pl.semaphore_wait(barrier, bits)


def remote(me, src, dst, send, recv, bit):
    return pltpu.make_async_remote_copy(
        src_ref=src,
        dst_ref=dst,
        send_sem=send,
        recv_sem=recv,
        device_id=(flip(me, bit),),
        device_id_type=MESH,
    )


def take(refs, *sizes):
    groups, at = [], 0
    for size in sizes:
        groups.append(refs[at : at + size])
        at += size
    return groups + [refs[at:]]


def row_exchange(me, mine, row_bits, rows, got, send_sem, recv_sem):
    bits = len(row_bits)
    flight = {}

    def send(s):
        bit = row_bits[s]
        index = tuple(1 - mine[q] if q == bit else slice(None) for q in reversed(range(bits)))
        copy = remote(me, rows.at[index], got[s], send_sem.at[s], recv_sem.at[s], bit)
        copy.start()
        flight[0] = copy

    def receive(s):
        flight[0].wait_send()
        flight[0].wait_recv()

        @pl.loop(0, 1 << (bits - 1))
        def _(j):
            here, there, pos = [], [], bits - 1
            for q in reversed(range(bits)):
                if q == row_bits[s]:
                    here.append(1 - mine[q])
                else:
                    pos -= 1
                    value = (j // (1 << pos)) % 2
                    here.append(value)
                    there.append(value)
            rows[tuple(here)] = got[s][tuple(there)]

        if s + 1 < bits:
            send(s + 1)

    return send, receive


def gather_kernel(devices, chunks, events, layers, arrays, *refs):
    bits = devices.bit_length() - 1
    ins, rows_in, outs, rows_out, rows_got, sems = take(
        refs, arrays, 1, layers * arrays, 1, bits
    )
    send_sem, recv_sem, csend_sem, crecv_sem, own_sem, ro_s, ro_r = sems
    me = lax.axis_index("dp")
    mine = [(me // (1 << b)) % 2 for b in range(bits)]
    greet(me, bits)
    rows_send, rows_receive = row_exchange(
        me, mine, AG_ROW_BITS, rows_out[0], rows_got, ro_s, ro_r
    )
    fetch = pltpu.make_async_copy(rows_in[0], rows_out[0], ro_s.at[0])
    fetch.start()
    fetch.wait()
    rows_send(0)
    own, sends, cores, pending = [], [], [], {}
    for c, (l, a, order) in enumerate(chunks):
        here = outs[l * arrays + a].at[place(bits, (), mine)]
        src = ins[a].at[l]
        copy = remote(me, src, here, send_sem.at[c, 0], recv_sem.at[c, 0], order[0])
        copy.start()
        pending[c] = copy
        sends.append(copy)
        local = pltpu.make_async_copy(src, here, own_sem.at[c])
        local.start()
        own.append(local)
    for c, (l, a, order) in enumerate(chunks):
        here = outs[l * arrays + a].at[place(bits, (), mine)]
        copy = remote(me, ins[a].at[l], here, csend_sem.at[c, 0], crecv_sem.at[c, 0], 0)
        copy.start()
        sends.append(copy)
        cores.append(copy)
    for local in own:
        local.wait()
    for c, s in events:
        if c == -2:
            rows_receive(s)
            continue
        l, a, order = chunks[c]
        full = outs[l * arrays + a]
        pending[c].wait_recv()
        if s + 1 < bits - 1:
            view = full.at[place(bits, order[: s + 1], mine)]
            copy = remote(
                me, view, view, send_sem.at[c, s + 1], recv_sem.at[c, s + 1], order[s + 1]
            )
            copy.start()
            pending[c] = copy
            sends.append(copy)
        new = full.at[place(bits, order[:s], mine, (order[s],))]
        copy = remote(me, new, new, csend_sem.at[c, s + 1], crecv_sem.at[c, s + 1], 0)
        copy.start()
        sends.append(copy)
        cores.append(copy)
    for copy in sends:
        copy.wait_send()
    for copy in cores:
        copy.wait_recv()


def gather_all(shards, rows, devices):
    bits = devices.bit_length() - 1
    moved = rows.reshape((2,) * bits + (rows.shape[0] // devices, rows.shape[1]))
    layers = shards[0].shape[0]
    n = len(AG_CHUNKS)
    sent = {(layer, a) for layer, a, _ in AG_CHUNKS}
    outs = [
        jax.ShapeDtypeStruct(
            (2,) * bits + (s.shape[1:] if (layer, a) in sent else (8, 128)), s.dtype
        )
        for layer in range(layers)
        for a, s in enumerate(shards)
    ]
    anywhere = pl.BlockSpec(memory_space=pl.ANY)
    dma = pltpu.SemaphoreType.DMA
    *res, arrived = pl.pallas_call(
        functools.partial(gather_kernel, devices, AG_CHUNKS, AG_EVENTS, layers, len(shards)),
        out_shape=outs + [jax.ShapeDtypeStruct(moved.shape, BF16)],
        in_specs=[VMEM] * len(shards) + [anywhere],
        out_specs=[anywhere] * len(outs) + [VMEM],
        scratch_shapes=[pltpu.VMEM(moved.shape[1:], BF16)] * bits
        + [dma((n, bits - 1))] * 2
        + [dma((n, bits))] * 2
        + [dma((n,))]
        + [dma((bits,))] * 2,
        compiler_params=pltpu.CompilerParams(collective_id=0, has_side_effects=True),
        name="gather_all",
    )(*shards, moved)
    full = [r.reshape((devices * r.shape[-2], r.shape[-1])) for r in res]
    weights = [full[l * len(shards) : (l + 1) * len(shards)] for l in range(layers)]
    return weights, arrived.reshape(rows.shape)


PAIRS = ((0, 0), (1, 2), (0, 1), (2, 2), (3, 3), (4, 4))


def scatter_kernel(devices, plan, jobs, arrs, counts, *refs):
    chunks, events, row_bits = plan
    bits = devices.bit_length() - 1
    half = devices // 2
    nx, ny, nsmall, nrows, nhost, nhost_out = counts
    na, nc = len(arrs), len(chunks)
    xs, ys, small_in, rows_in, host_in, refs = take(refs, nx, ny, nsmall, nrows, nhost)
    outs, small_out, rows_out, host_out, refs = take(refs, na, nsmall, nrows, nhost_out)
    xr, yr, sums, parts, refs = take(refs, nx, ny, nc, nc * (bits - 1))
    small_mid, small_got, rows_got, refs = take(
        refs, nsmall * (bits - 1), nsmall * bits, nrows * bits
    )
    host_scratch_refs, sems = refs[:-10], refs[-10:]
    xs_s, xs_r, ys_s, ys_r, st_s, st_r, sm_s, sm_r, ro_s, ro_r = sems
    me = lax.axis_index("dp")
    mine = [(me // (1 << b)) % 2 for b in range(bits)]
    greet(me, bits)
    core = mine[0]
    swaps_x, swaps_y, got_x, got_y = {}, {}, set(), set()
    for a, _, _, _ in chunks:
        xi, yi = jobs[a]
        if xi not in swaps_x:
            swaps_x[xi] = remote(
                me, xs[xi].at[:, 1 - core], xr[xi], xs_s.at[xi], xs_r.at[xi], 0
            )
            swaps_x[xi].start()
        if yi not in swaps_y:
            swaps_y[yi] = remote(me, ys[yi], yr[yi], ys_s.at[yi], ys_r.at[yi], 0)
            swaps_y[yi].start()
    sends, pending = [], {}

    def small_send(s):
        src = small_in[0] if s == 0 else small_mid[s - 1]
        copy = remote(me, src, small_got[s], sm_s.at[s], sm_r.at[s], s)
        copy.start()
        pending["small"] = copy
        sends.append(copy)

    def small_receive(s):
        src = small_in[0] if s == 0 else small_mid[s - 1]
        pending["small"].wait_recv()
        total = src[...] + small_got[s][...]
        if s + 1 < bits:
            small_mid[s][...] = total
            small_send(s + 1)
        else:
            small_out[0][...] = total

    if nrows:
        rows_send, rows_receive = row_exchange(
            me, mine, row_bits, rows_out[0], rows_got, ro_s, ro_r
        )

    def send(c, s):
        order = chunks[c][3]
        index = tuple(
            1 - mine[q] if q == order[s] else mine[q] if q in order[:s] else slice(None)
            for q in reversed(range(1, bits))
        )
        copy = remote(
            me,
            sums[c].at[index],
            parts[c * (bits - 1) + s],
            st_s.at[c, s],
            st_r.at[c, s],
            order[s],
        )
        copy.start()
        pending[c] = copy
        sends.append(copy)

    def compute(c):
        a, first, end, _ = chunks[c]
        xi, yi = jobs[a]
        rows = arrs[a][0]
        if xi not in got_x:
            swaps_x[xi].wait_recv()
            got_x.add(xi)
        if yi not in got_y:
            swaps_y[yi].wait_recv()
            got_y.add(yi)

        def tile(start, width, offset):
            left = xs[xi][:, core].reshape(half * rows, -1)
            other = xr[xi][...].reshape(half * rows, -1)
            value = dot(left, ys[yi][:, pl.ds(start, width)])
            value = value + dot(other, yr[yi][:, pl.ds(start, width)])
            sums[c][..., pl.ds(offset, width)] = value.astype(BF16).reshape(
                (2,) * (bits - 1) + (rows, width)
            )

        width, step = end - first, 256
        whole = width // step

        @pl.loop(0, whole)
        def _(i):
            tile(
                pl.multiple_of(first + i * step, 128), step, pl.multiple_of(i * step, 128)
            )

        if width % step:
            tile(first + whole * step, width % step, whole * step)
        send(c, 0)

    def receive(c, s):
        a, first, end, order = chunks[c]
        pending[c].wait_recv()
        fixed = order[: s + 1]
        free = [q for q in reversed(range(1, bits)) if q not in fixed]

        def add(j, last):
            here, there, pos = [], [], len(free)
            for q in reversed(range(1, bits)):
                if q in fixed:
                    here.append(mine[q])
                else:
                    pos -= 1
                    value = (j // (1 << pos)) % 2
                    here.append(value)
                    there.append(value)
            part = parts[c * (bits - 1) + s]
            total = part[tuple(there)].astype(F32) + sums[c][tuple(here)].astype(F32)
            if last:
                outs[a][:, first:end] = total
            else:
                sums[c][tuple(here)] = total.astype(BF16)

        if not free:
            add(0, True)
        else:

            @pl.loop(0, 1 << len(free))
            def _(j):
                add(j, False)

            send(c, s + 1)

    steps = host_steps(host_in, host_out, host_scratch_refs) if nhost else iter(())
    if nsmall:
        small_send(0)
    if nrows:
        fetch = pltpu.make_async_copy(rows_in[0], rows_out[0], ro_s.at[0])
        fetch.start()
        fetch.wait()
        rows_send(0)
    for c, s in events:
        if c == -1:
            small_receive(s)
        elif c == -2:
            rows_receive(s)
        elif c == -3:
            next(steps, None)
        elif s < 0:
            compute(c)
        else:
            receive(c, s)
    run_steps(steps)
    for copy in list(swaps_x.values()) + list(swaps_y.values()) + sends:
        copy.wait_send()


def scatter(plan, jobs, turned, grads, devices, number, small=None, rows=None, host=()):
    chunks = plan[0]
    bits = devices.bit_length() - 1
    nx, ny = len(turned), len(grads)
    half = devices // 2
    split = [x.reshape(half, 2, x.shape[0] // devices, x.shape[1]) for x in turned]
    arrs = [(turned[xi].shape[0] // devices, grads[yi].shape[1]) for xi, yi in jobs]
    smalls = [] if small is None else [small]
    moved = []
    if rows is not None:
        moved.append(rows.reshape((2,) * bits + (rows.shape[0] // devices, rows.shape[1])))
    shape = jax.ShapeDtypeStruct
    extra = host_shapes(host) if host else []
    outs = [shape(size, F32) for size in arrs] + [shape(x.shape, F32) for x in smalls]
    outs += [shape(x.shape, BF16) for x in moved] + extra
    scratch = [pltpu.VMEM((half, x.shape[0] // devices, x.shape[1]), BF16) for x in turned]
    scratch += [pltpu.VMEM(y.shape, BF16) for y in grads]
    for a, first, end, _ in chunks:
        scratch.append(pltpu.VMEM((2,) * (bits - 1) + (arrs[a][0], end - first), BF16))
    for a, first, end, _ in chunks:
        for s in range(bits - 1):
            scratch.append(pltpu.VMEM((2,) * (bits - 2 - s) + (arrs[a][0], end - first), BF16))
    for x in smalls:
        scratch += [pltpu.VMEM(x.shape, F32)] * (2 * bits - 1)
    for x in moved:
        scratch += [pltpu.VMEM(x.shape[1:], BF16)] * bits
    if host:
        scratch += host_scratch(host)
    dma = pltpu.SemaphoreType.DMA
    scratch += [dma((nx,))] * 2 + [dma((ny,))] * 2 + [dma((len(chunks), bits - 1))] * 2
    scratch += [dma((bits,))] * 4
    counts = (nx, ny, len(smalls), len(moved), len(host), len(extra))
    res = pl.pallas_call(
        functools.partial(scatter_kernel, devices, plan, jobs, arrs, counts),
        out_shape=outs,
        in_specs=[VMEM] * (nx + ny + len(smalls))
        + [pl.BlockSpec(memory_space=pl.ANY)] * len(moved)
        + [VMEM] * len(host),
        out_specs=[VMEM] * len(outs),
        scratch_shapes=scratch,
        compiler_params=pltpu.CompilerParams(
            collective_id=number, has_side_effects=True, vmem_limit_bytes=67043328
        ),
        name="scatter",
    )(*split, *grads, *smalls, *moved, *host)
    owned, small_total, back, own_work = take(res, len(arrs), len(smalls), len(moved))
    return owned, small_total, [x.reshape(rows.shape) for x in back], own_work


def scatter_plain(turned, grads, small):
    owned = [
        lax.psum_scatter(
            dot(turned[xi], grads[yi]).astype(BF16), "dp", scatter_dimension=0, tiled=True
        ).astype(F32)
        for xi, yi in PAIRS
    ]
    return owned + [lax.psum(small, "dp")]


def doc_layout(doc_lengths, rows_count):
    rows_index = jnp.arange(rows_count, dtype=jnp.int32)
    doc_ends = jnp.cumsum(doc_lengths, dtype=jnp.int32)
    later = (rows_index[:, None] >= doc_ends[None, :]).astype(jnp.int32)
    segment = jnp.sum(later, axis=1, dtype=jnp.int32)
    position = rows_index - jnp.sum(later * doc_lengths[None, :], axis=1, dtype=jnp.int32)
    return (segment, position)


def inverse_rms(values):
    return lax.rsqrt(jnp.mean(values * values, axis=-1, keepdims=True) + EPSILON)


def norm_backward(grad, values, scale, gain):
    normed = values * scale
    grad_gain = jnp.sum(grad * normed, axis=0)
    inner = grad * gain
    return scale * (inner - normed * jnp.mean(inner * normed, axis=-1, keepdims=True)), grad_gain


def layer_forward(hidden, weights, small, layout):
    w_in, w_mix, w_qkv, w_attn, w_gate_up, w_down = weights
    gains, taps, gain_inner, heads, skip = small
    position, inside, outside, cosine, sine = layout
    scale = inverse_rms(hidden)
    normed = (hidden * scale * gains[0]).astype(BF16)
    inner = dot(normed, w_in)
    packed = lax.dot_general(
        w_qkv, normed, (((0,), (1,)), ((), ())), preferred_element_type=F32
    )
    mixed, mixed_rows, y = mixer_forward(inner, taps, heads, skip, gain_inner, position, inside)
    context, context_rows = attention_forward(packed, cosine, sine, outside)
    middle = hidden + dot(mixed, w_mix) + dot(context, w_attn)
    scale_two = inverse_rms(middle)
    normed_two = (middle * scale_two * gains[1]).astype(BF16)
    both = dot(normed_two, w_gate_up)
    active = (jax.nn.silu(both[:, :FF]) * both[:, FF:]).astype(BF16)
    out = middle + dot(active, w_down)
    turned = [normed.T, mixed_rows, context_rows, normed_two.T, active.T]
    return out, (hidden, scale, inner, packed, y, middle, scale_two, both, turned)


def backward_start(grad, kept, weights, small, layout):
    w_in, w_mix, w_qkv, w_attn, w_gate_up, w_down = weights
    gains, taps, gain_inner, heads, skip = small
    position, inside, outside, cosine, sine = layout
    hidden, scale, inner, packed, y, middle, scale_two, both, turned = kept
    ddown = grad.astype(BF16)
    dactive = dot_rt(ddown, w_down)
    gate, up = both[:, :FF], both[:, FF:]
    sig = jax.nn.sigmoid(gate)
    dgate = dactive * up * (sig * (1.0 + gate * (1.0 - sig)))
    dboth = jnp.concatenate([dgate, dactive * (gate * sig)], axis=1).astype(BF16)
    dmiddle, dgain_two = norm_backward(dot_rt(dboth, w_gate_up), middle, scale_two, gains[1])
    dmiddle = grad + dmiddle
    dbranch = dmiddle.astype(BF16)
    dmixed = dot_rt(dbranch, w_mix)
    dcontext = dot_rt(dbranch, w_attn).astype(BF16)
    host = (inner, taps, heads, skip, gain_inner, position, inside, y, dmixed)
    host += (packed, cosine, sine, outside, dcontext)
    return dmiddle, dgain_two, dbranch, dboth, ddown, host


def backward_end(dmiddle, dgain_two, kept, weights, small, done):
    w_in, w_qkv = weights[0], weights[2]
    hidden, scale = kept[:2]
    dinner, dtaps, dgain_inner, dskip, dheads, dpacked = done
    dnormed = dot_rt(dinner, w_in) + dot_rt(dpacked, w_qkv)
    dhidden, dgain = norm_backward(dnormed, hidden, scale, small[0][0])
    flat = [dgain, dgain_two, dtaps.reshape(-1), dgain_inner[0], dheads[0, :HEADS]]
    flat += [jnp.sum(dskip.reshape(HEADS, HDIM), axis=1), dheads[1, :HEADS]]
    flat = jnp.concatenate(flat)
    lines = -(-flat.shape[0] // 1024) * 8
    small_sum = jnp.pad(flat, (0, lines * 128 - flat.shape[0])).reshape(lines, 128)
    return dmiddle + dhidden, small_sum


def shards(
    tokens,
    cotangent,
    destination,
    lengths,
    norm_gains,
    in_proj,
    conv_weight,
    ssm_gain,
    mixer_out,
    qkv_proj,
    attn_out,
    gate_up,
    down_proj,
    a_log,
    d_skip,
    dt_bias,
):
    devices = lax.axis_size("dp")
    me = lax.axis_index("dp")
    rows_here, width = tokens.shape
    share = rows_here // devices
    own_kernels = devices == 32
    index = jnp.arange(rows_here, dtype=jnp.int32)
    slabs = destination.reshape(devices, rows_here)

    own = lax.dynamic_slice_in_dim(slabs, me, 1, 0)[0] // rows_here
    same = (own[:, None] == own[None, :]) & (index[None, :] < index[:, None])
    slot = own * share + jnp.sum(same.astype(jnp.int32), axis=1)
    leave = (slot[None, :] == index[:, None]).astype(BF16)

    def exchange(rows):
        split = rows.reshape(devices, share, width)
        moved = lax.all_to_all(split, "dp", split_axis=0, concat_axis=0, tiled=True)
        return moved.reshape(rows_here, width)

    outgoing = dot(leave, tokens).astype(BF16)
    matrices = (in_proj, mixer_out, qkv_proj, attn_out, gate_up, down_proj)
    gain_part, conv_part, inner_part = (x.shape[-1] for x in (norm_gains, conv_weight, ssm_gain))
    packed = jnp.concatenate(
        [norm_gains.reshape(LAYERS, -1), conv_weight.reshape(LAYERS, -1), ssm_gain], axis=1
    )
    used = packed.shape[1]
    if own_kernels:
        room = SMALL_ROWS * 128
        padded = jnp.pad(packed, ((0, 0), (0, room - used))).reshape(LAYERS, SMALL_ROWS, 128)
        gathered, arrived = gather_all(list(matrices) + [padded], outgoing, devices)
        weights = [g[:-1] for g in gathered]
        after = gathered[0][-1][:1, :1] * 0
        weights[1][LATE_ARRAY] = lax.all_gather(
            matrices[LATE_ARRAY][1] + after, "dp", axis=0, tiled=True
        )
        smalls = [g[-1].reshape(devices, room)[:, :used] for g in gathered]
        late_cotangent = cotangent + after
    else:
        arrived = exchange(outgoing)
        weights = [
            [lax.all_gather(x[layer], "dp", axis=0, tiled=True) for x in matrices]
            for layer in range(LAYERS)
        ]
        every = lax.all_gather(packed, "dp", axis=0)
        smalls = [every[:, layer] for layer in range(LAYERS)]
        late_cotangent = cotangent
    arrived_cotangent = exchange(dot(leave, late_cotangent).astype(BF16))

    local = slabs - me * rows_here
    mask = ((local >= 0) & (local < rows_here)).astype(BF16)
    below = (index[:, None] < index[None, :]).astype(BF16)
    rank = dot(mask, below).astype(jnp.int32)
    order = rank + share * jnp.arange(devices, dtype=jnp.int32)[:, None]
    hits = local.reshape(-1)[None, :] == index[:, None]
    taken = jnp.sum(jnp.where(hits, order.reshape(-1)[None, :], 0), axis=1)
    enter = (taken[:, None] == index[None, :]).astype(BF16)
    hidden = dot(enter, arrived)
    upstream = dot(enter, arrived_cotangent)

    segment, position = doc_layout(lengths[0], rows_here)
    inside = (segment[:, None] == segment[None, :]) & (index[:, None] >= index[None, :])
    inverse = ROPE_BASE ** (-(jnp.arange(HD // 2, dtype=F32) * 2.0 / HD))
    angles = position.astype(F32)[:, None] * inverse[None, :]
    outside = jnp.where(inside.T, 0.0, -1e30)
    layout = (position[:, None], inside.astype(F32), outside, jnp.cos(angles).T, jnp.sin(angles).T)

    def spread(piece, count):
        shaped = piece.reshape(devices, count, -1)
        return jnp.swapaxes(shaped, 0, 1).reshape(count, -1).astype(F32)

    def small_of(layer):
        both = smalls[layer]
        mid = 2 * gain_part
        heads = jnp.stack([a_log[layer], d_skip[layer], dt_bias[layer]])
        return (
            spread(both[:, :mid], 2),
            spread(both[:, mid : mid + TAPS * conv_part], TAPS),
            spread(both[:, mid + TAPS * conv_part :], 1),
            jnp.pad(heads, ((0, 5), (0, LANES - HEADS))),
            jnp.repeat(d_skip[layer], HDIM)[None],
        )

    params = [small_of(layer) for layer in range(LAYERS)]

    kept = [None] * LAYERS
    for layer in range(LAYERS):
        hidden, kept[layer] = layer_forward(hidden, weights[layer], params[layer], layout)

    def permute_back(choice, rows):
        return lax.dot_general(
            choice, rows.astype(BF16), (((0,), (0,)), ((), ())), preferred_element_type=F32
        )

    top, low = 1, 0
    start = backward_start(upstream, kept[top], weights[top], params[top], layout)
    dmiddle, dgain_two, dbranch, dboth, ddown, host = start
    if own_kernels:
        up_down, _, _, done = scatter(
            PLAN_A, ((0, 0), (1, 1)), kept[top][-1][3:], [dboth, ddown], devices, 1, host=host
        )
    else:
        done = host_plain(host)
    flowing, small_top = backward_end(
        dmiddle, dgain_two, kept[top], weights[top], params[top], done
    )
    turned_top = kept[top][-1]
    grads_top = [done[0], done[5], dbranch, dboth, ddown]

    start = backward_start(flowing, kept[low], weights[low], params[low], layout)
    dmiddle, dgain_two, dbranch, dboth, ddown, host = start
    leaving = permute_back(enter, hidden).astype(BF16)
    turned_low = kept[low][-1]
    if own_kernels:
        second, sum_top, home, done = scatter(
            PLAN_B,
            ((0, 0), (1, 2), (0, 1), (2, 2), (3, 3), (4, 4)),
            turned_top[:3] + turned_low[3:],
            grads_top[:3] + [dboth, ddown],
            devices,
            2,
            small=small_top,
            rows=leaving,
            host=host,
        )
    else:
        done = host_plain(host)
    flowing, small_low = backward_end(
        dmiddle, dgain_two, kept[low], weights[low], params[low], done
    )
    grads_low = [done[0], done[5], dbranch, dboth, ddown]
    leaving_grad = permute_back(enter, flowing).astype(BF16)
    if own_kernels:
        third, sum_low, home_grad, _ = scatter(
            PLAN_C,
            ((0, 0), (1, 2), (0, 1), (2, 2)),
            turned_low[:3],
            grads_low[:3],
            devices,
            3,
            small=small_low,
            rows=leaving_grad,
        )
        home, home_grad = home[0], home_grad[0]
        owned = [third + second[4:] + sum_low, second[:4] + up_down + sum_top]
    else:
        owned = [
            scatter_plain(turned_low, grads_low, small_low),
            scatter_plain(turned_top, grads_top, small_top),
        ]
        home, home_grad = exchange(leaving), exchange(leaving_grad)
    out_tokens = permute_back(leave, home).astype(BF16)
    in_grad = permute_back(leave, home_grad)

    big = [jnp.stack([owned[layer][k] for layer in range(LAYERS)]) for k in range(6)]
    totals = jnp.stack([owned[layer][6].reshape(-1) for layer in range(LAYERS)])
    model = gain_part * devices
    sizes = (2 * model, TAPS * CONVCH, INNER, HEADS, HEADS, HEADS)
    pieces, at = [], 0
    for size in sizes:
        pieces.append(totals[:, at : at + size])
        at += size

    def mine(piece, count, part):
        shaped = piece.reshape(LAYERS, count, devices * part)
        return lax.dynamic_slice_in_dim(shaped, me * part, part, 2)

    return (
        out_tokens,
        in_grad,
        mine(pieces[0], 2, gain_part),
        big[0],
        mine(pieces[1], TAPS, conv_part),
        mine(pieces[2], 1, inner_part)[:, 0],
        big[1],
        big[2],
        big[3],
        big[4],
        big[5],
        pieces[3],
        pieces[4],
        pieces[5],
    )


def solution(mesh):
    placed = (
        P("dp", None),
        P("dp", None),
        P(),
        P("dp", None),
        P(None, None, "dp"),
        P(None, "dp", None),
        P(None, None, "dp"),
        P(None, "dp"),
        P(None, "dp", None),
        P(None, "dp", None),
        P(None, "dp", None),
        P(None, "dp", None),
        P(None, "dp", None),
        P(),
        P(),
        P(),
    )
    return jax.shard_map(
        shards,
        mesh=mesh,
        in_specs=placed,
        out_specs=(
            P("dp", None),
            P("dp", None),
            P(None, None, "dp"),
            P(None, "dp", None),
            P(None, None, "dp"),
            P(None, "dp"),
            P(None, "dp", None),
            P(None, "dp", None),
            P(None, "dp", None),
            P(None, "dp", None),
            P(None, "dp", None),
            P(),
            P(),
            P(),
        ),
        check_vma=False,
    )
```
